8 devices in a mesh: local: 4 (over z, y, x), data: 2 (over core).
Axes of the slice: x: 2, y: 2, z: 1, core: 2. Of those that a mesh axis runs over, the one named last changes fastest.
Arguments:
- x_in: bfloat16 [32768, 1024], P(('local', 'data'))
- grad_out: bfloat16 [32768, 1024], P(('local', 'data'))
- w_in: bfloat16 [5, 1024, 4096], P(None, ('local', 'data'))
- w_out: bfloat16 [5, 4096, 1024], P(None, ('local', 'data'))
Outputs:
- output 1: bfloat16 [32768, 1024], P(('local', 'data'))
- output 2: float32 [5, 1024, 4096], P(None, ('local', 'data'))
- output 3: float32 [5, 4096, 1024], P(None, ('local', 'data'))
- output 4: bfloat16 [32768, 1024], P(('local', 'data'))
All inputs are finite; a program needn't handle non-finite values.
Results may differ from the reference program's by a relative error of at most 0.02.
Values are sent between devices in bfloat16 or wider.
A program may use at most 1 GiB of HBM per device.

```python
import jax
import jax.numpy as jnp
from jax import lax

MODEL_DIM = 1024
FFN_DIM = 4096
LAYERS = 5
TOK_DEV = 4096
TOKENS = 32768
NORM_EPS = 1e-6


def setup_inputs(seed: int = 0) -> dict:
    key_list = jax.random.split(jax.random.key(seed), 4)
    x_in = jax.random.normal(key_list[0], (TOKENS, MODEL_DIM), jnp.float32)
    grad_out = jax.random.normal(key_list[1], (TOKENS, MODEL_DIM), jnp.float32) * TOKENS ** -0.5
    w_in = jax.random.normal(key_list[2], (LAYERS, MODEL_DIM, FFN_DIM), jnp.float32) * MODEL_DIM ** -0.5
    w_out = jax.random.normal(key_list[3], (LAYERS, FFN_DIM, MODEL_DIM), jnp.float32) * (1.5 * FFN_DIM ** -0.5)
    return {'x_in': x_in.astype(jnp.bfloat16), 'grad_out': grad_out.astype(jnp.bfloat16), 'w_in': w_in.astype(jnp.bfloat16), 'w_out': w_out.astype(jnp.bfloat16)}


def norm_rows(x_rows):
    x_wide = x_rows.astype(jnp.float32)
    inv_rms = lax.rsqrt(jnp.mean(x_wide * x_wide, axis=-1, keepdims=True) + NORM_EPS)
    return x_wide * inv_rms, inv_rms


def layer_inner(x_rows, w_in):
    unit_wide, inv_rms = norm_rows(x_rows)
    unit_rows = unit_wide.astype(jnp.bfloat16)
    pre_act = jnp.dot(unit_rows, w_in, preferred_element_type=jnp.float32).astype(jnp.bfloat16)
    gelu_val, gelu_back = jax.vjp(jax.nn.gelu, pre_act.astype(jnp.float32))
    return unit_wide, inv_rms, unit_rows, gelu_val.astype(jnp.bfloat16), gelu_back


def layer_forward(x_rows, w_in, w_out):
    hidden = layer_inner(x_rows, w_in)[3]
    branch = jnp.dot(hidden, w_out, preferred_element_type=jnp.float32)
    return (x_rows.astype(jnp.float32) + branch).astype(jnp.bfloat16)


def layer_backward(x_rows, grad_rows, w_in, w_out):
    unit_wide, inv_rms, unit_rows, hidden, gelu_back = layer_inner(x_rows, w_in)
    grad_hidden = jnp.dot(grad_rows, w_out.T, preferred_element_type=jnp.float32)
    grad_pre = gelu_back(grad_hidden)[0].astype(jnp.bfloat16)
    grad_w_out = jnp.dot(hidden.T, grad_rows, preferred_element_type=jnp.float32)
    grad_w_in = jnp.dot(unit_rows.T, grad_pre, preferred_element_type=jnp.float32)
    grad_unit = jnp.dot(grad_pre, w_in.T, preferred_element_type=jnp.float32)
    row_mean = jnp.mean(grad_unit * unit_wide, axis=-1, keepdims=True)
    grad_x = grad_rows.astype(jnp.float32) + inv_rms * (grad_unit - unit_wide * row_mean)
    return grad_x.astype(jnp.bfloat16), grad_w_in, grad_w_out


def block_grads(x_rows, grad_rows, w_in, w_out):
    def fwd_step(x_cur, weights):
        return layer_forward(x_cur, weights[0], weights[1]), x_cur

    x_last, saved_x = lax.scan(fwd_step, x_rows, (w_in, w_out))

    def bwd_step(grad_cur, step_items):
        grad_next, part_in, part_out = layer_backward(step_items[0], grad_cur, step_items[1], step_items[2])
        return grad_next, (part_in, part_out)

    grad_first, part_pair = lax.scan(bwd_step, grad_rows, (saved_x, w_in, w_out), reverse=True)
    return x_last, grad_first, part_pair[0], part_pair[1]


def reference(x_in, grad_out, w_in, w_out):
    blocks = TOKENS // TOK_DEV
    x_blocks = x_in.reshape(blocks, TOK_DEV, MODEL_DIM)
    grad_blocks = grad_out.reshape(blocks, TOK_DEV, MODEL_DIM)

    def block_step(acc_pair, step_items):
        x_last, grad_first, part_in, part_out = block_grads(step_items[0], step_items[1], w_in, w_out)
        return (acc_pair[0] + part_in, acc_pair[1] + part_out), (x_last, grad_first)

    start_acc = (jnp.zeros((LAYERS, MODEL_DIM, FFN_DIM), jnp.float32), jnp.zeros((LAYERS, FFN_DIM, MODEL_DIM), jnp.float32))
    acc_pair, row_outs = lax.scan(block_step, start_acc, (x_blocks, grad_blocks))
    return row_outs[0].reshape(TOKENS, MODEL_DIM), acc_pair[0], acc_pair[1], row_outs[1].reshape(TOKENS, MODEL_DIM)
```

```python
import functools

import jax
import jax.numpy as jnp
from jax import lax
from jax.experimental import pallas as pl
from jax.experimental.pallas import tpu as pltpu
from jax.sharding import PartitionSpec as P

NORM_EPS = 1e-6
GELU_A = 0.7978845608028654
GELU_B = GELU_A * 0.044715
LAST_LAST = (((1,), (1,)), ((), ()))
FIRST_FIRST = (((0,), (0,)), ((), ()))
BF16 = jnp.bfloat16
F32 = jnp.float32

CHIPS = 4
SHARDS = 8
LANES = 128
TOK_TILE = 256
CHUNK = 256
VMEM_LIMIT = 60 * 1024 * 1024


def unit_rows_of(x_tile):
    x_wide = x_tile.astype(F32)
    inv_rms = lax.rsqrt(jnp.mean(x_wide * x_wide, axis=-1, keepdims=True) + NORM_EPS)
    return x_wide, inv_rms


def lane_join(ref, first, count, rows=None):
    if rows is None:
        return jnp.concatenate([ref[first + b] for b in range(count)], axis=1)
    return jnp.concatenate([ref[first + b, rows, :] for b in range(count)], axis=1)


def weight_copies(order_ref, w_in_pieces, w_out_pieces, w_in_buf, w_out_buf, sem):
    hidden_blocks = w_in_buf.shape[0] // SHARDS
    depth = w_in_buf.shape[1] // SHARDS
    width = w_out_buf.shape[1] // SHARDS
    groups = []
    for p in range(SHARDS):
        block = order_ref[1, p] * hidden_blocks
        copies = []
        for q, (ref, at) in enumerate(w_in_pieces):
            row = pl.multiple_of(order_ref[0, q] * depth, depth)
            copies.append(
                pltpu.make_async_copy(
                    ref.at[at, pl.ds(block, hidden_blocks)],
                    w_in_buf.at[pl.ds(p * hidden_blocks, hidden_blocks), pl.ds(row, depth)],
                    sem.at[p],
                )
            )
        ref, at = w_out_pieces[p]
        copies.append(pltpu.make_async_copy(ref.at[at], w_out_buf.at[:, pl.ds(p * width, width)], sem.at[p]))
        groups.append(copies)
    return groups


def with_weights(order_ref, w_in_pieces, w_out_pieces, w_in_buf, w_out_buf, sem, body):
    step = pl.program_id(0)

    @pl.when(step == 0)
    def _():
        groups = weight_copies(order_ref, w_in_pieces, w_out_pieces, w_in_buf, w_out_buf, sem)
        for copies in groups:
            for copy in copies:
                copy.start()

        def wait(p):
            for copy in groups[p]:
                copy.wait()

        body(wait)

    @pl.when(step > 0)
    def _():
        body(lambda p: None)


def forward_kernel(pieces, order_ref, x_ref, *refs):
    n_in, n_out = len(pieces[0]), len(pieces[1])
    w_in_refs, w_out_refs = refs[:n_in], refs[n_in : n_in + n_out]
    y_ref, w_in_buf, w_out_buf, sem = refs[n_in + n_out :]
    w_in_pieces = [(w_in_refs[a], i) for a, i in piece_list(pieces[0])]
    w_out_pieces = [(w_out_refs[a], i) for a, i in piece_list(pieces[1])]
    hidden_size = w_out_buf.shape[1]
    per_group = hidden_size // SHARDS // CHUNK
    blocks = CHUNK // LANES
    d_blocks = w_out_buf.shape[0]

    def body(wait):
        x_wide, inv_rms = unit_rows_of(x_ref[...])
        unit = (x_wide * inv_rms).astype(BF16)
        total = None
        pending = []

        def finish(total):
            chunk, hidden = pending.pop(0)
            w_out = lane_join(w_out_buf, 0, d_blocks, pl.ds(chunk * CHUNK, CHUNK))
            part = jnp.dot(hidden, w_out, preferred_element_type=F32)
            return part if total is None else total + part

        for chunk in range(hidden_size // CHUNK):
            if chunk % per_group == 0:
                wait(chunk // per_group)
            w_in = lane_join(w_in_buf, chunk * blocks, blocks)
            pre = jnp.dot(unit, w_in, preferred_element_type=F32).astype(BF16).astype(F32)
            tanh = jnp.tanh(pre * (GELU_A + GELU_B * (pre * pre)))
            pending.append((chunk, (pre * (0.5 * tanh + 0.5)).astype(BF16)))
            if len(pending) > 2:
                total = finish(total)
        while pending:
            total = finish(total)
        y_ref[...] = (x_ref[...].astype(F32) + total).astype(BF16)

    with_weights(order_ref, w_in_pieces, w_out_pieces, w_in_buf, w_out_buf, sem, body)


def backward_kernel(pieces, order_ref, x_ref, dy_ref, *refs):
    n_in, n_out = len(pieces[0]), len(pieces[1])
    w_in_refs, w_out_refs = refs[:n_in], refs[n_in : n_in + n_out]
    unit_ref, hidden_ref, dpre_ref, dx_ref, w_in_buf, w_out_buf, sem = refs[n_in + n_out :]
    w_in_pieces = [(w_in_refs[a], i) for a, i in piece_list(pieces[0])]
    w_out_pieces = [(w_out_refs[a], i) for a, i in piece_list(pieces[1])]
    hidden_size = w_out_buf.shape[1]
    per_group = hidden_size // SHARDS // CHUNK
    blocks = CHUNK // LANES
    d_blocks = w_out_buf.shape[0]

    def body(wait):
        x_wide, inv_rms = unit_rows_of(x_ref[...])
        unit = (x_wide * inv_rms).astype(BF16)
        for b in range(d_blocks):
            unit_ref[b] = unit[:, b * LANES : (b + 1) * LANES]
        dy = dy_ref[...]
        total = None
        pending = []

        def finish(total):
            chunk, dpre = pending.pop(0)
            part = lax.dot_general(dpre, lane_join(w_in_buf, chunk * blocks, blocks), LAST_LAST, preferred_element_type=F32)
            return part if total is None else total + part

        for chunk in range(hidden_size // CHUNK):
            group = chunk // per_group
            if chunk % per_group == 0:
                wait(group)
            w_in = lane_join(w_in_buf, chunk * blocks, blocks)
            w_out = lane_join(w_out_buf, 0, d_blocks, pl.ds(chunk * CHUNK, CHUNK))
            pre = jnp.dot(unit, w_in, preferred_element_type=F32).astype(BF16).astype(F32)
            dhidden = lax.dot_general(dy, w_out, LAST_LAST, preferred_element_type=F32)
            poly = GELU_A + GELU_B * (pre * pre)
            cdf = 0.5 * jnp.tanh(pre * poly) + 0.5
            hidden = pre * cdf
            slope = cdf + (hidden * (6.0 * poly - 4.0 * GELU_A)) * (1.0 - cdf)
            hidden = hidden.astype(BF16)
            dpre = (slope * dhidden).astype(BF16)
            first = order_ref[1, group] * (per_group * blocks) + chunk % per_group * blocks
            for b in range(blocks):
                hidden_ref[first + b] = hidden[:, b * LANES : (b + 1) * LANES]
                dpre_ref[first + b] = dpre[:, b * LANES : (b + 1) * LANES]
            pending.append((chunk, dpre))
            if len(pending) > 2:
                total = finish(total)
        while pending:
            total = finish(total)
        value = x_ref[...].astype(F32) * inv_rms
        row_mean = jnp.mean(total * value, axis=-1, keepdims=True)
        dx_ref[...] = (dy_ref[...].astype(F32) + inv_rms * (total - value * row_mean)).astype(BF16)

    with_weights(order_ref, w_in_pieces, w_out_pieces, w_in_buf, w_out_buf, sem, body)


def piece_list(arrays):
    return [(a, i) for a, i in arrays.order]


class Pieces:
    def __init__(self, arrays, order):
        self.arrays, self.order = arrays, order

    def __len__(self):
        return len(self.arrays)


def layer_call(kernel, name, order, rows, w_in, w_out, outs, flops):
    tokens, width = rows[0].shape
    hidden_size = w_out.arrays[0].shape[2] * SHARDS
    blocks_d, blocks_f = width // LANES, hidden_size // LANES
    row_spec = pl.BlockSpec((TOK_TILE, width), lambda i, order: (i, 0))
    shapes, specs = [], []
    for kind in outs:
        if kind == "rows":
            shapes.append(jax.ShapeDtypeStruct((tokens, width), BF16))
            specs.append(row_spec)
        else:
            shapes.append(jax.ShapeDtypeStruct((kind // LANES, tokens, LANES), BF16))
            specs.append(pl.BlockSpec((kind // LANES, TOK_TILE, LANES), lambda i, order: (0, i, 0)))
    n_weights = len(w_in) + len(w_out)
    moved = 2 * (2 * width * hidden_size + tokens * width * len(rows) + sum(s.size for s in shapes))
    return pl.pallas_call(
        functools.partial(kernel, (w_in, w_out)),
        grid_spec=pltpu.PrefetchScalarGridSpec(
            num_scalar_prefetch=1,
            grid=(tokens // TOK_TILE,),
            in_specs=[row_spec] * len(rows) + [pl.BlockSpec(memory_space=pl.ANY)] * n_weights,
            out_specs=specs,
            scratch_shapes=[
                pltpu.VMEM((blocks_f, width, LANES), BF16),
                pltpu.VMEM((blocks_d, hidden_size, LANES), BF16),
                pltpu.SemaphoreType.DMA((SHARDS,)),
            ],
        ),
        out_shape=shapes,
        compiler_params=pltpu.CompilerParams(vmem_limit_bytes=VMEM_LIMIT),
        cost_estimate=pl.CostEstimate(flops=flops * 2 * tokens * width * hidden_size, bytes_accessed=moved, transcendentals=0),
        name=name,
    )(order, *rows, *w_in.arrays, *w_out.arrays)


def weight_grad_kernel(dy_lanes, half_ref, left_ref, right_ref, *refs):
    out_ref = refs[-1]
    left = lane_join(left_ref, 0, left_ref.shape[0])
    right = right_ref[...] if not dy_lanes else lane_join(right_ref, 0, right_ref.shape[0])
    total = lax.dot_general(left, right, FIRST_FIRST, preferred_element_type=F32)
    if len(refs) == 2:
        total = total + refs[0][...]
    out_ref[...] = total


def grad_w_out_half(half, hidden, dy, arrived):
    blocks_f, tokens, _ = hidden.shape
    width = dy.shape[1]
    per_shard = blocks_f // SHARDS
    hidden = hidden.reshape(CHIPS, 2, per_shard, tokens, LANES)
    out_spec = pl.BlockSpec((per_shard * LANES, width), lambda i, half: (i, 0))
    extra = [] if arrived is None else [arrived]
    return pl.pallas_call(
        functools.partial(weight_grad_kernel, False),
        grid_spec=pltpu.PrefetchScalarGridSpec(
            num_scalar_prefetch=1,
            grid=(CHIPS,),
            in_specs=[
                pl.BlockSpec((None, None, per_shard, tokens, LANES), lambda i, half: (i, half[0], 0, 0, 0)),
                pl.BlockSpec((tokens, width), lambda i, half: (0, 0), pipeline_mode=pl.Buffered(1)),
            ]
            + [out_spec] * len(extra),
            out_specs=out_spec,
        ),
        out_shape=jax.ShapeDtypeStruct((CHIPS * per_shard * LANES, width), F32),
        compiler_params=pltpu.CompilerParams(vmem_limit_bytes=VMEM_LIMIT),
        cost_estimate=pl.CostEstimate(
            flops=2 * tokens * width * CHIPS * per_shard * LANES,
            bytes_accessed=tokens * (blocks_f * LANES + 2 * width) + 2 * blocks_f * LANES * width * (1 + len(extra)),
            transcendentals=0,
        ),
        name="grad_w_out_half",
    )(half, hidden, dy, *extra)


def grad_w_in_half(half, unit, dpre, arrived):
    blocks_d, tokens, _ = unit.shape
    blocks_f = dpre.shape[0]
    per_shard = blocks_d // SHARDS
    step = 4
    unit = unit.reshape(CHIPS, 2, tokens, LANES)
    rows = CHIPS * per_shard * LANES
    out_spec = pl.BlockSpec((rows, step * LANES), lambda i, half: (0, i))
    extra = [] if arrived is None else [arrived]
    return pl.pallas_call(
        functools.partial(weight_grad_kernel, True),
        grid_spec=pltpu.PrefetchScalarGridSpec(
            num_scalar_prefetch=1,
            grid=(blocks_f // step,),
            in_specs=[
                pl.BlockSpec((CHIPS, None, tokens, LANES), lambda i, half: (0, half[0], 0, 0), pipeline_mode=pl.Buffered(1)),
                pl.BlockSpec((step, tokens, LANES), lambda i, half: (i, 0, 0)),
            ]
            + [out_spec] * len(extra),
            out_specs=out_spec,
        ),
        out_shape=jax.ShapeDtypeStruct((rows, blocks_f * LANES), F32),
        compiler_params=pltpu.CompilerParams(vmem_limit_bytes=VMEM_LIMIT),
        cost_estimate=pl.CostEstimate(
            flops=2 * tokens * rows * blocks_f * LANES,
            bytes_accessed=2 * tokens * (blocks_f * LANES + rows) + 4 * blocks_f * LANES * rows * (1 + len(extra)),
            transcendentals=0,
        ),
        name="grad_w_in_half",
    )(half, unit, dpre, *extra)


def to_lanes(w):
    rows, columns = w.shape
    return w.reshape(rows, columns // LANES, LANES).transpose(1, 0, 2)


def solution(mesh):
    row_spec = P(("local", "data"), None)
    weight_spec = P(None, ("local", "data"), None)
    swap_cores = [(0, 1), (1, 0)]
    swap_x = [(i, i ^ 1) for i in range(CHIPS)]
    swap_y = [(i, i ^ 2) for i in range(CHIPS)]

    def device_step(x_rows, grad_rows, w_in_part, w_out_part):
        layers = w_in_part.shape[0]
        core = lax.axis_index("data").astype(jnp.int32)
        chip = lax.axis_index("local").astype(jnp.int32)
        chip_x, chip_y = chip % 2, chip // 2
        mine, other = jnp.reshape(core, (1,)), jnp.reshape(1 - core, (1,))

        seq = [2 * (i // 2) + (core if i % 2 == 0 else 1 - core) for i in range(SHARDS)]
        order_fwd = jnp.stack([jnp.stack(seq), jnp.stack(seq)]).astype(jnp.int32)
        fwd_list = [(i % 2, i // 2) for i in range(SHARDS)]
        bwd_list = [(0, 0), (0, 1), (2, 0), (2, 1), (1, 0), (1, 1), (3, 0), (3, 1)]
        in_chips = [2 * chip_y, 2 * chip_y + 1, 2 - 2 * chip_y, 3 - 2 * chip_y]
        out_chips = [chip_x, chip_x + 2, 1 - chip_x, 3 - chip_x]

        def bwd_seq(chips):
            kept, got = chips[:2], chips[2:]
            return jnp.stack(
                [2 * c + core for c in kept] + [2 * c + 1 - core for c in kept] + [2 * c + core for c in got] + [2 * c + 1 - core for c in got]
            )

        order_bwd = jnp.stack([bwd_seq(in_chips), bwd_seq(out_chips)]).astype(jnp.int32)

        saved_x, kept_in, kept_out = [], [], []
        x_cur = x_rows
        for n in range(layers):
            half_in = lax.all_gather(to_lanes(w_in_part[n]), "local")
            half_out = lax.all_gather(to_lanes(w_out_part[n]), "local")
            twin_in = lax.ppermute(half_in, "data", swap_cores)
            twin_out = lax.ppermute(half_out, "data", swap_cores)
            saved_x.append(x_cur)
            keep_in = lax.dynamic_slice_in_dim(half_in, 2 * chip_y, 2, 0)
            pair_out = half_out.reshape((2, 2) + half_out.shape[1:])
            keep_out = lax.dynamic_slice_in_dim(pair_out, chip_x, 1, 1)[:, 0]
            (x_next,) = layer_call(
                forward_kernel, "layer_forward", order_fwd, [x_cur], Pieces([half_in, twin_in], fwd_list), Pieces([half_out, twin_out], fwd_list), ["rows"], 2
            )
            x_cur, keep_in, keep_out = lax.optimization_barrier((x_next, keep_in, keep_out))
            kept_in.append(keep_in)
            kept_out.append(keep_out)

        grad_cur = grad_rows
        grads_in, grads_out = [], []
        for n in reversed(range(layers)):
            keep_in, keep_out, grad_here = lax.optimization_barrier((kept_in[n], kept_out[n], grad_cur))
            got_in = lax.ppermute(keep_in, "local", swap_y)
            got_out = lax.ppermute(keep_out, "local", swap_x)
            twin_in = lax.ppermute(keep_in, "data", swap_cores)
            twin_out = lax.ppermute(keep_out, "data", swap_cores)
            twin_got_in = lax.ppermute(got_in, "data", swap_cores)
            twin_got_out = lax.ppermute(got_out, "data", swap_cores)
            if grads_in:
                grad_here, grads_in[-1], grads_out[-1] = lax.optimization_barrier((grad_here, grads_in[-1], grads_out[-1]))
                reduce(grads_in, grads_out)
            unit, hidden, dpre, grad_cur = layer_call(
                backward_kernel,
                "layer_backward",
                order_bwd,
                [saved_x[n], grad_here],
                Pieces([keep_in, got_in, twin_in, twin_got_in], bwd_list),
                Pieces([keep_out, got_out, twin_out, twin_got_out], bwd_list),
                [x_rows.shape[1], w_out_part.shape[1] * SHARDS, w_out_part.shape[1] * SHARDS, "rows"],
                3,
            )
            out_there = grad_w_out_half(other, hidden, grad_here, None)
            out_arrived = lax.ppermute(out_there, "data", swap_cores)
            in_there = grad_w_in_half(other, unit, dpre, None)
            in_arrived = lax.ppermute(in_there, "data", swap_cores)
            grads_out.append(grad_w_out_half(mine, hidden, grad_here, out_arrived))
            grads_in.append(grad_w_in_half(mine, unit, dpre, in_arrived))
        reduce(grads_in, grads_out)
        return x_cur, jnp.stack(grads_in[::-1]), jnp.stack(grads_out[::-1]), grad_cur

    def reduce(grads_in, grads_out):
        grads_out[-1] = lax.psum_scatter(grads_out[-1], "local", scatter_dimension=0, tiled=True)
        grads_in[-1] = lax.psum_scatter(grads_in[-1], "local", scatter_dimension=0, tiled=True)

    return jax.shard_map(
        device_step,
        mesh=mesh,
        in_specs=(row_spec, row_spec, weight_spec, weight_spec),
        out_specs=(row_spec, weight_spec, weight_spec, row_spec),
        check_vma=False,
    )
```

```python
import functools

import jax
import jax.numpy as jnp
from jax import lax
from jax.experimental import pallas as pl
from jax.experimental.pallas import tpu as pltpu
from jax.sharding import PartitionSpec as P


NORM_EPS = 1e-6
GELU_A = 0.7978845608028654
GELU_B = GELU_A * 0.044715
LAST_LAST = (((1,), (1,)), ((), ()))
FIRST_FIRST = (((0,), (0,)), ((), ()))
BF16 = jnp.bfloat16
F32 = jnp.float32

CHIPS = 4
SHARDS = 8
LANES = 128
TOK_TILE = 256
CHUNK = 256
VMEM_LIMIT = 60 * 1024 * 1024


def unit_rows_of(x_tile):
    x_wide = x_tile.astype(F32)
    inv_rms = lax.rsqrt(jnp.mean(x_wide * x_wide, axis=-1, keepdims=True) + NORM_EPS)
    return x_wide, inv_rms


def lane_join(ref, first, count, rows=None):
    if rows is None:
        return jnp.concatenate([ref[first + b] for b in range(count)], axis=1)
    return jnp.concatenate([ref[first + b, rows, :] for b in range(count)], axis=1)


def weight_copies(order_ref, w_in_pieces, w_out_pieces, w_in_buf, w_out_buf, sem):
    hidden_blocks = w_in_buf.shape[0] // SHARDS
    depth = w_in_buf.shape[1] // SHARDS
    width = w_out_buf.shape[1] // SHARDS
    groups = []
    for p in range(SHARDS):
        block = order_ref[1, p] * hidden_blocks
        copies = []
        for q, (ref, at) in enumerate(w_in_pieces):
            row = pl.multiple_of(order_ref[0, q] * depth, depth)
            copies.append(
                pltpu.make_async_copy(
                    ref.at[at, pl.ds(block, hidden_blocks)],
                    w_in_buf.at[pl.ds(p * hidden_blocks, hidden_blocks), pl.ds(row, depth)],
                    sem.at[p],
                )
            )
        ref, at = w_out_pieces[p]
        copies.append(pltpu.make_async_copy(ref.at[at], w_out_buf.at[:, pl.ds(p * width, width)], sem.at[p]))
        groups.append(copies)
    return groups


def with_weights(order_ref, w_in_pieces, w_out_pieces, w_in_buf, w_out_buf, sem, body):
    step = pl.program_id(0)

    @pl.when(step == 0)
    def _():
        groups = weight_copies(order_ref, w_in_pieces, w_out_pieces, w_in_buf, w_out_buf, sem)
        for copies in groups:
            for copy in copies:
                copy.start()

        def wait(p):
            for copy in groups[p]:
                copy.wait()

        body(wait)

    @pl.when(step > 0)
    def _():
        body(lambda p: None)


def forward_kernel(pieces, order_ref, x_ref, *refs):
    n_in, n_out = len(pieces[0]), len(pieces[1])
    w_in_refs, w_out_refs = refs[:n_in], refs[n_in : n_in + n_out]
    y_ref, w_in_buf, w_out_buf, sem = refs[n_in + n_out :]
    w_in_pieces = [(w_in_refs[a], i) for a, i in piece_list(pieces[0])]
    w_out_pieces = [(w_out_refs[a], i) for a, i in piece_list(pieces[1])]
    hidden_size = w_out_buf.shape[1]
    per_group = hidden_size // SHARDS // CHUNK
    blocks = CHUNK // LANES
    d_blocks = w_out_buf.shape[0]

    def body(wait):
        x_wide, inv_rms = unit_rows_of(x_ref[...])
        unit = (x_wide * inv_rms).astype(BF16)
        total = None
        pending = []

        def finish(total):
            chunk, hidden = pending.pop(0)
            w_out = lane_join(w_out_buf, 0, d_blocks, pl.ds(chunk * CHUNK, CHUNK))
            part = jnp.dot(hidden, w_out, preferred_element_type=F32)
            return part if total is None else total + part

        for chunk in range(hidden_size // CHUNK):
            if chunk % per_group == 0:
                wait(chunk // per_group)
            w_in = lane_join(w_in_buf, chunk * blocks, blocks)
            pre = jnp.dot(unit, w_in, preferred_element_type=F32).astype(BF16).astype(F32)
            tanh = jnp.tanh(pre * (GELU_A + GELU_B * (pre * pre)))
            pending.append((chunk, (pre * (0.5 * tanh + 0.5)).astype(BF16)))
            if len(pending) > 2:
                total = finish(total)
        while pending:
            total = finish(total)
        y_ref[...] = (x_ref[...].astype(F32) + total).astype(BF16)

    with_weights(order_ref, w_in_pieces, w_out_pieces, w_in_buf, w_out_buf, sem, body)


def backward_kernel(pieces, order_ref, x_ref, dy_ref, *refs):
    n_in, n_out = len(pieces[0]), len(pieces[1])
    w_in_refs, w_out_refs = refs[:n_in], refs[n_in : n_in + n_out]
    unit_ref, hidden_ref, dpre_ref, dx_ref, w_in_buf, w_out_buf, sem = refs[n_in + n_out :]
    w_in_pieces = [(w_in_refs[a], i) for a, i in piece_list(pieces[0])]
    w_out_pieces = [(w_out_refs[a], i) for a, i in piece_list(pieces[1])]
    hidden_size = w_out_buf.shape[1]
    per_group = hidden_size // SHARDS // CHUNK
    blocks = CHUNK // LANES
    d_blocks = w_out_buf.shape[0]

    def body(wait):
        x_wide, inv_rms = unit_rows_of(x_ref[...])
        unit = (x_wide * inv_rms).astype(BF16)
        for b in range(d_blocks):
            unit_ref[b] = unit[:, b * LANES : (b + 1) * LANES]
        dy = dy_ref[...]
        total = None
        pending = []

        def finish(total):
            chunk, dpre = pending.pop(0)
            part = lax.dot_general(dpre, lane_join(w_in_buf, chunk * blocks, blocks), LAST_LAST, preferred_element_type=F32)
            return part if total is None else total + part

        for chunk in range(hidden_size // CHUNK):
            group = chunk // per_group
            if chunk % per_group == 0:
                wait(group)
            w_in = lane_join(w_in_buf, chunk * blocks, blocks)
            w_out = lane_join(w_out_buf, 0, d_blocks, pl.ds(chunk * CHUNK, CHUNK))
            pre = jnp.dot(unit, w_in, preferred_element_type=F32).astype(BF16).astype(F32)
            dhidden = lax.dot_general(dy, w_out, LAST_LAST, preferred_element_type=F32)
            poly = GELU_A + GELU_B * (pre * pre)
            cdf = 0.5 * jnp.tanh(pre * poly) + 0.5
            hidden = pre * cdf
            slope = cdf + (hidden * (6.0 * poly - 4.0 * GELU_A)) * (1.0 - cdf)
            hidden = hidden.astype(BF16)
            dpre = (slope * dhidden).astype(BF16)
            first = order_ref[1, group] * (per_group * blocks) + chunk % per_group * blocks
            for b in range(blocks):
                hidden_ref[first + b] = hidden[:, b * LANES : (b + 1) * LANES]
                dpre_ref[first + b] = dpre[:, b * LANES : (b + 1) * LANES]
            pending.append((chunk, dpre))
            if len(pending) > 2:
                total = finish(total)
        while pending:
            total = finish(total)
        value = x_ref[...].astype(F32) * inv_rms
        row_mean = jnp.mean(total * value, axis=-1, keepdims=True)
        dx_ref[...] = (dy_ref[...].astype(F32) + inv_rms * (total - value * row_mean)).astype(BF16)

    with_weights(order_ref, w_in_pieces, w_out_pieces, w_in_buf, w_out_buf, sem, body)


def piece_list(arrays):
    return [(a, i) for a, i in arrays.order]


class Pieces:
    def __init__(self, arrays, order):
        self.arrays, self.order = arrays, order

    def __len__(self):
        return len(self.arrays)


def layer_call(kernel, order, rows, w_in, w_out, outs, flops):
    tokens, width = rows[0].shape
    hidden_size = w_out.arrays[0].shape[2] * SHARDS
    blocks_d, blocks_f = width // LANES, hidden_size // LANES
    row_spec = pl.BlockSpec((TOK_TILE, width), lambda i, order: (i, 0))
    shapes, specs = [], []
    for kind in outs:
        if kind == "rows":
            shapes.append(jax.ShapeDtypeStruct((tokens, width), BF16))
            specs.append(row_spec)
        else:
            shapes.append(jax.ShapeDtypeStruct((kind // LANES, tokens, LANES), BF16))
            specs.append(pl.BlockSpec((kind // LANES, TOK_TILE, LANES), lambda i, order: (0, i, 0)))
    n_weights = len(w_in) + len(w_out)
    moved = 2 * (2 * width * hidden_size + tokens * width * len(rows) + sum(s.size for s in shapes))
    return pl.pallas_call(
        functools.partial(kernel, (w_in, w_out)),
        grid_spec=pltpu.PrefetchScalarGridSpec(
            num_scalar_prefetch=1,
            grid=(tokens // TOK_TILE,),
            in_specs=[row_spec] * len(rows) + [pl.BlockSpec(memory_space=pl.ANY)] * n_weights,
            out_specs=specs,
            scratch_shapes=[
                pltpu.VMEM((blocks_f, width, LANES), BF16),
                pltpu.VMEM((blocks_d, hidden_size, LANES), BF16),
                pltpu.SemaphoreType.DMA((SHARDS,)),
            ],
        ),
        out_shape=shapes,
        compiler_params=pltpu.CompilerParams(vmem_limit_bytes=VMEM_LIMIT),
        cost_estimate=pl.CostEstimate(flops=flops * 2 * tokens * width * hidden_size, bytes_accessed=moved, transcendentals=0),
    )(order, *rows, *w_in.arrays, *w_out.arrays)


def weight_grad_kernel(dy_lanes, half_ref, left_ref, right_ref, *refs):
    out_ref = refs[-1]
    left = lane_join(left_ref, 0, left_ref.shape[0])
    right = right_ref[...] if not dy_lanes else lane_join(right_ref, 0, right_ref.shape[0])
    total = lax.dot_general(left, right, FIRST_FIRST, preferred_element_type=F32)
    if len(refs) == 2:
        total = total + refs[0][...]
    out_ref[...] = total


def grad_w_out_half(half, hidden, dy, arrived):
    blocks_f, tokens, _ = hidden.shape
    width = dy.shape[1]
    per_shard = blocks_f // SHARDS
    hidden = hidden.reshape(CHIPS, 2, per_shard, tokens, LANES)
    out_spec = pl.BlockSpec((per_shard * LANES, width), lambda i, half: (i, 0))
    extra = [] if arrived is None else [arrived]
    return pl.pallas_call(
        functools.partial(weight_grad_kernel, False),
        grid_spec=pltpu.PrefetchScalarGridSpec(
            num_scalar_prefetch=1,
            grid=(CHIPS,),
            in_specs=[
                pl.BlockSpec((None, None, per_shard, tokens, LANES), lambda i, half: (i, half[0], 0, 0, 0)),
                pl.BlockSpec((tokens, width), lambda i, half: (0, 0), pipeline_mode=pl.Buffered(1)),
            ]
            + [out_spec] * len(extra),
            out_specs=out_spec,
        ),
        out_shape=jax.ShapeDtypeStruct((CHIPS * per_shard * LANES, width), F32),
        compiler_params=pltpu.CompilerParams(vmem_limit_bytes=VMEM_LIMIT),
        cost_estimate=pl.CostEstimate(
            flops=2 * tokens * width * CHIPS * per_shard * LANES,
            bytes_accessed=tokens * (blocks_f * LANES + 2 * width) + 2 * blocks_f * LANES * width * (1 + len(extra)),
            transcendentals=0,
        ),
        name="grad_w_out_half",
    )(half, hidden, dy, *extra)


def grad_w_in_half(half, unit, dpre, arrived):
    blocks_d, tokens, _ = unit.shape
    blocks_f = dpre.shape[0]
    per_shard = blocks_d // SHARDS
    step = 4
    unit = unit.reshape(CHIPS, 2, tokens, LANES)
    rows = CHIPS * per_shard * LANES
    out_spec = pl.BlockSpec((rows, step * LANES), lambda i, half: (0, i))
    extra = [] if arrived is None else [arrived]
    return pl.pallas_call(
        functools.partial(weight_grad_kernel, True),
        grid_spec=pltpu.PrefetchScalarGridSpec(
            num_scalar_prefetch=1,
            grid=(blocks_f // step,),
            in_specs=[
                pl.BlockSpec((CHIPS, None, tokens, LANES), lambda i, half: (0, half[0], 0, 0), pipeline_mode=pl.Buffered(1)),
                pl.BlockSpec((step, tokens, LANES), lambda i, half: (i, 0, 0)),
            ]
            + [out_spec] * len(extra),
            out_specs=out_spec,
        ),
        out_shape=jax.ShapeDtypeStruct((rows, blocks_f * LANES), F32),
        compiler_params=pltpu.CompilerParams(vmem_limit_bytes=VMEM_LIMIT),
        cost_estimate=pl.CostEstimate(
            flops=2 * tokens * rows * blocks_f * LANES,
            bytes_accessed=2 * tokens * (blocks_f * LANES + rows) + 4 * blocks_f * LANES * rows * (1 + len(extra)),
            transcendentals=0,
        ),
        name="grad_w_in_half",
    )(half, unit, dpre, *extra)


def to_lanes(w):
    rows, columns = w.shape
    return w.reshape(rows, columns // LANES, LANES).transpose(1, 0, 2)


def solution(mesh):
    row_spec = P(("local", "data"), None)
    weight_spec = P(None, ("local", "data"), None)
    swap_cores = [(0, 1), (1, 0)]
    swap_x = [(i, i ^ 1) for i in range(CHIPS)]
    swap_y = [(i, i ^ 2) for i in range(CHIPS)]

    def device_step(x_rows, grad_rows, w_in_part, w_out_part):
        layers = w_in_part.shape[0]
        core = lax.axis_index("data").astype(jnp.int32)
        chip = lax.axis_index("local").astype(jnp.int32)
        chip_x, chip_y = chip % 2, chip // 2
        mine, other = jnp.reshape(core, (1,)), jnp.reshape(1 - core, (1,))

        seq = [2 * (i // 2) + (core if i % 2 == 0 else 1 - core) for i in range(SHARDS)]
        order_fwd = jnp.stack([jnp.stack(seq), jnp.stack(seq)]).astype(jnp.int32)
        fwd_list = [(i % 2, i // 2) for i in range(SHARDS)]
        bwd_list = [(0, 0), (0, 1), (2, 0), (2, 1), (1, 0), (1, 1), (3, 0), (3, 1)]
        in_chips = [2 * chip_y, 2 * chip_y + 1, 2 - 2 * chip_y, 3 - 2 * chip_y]
        out_chips = [chip_x, chip_x + 2, 1 - chip_x, 3 - chip_x]

        def bwd_seq(chips):
            kept, got = chips[:2], chips[2:]
            return jnp.stack(
                [2 * c + core for c in kept] + [2 * c + 1 - core for c in kept] + [2 * c + core for c in got] + [2 * c + 1 - core for c in got]
            )

        order_bwd = jnp.stack([bwd_seq(in_chips), bwd_seq(out_chips)]).astype(jnp.int32)

        def gather(n, after):
            own_in, own_out = to_lanes(w_in_part[n]), to_lanes(w_out_part[n])
            if after is not None:
                own_in, own_out, _ = lax.optimization_barrier((own_in, own_out, after))
            half_in = lax.all_gather(own_in, "local")
            half_out = lax.all_gather(own_out, "local")
            return half_in, half_out

        saved_x, kept_in, kept_out = [], [], []
        x_cur = x_rows
        halves = gather(0, None)
        for n in range(layers):
            half_in, half_out = halves
            twin_in = lax.ppermute(half_in, "data", swap_cores)
            twin_out = lax.ppermute(half_out, "data", swap_cores)
            saved_x.append(x_cur)
            if n + 1 < layers:
                halves = gather(n + 1, half_in)
            keep_in = lax.dynamic_slice_in_dim(half_in, 2 * chip_y, 2, 0)
            pair_out = half_out.reshape((2, 2) + half_out.shape[1:])
            keep_out = lax.dynamic_slice_in_dim(pair_out, chip_x, 1, 1)[:, 0]
            (x_next,) = layer_call(
                forward_kernel, order_fwd, [x_cur], Pieces([half_in, twin_in], fwd_list), Pieces([half_out, twin_out], fwd_list), ["rows"], 2
            )
            x_cur, keep_in, keep_out = lax.optimization_barrier((x_next, keep_in, keep_out))
            kept_in.append(keep_in)
            kept_out.append(keep_out)

        def exchange(n, grad_cur):
            keep_in, keep_out, grad_cur = lax.optimization_barrier((kept_in[n], kept_out[n], grad_cur))
            got_in = lax.ppermute(keep_in, "local", swap_y)
            got_out = lax.ppermute(keep_out, "local", swap_x)
            twin_in = lax.ppermute(keep_in, "data", swap_cores)
            twin_out = lax.ppermute(keep_out, "data", swap_cores)
            return [keep_in, got_in, twin_in], [keep_out, got_out, twin_out], grad_cur

        def swap_got(in_arrays, out_arrays):
            in_arrays.append(lax.ppermute(in_arrays[1], "data", swap_cores))
            out_arrays.append(lax.ppermute(out_arrays[1], "data", swap_cores))

        grad_cur = grad_rows
        grads_in, grads_out = [None] * layers, [None] * layers
        in_arrays, out_arrays, grad_cur = exchange(layers - 1, grad_cur)
        swap_got(in_arrays, out_arrays)
        for n in reversed(range(layers)):
            if n + 1 < layers:
                reduce(grads_in, grads_out, n + 1)
            unit, hidden, dpre, grad_next = layer_call(
                backward_kernel,
                order_bwd,
                [saved_x[n], grad_cur],
                Pieces(in_arrays, bwd_list),
                Pieces(out_arrays, bwd_list),
                [x_rows.shape[1], w_out_part.shape[1] * SHARDS, w_out_part.shape[1] * SHARDS, "rows"],
                3,
            )
            if n > 0:
                in_arrays, out_arrays, grad_next = exchange(n - 1, grad_next)
            out_there = grad_w_out_half(other, hidden, grad_cur, None)
            out_arrived = lax.ppermute(out_there, "data", swap_cores)
            in_there = grad_w_in_half(other, unit, dpre, None)
            in_arrived = lax.ppermute(in_there, "data", swap_cores)
            grad_out_half = grad_w_out_half(mine, hidden, grad_cur, out_arrived)
            if n > 0:
                in_arrays[1], out_arrays[1], grad_out_half = lax.optimization_barrier((in_arrays[1], out_arrays[1], grad_out_half))
                swap_got(in_arrays, out_arrays)
            grad_in_half = grad_w_in_half(mine, unit, dpre, in_arrived)
            if n > 0:
                grad_next, grad_out_half, grad_in_half = lax.optimization_barrier((grad_next, grad_out_half, grad_in_half))
            grads_in[n], grads_out[n], grad_cur = grad_in_half, grad_out_half, grad_next
        reduce(grads_in, grads_out, 0)
        return x_cur, jnp.stack(grads_in), jnp.stack(grads_out), grad_cur

    def reduce(grads_in, grads_out, n):
        grads_out[n] = lax.psum_scatter(grads_out[n], "local", scatter_dimension=0, tiled=True)
        grads_in[n] = lax.psum_scatter(grads_in[n], "local", scatter_dimension=0, tiled=True)

    return jax.shard_map(
        device_step,
        mesh=mesh,
        in_specs=(row_spec, row_spec, weight_spec, weight_spec),
        out_specs=(row_spec, weight_spec, weight_spec, row_spec),
        check_vma=False,
    )
```

```python
import functools

import jax
import jax.numpy as jnp
from jax import lax
from jax.experimental import pallas as pl
from jax.experimental.pallas import tpu as pltpu
from jax.sharding import PartitionSpec as P


NORM_EPS = 1e-6
GELU_A = 0.7978845608028654
GELU_B = GELU_A * 0.044715
LAST_LAST = (((1,), (1,)), ((), ()))
FIRST_FIRST = (((0,), (0,)), ((), ()))
BF16 = jnp.bfloat16
F32 = jnp.float32

CHIPS = 4
SHARDS = 8
LANES = 128
TOK_TILE = 256
CHUNK = 256
VMEM_LIMIT = 60 * 1024 * 1024
MESH = pl.DeviceIdType.MESH


def unit_rows_of(x_tile):
    x_wide = x_tile.astype(F32)
    inv_rms = lax.rsqrt(jnp.mean(x_wide * x_wide, axis=-1, keepdims=True) + NORM_EPS)
    return x_wide, inv_rms


def lane_join(ref, first, count, rows=None):
    if rows is None:
        return jnp.concatenate([ref[first + b] for b in range(count)], axis=1)
    return jnp.concatenate([ref[first + b, rows, :] for b in range(count)], axis=1)


def weight_copies(order_ref, w_in_pieces, w_out_pieces, w_in_buf, w_out_buf, sem):
    hidden_blocks = w_in_buf.shape[0] // SHARDS
    depth = w_in_buf.shape[1] // SHARDS
    width = w_out_buf.shape[1] // SHARDS
    groups = []
    for p in range(SHARDS):
        block = order_ref[1, p] * hidden_blocks
        copies = []
        for q, (ref, at) in enumerate(w_in_pieces):
            row = pl.multiple_of(order_ref[0, q] * depth, depth)
            copies.append(
                pltpu.make_async_copy(
                    ref.at[at, pl.ds(block, hidden_blocks)],
                    w_in_buf.at[pl.ds(p * hidden_blocks, hidden_blocks), pl.ds(row, depth)],
                    sem.at[p],
                )
            )
        ref, at = w_out_pieces[p]
        copies.append(pltpu.make_async_copy(ref.at[at], w_out_buf.at[:, pl.ds(p * width, width)], sem.at[p]))
        groups.append(copies)
    return groups


def with_weights(order_ref, w_in_pieces, w_out_pieces, w_in_buf, w_out_buf, sem, body):
    step = pl.program_id(0)

    @pl.when(step == 0)
    def _():
        groups = weight_copies(order_ref, w_in_pieces, w_out_pieces, w_in_buf, w_out_buf, sem)
        for copies in groups:
            for copy in copies:
                copy.start()

        def wait(p):
            for copy in groups[p]:
                copy.wait()

        body(wait)

    @pl.when(step > 0)
    def _():
        body(lambda p: None)


def backward_kernel(pieces, order_ref, x_ref, dy_ref, *refs):
    n_in, n_out = len(pieces[0]), len(pieces[1])
    w_in_refs, w_out_refs = refs[:n_in], refs[n_in : n_in + n_out]
    unit_ref, hidden_ref, dpre_ref, dx_ref, w_in_buf, w_out_buf, sem = refs[n_in + n_out :]
    w_in_pieces = [(w_in_refs[a], i) for a, i in piece_list(pieces[0])]
    w_out_pieces = [(w_out_refs[a], i) for a, i in piece_list(pieces[1])]
    hidden_size = w_out_buf.shape[1]
    per_group = hidden_size // SHARDS // CHUNK
    blocks = CHUNK // LANES
    d_blocks = w_out_buf.shape[0]

    def body(wait):
        x_wide, inv_rms = unit_rows_of(x_ref[...])
        unit = (x_wide * inv_rms).astype(BF16)
        for b in range(d_blocks):
            unit_ref[b] = unit[:, b * LANES : (b + 1) * LANES]
        dy = dy_ref[...]
        total = None
        pending = []

        def finish(total):
            chunk, dpre = pending.pop(0)
            part = lax.dot_general(dpre, lane_join(w_in_buf, chunk * blocks, blocks), LAST_LAST, preferred_element_type=F32)
            return part if total is None else total + part

        for chunk in range(hidden_size // CHUNK):
            group = chunk // per_group
            if chunk % per_group == 0:
                wait(group)
            w_in = lane_join(w_in_buf, chunk * blocks, blocks)
            w_out = lane_join(w_out_buf, 0, d_blocks, pl.ds(chunk * CHUNK, CHUNK))
            pre = jnp.dot(unit, w_in, preferred_element_type=F32).astype(BF16).astype(F32)
            dhidden = lax.dot_general(dy, w_out, LAST_LAST, preferred_element_type=F32)
            poly = GELU_A + GELU_B * (pre * pre)
            cdf = 0.5 * jnp.tanh(pre * poly) + 0.5
            hidden = pre * cdf
            slope = cdf + (hidden * (6.0 * poly - 4.0 * GELU_A)) * (1.0 - cdf)
            hidden = hidden.astype(BF16)
            dpre = (slope * dhidden).astype(BF16)
            first = order_ref[1, group] * (per_group * blocks) + chunk % per_group * blocks
            for b in range(blocks):
                hidden_ref[first + b] = hidden[:, b * LANES : (b + 1) * LANES]
                dpre_ref[first + b] = dpre[:, b * LANES : (b + 1) * LANES]
            pending.append((chunk, dpre))
            if len(pending) > 2:
                total = finish(total)
        while pending:
            total = finish(total)
        value = x_ref[...].astype(F32) * inv_rms
        row_mean = jnp.mean(total * value, axis=-1, keepdims=True)
        dx_ref[...] = (dy_ref[...].astype(F32) + inv_rms * (total - value * row_mean)).astype(BF16)

    with_weights(order_ref, w_in_pieces, w_out_pieces, w_in_buf, w_out_buf, sem, body)


def piece_list(arrays):
    return [(a, i) for a, i in arrays.order]


class Pieces:
    def __init__(self, arrays, order):
        self.arrays, self.order = arrays, order

    def __len__(self):
        return len(self.arrays)


def layer_call(kernel, order, rows, w_in, w_out, outs, flops):
    tokens, width = rows[0][0].shape[1:]
    hidden_size = w_out.arrays[0].shape[2] * SHARDS
    blocks_d, blocks_f = width // LANES, hidden_size // LANES
    row_spec = pl.BlockSpec((TOK_TILE, width), lambda i, order: (i, 0))
    shapes, specs = [], []
    for kind in outs:
        if kind == "rows":
            shapes.append(jax.ShapeDtypeStruct((tokens, width), BF16))
            specs.append(row_spec)
        else:
            shapes.append(jax.ShapeDtypeStruct((kind // LANES, tokens, LANES), BF16))
            specs.append(pl.BlockSpec((kind // LANES, TOK_TILE, LANES), lambda i, order: (0, i, 0)))
    n_weights = len(w_in) + len(w_out)
    moved = 2 * (2 * width * hidden_size + tokens * width * len(rows) + sum(s.size for s in shapes))
    return pl.pallas_call(
        functools.partial(kernel, (w_in, w_out)),
        grid_spec=pltpu.PrefetchScalarGridSpec(
            num_scalar_prefetch=1,
            grid=(tokens // TOK_TILE,),
            in_specs=[pl.BlockSpec((None, TOK_TILE, width), lambda i, order, at=at: (at, i, 0)) for _, at in rows]
            + [pl.BlockSpec(memory_space=pl.ANY)] * n_weights,
            out_specs=specs,
            scratch_shapes=[
                pltpu.VMEM((blocks_f, width, LANES), BF16),
                pltpu.VMEM((blocks_d, hidden_size, LANES), BF16),
                pltpu.SemaphoreType.DMA((SHARDS,)),
            ],
        ),
        out_shape=shapes,
        compiler_params=pltpu.CompilerParams(vmem_limit_bytes=VMEM_LIMIT),
        cost_estimate=pl.CostEstimate(flops=flops * 2 * tokens * width * hidden_size, bytes_accessed=moved, transcendentals=0),
    )(order, *[array for array, _ in rows], *w_in.arrays, *w_out.arrays)


def weight_grad_kernel(dy_lanes, half_ref, left_ref, right_ref, *refs):
    out_ref = refs[-1]
    left = lane_join(left_ref, 0, left_ref.shape[0])
    right = right_ref[...] if not dy_lanes else lane_join(right_ref, 0, right_ref.shape[0])
    total = lax.dot_general(left, right, FIRST_FIRST, preferred_element_type=F32)
    if len(refs) == 2:
        total = total + refs[0][...]
    out_ref[...] = total


def grad_w_out_half(half, hidden, dy, arrived):
    blocks_f, tokens, _ = hidden.shape
    width = dy.shape[1]
    per_shard = blocks_f // SHARDS
    hidden = hidden.reshape(CHIPS, 2, per_shard, tokens, LANES)
    out_spec = pl.BlockSpec((per_shard * LANES, width), lambda i, half: (i, 0))
    extra = [] if arrived is None else [arrived]
    return pl.pallas_call(
        functools.partial(weight_grad_kernel, False),
        grid_spec=pltpu.PrefetchScalarGridSpec(
            num_scalar_prefetch=1,
            grid=(CHIPS,),
            in_specs=[
                pl.BlockSpec((None, None, per_shard, tokens, LANES), lambda i, half: (i, half[0], 0, 0, 0)),
                pl.BlockSpec((tokens, width), lambda i, half: (0, 0), pipeline_mode=pl.Buffered(1)),
            ]
            + [out_spec] * len(extra),
            out_specs=out_spec,
        ),
        out_shape=jax.ShapeDtypeStruct((CHIPS * per_shard * LANES, width), F32),
        compiler_params=pltpu.CompilerParams(vmem_limit_bytes=VMEM_LIMIT),
        cost_estimate=pl.CostEstimate(
            flops=2 * tokens * width * CHIPS * per_shard * LANES,
            bytes_accessed=tokens * (blocks_f * LANES + 2 * width) + 2 * blocks_f * LANES * width * (1 + len(extra)),
            transcendentals=0,
        ),
        name="grad_w_out_half",
    )(half, hidden, dy, *extra)


def grad_w_in_half(half, unit, dpre, arrived):
    blocks_d, tokens, _ = unit.shape
    blocks_f = dpre.shape[0]
    per_shard = blocks_d // SHARDS
    step = 4
    unit = unit.reshape(CHIPS, 2, tokens, LANES)
    rows = CHIPS * per_shard * LANES
    out_spec = pl.BlockSpec((rows, step * LANES), lambda i, half: (0, i))
    extra = [] if arrived is None else [arrived]
    return pl.pallas_call(
        functools.partial(weight_grad_kernel, True),
        grid_spec=pltpu.PrefetchScalarGridSpec(
            num_scalar_prefetch=1,
            grid=(blocks_f // step,),
            in_specs=[
                pl.BlockSpec((CHIPS, None, tokens, LANES), lambda i, half: (0, half[0], 0, 0), pipeline_mode=pl.Buffered(1)),
                pl.BlockSpec((step, tokens, LANES), lambda i, half: (i, 0, 0)),
            ]
            + [out_spec] * len(extra),
            out_specs=out_spec,
        ),
        out_shape=jax.ShapeDtypeStruct((rows, blocks_f * LANES), F32),
        compiler_params=pltpu.CompilerParams(vmem_limit_bytes=VMEM_LIMIT),
        cost_estimate=pl.CostEstimate(
            flops=2 * tokens * rows * blocks_f * LANES,
            bytes_accessed=2 * tokens * (blocks_f * LANES + rows) + 4 * blocks_f * LANES * rows * (1 + len(extra)),
            transcendentals=0,
        ),
        name="grad_w_in_half",
    )(half, unit, dpre, *extra)


class Place:
    def __init__(self):
        self.chip = lax.axis_index("local")
        self.core = lax.axis_index("data")
        self.chip_x, self.chip_y = lax.rem(self.chip, 2), lax.div(self.chip, 2)

    def chip_at(self, mask):
        mask_x, mask_y = (mask % 2, mask // 2) if isinstance(mask, int) else (lax.rem(mask, 2), lax.div(mask, 2))
        return lax.rem(self.chip_x + mask_x, 2) + 2 * lax.rem(self.chip_y + mask_y, 2)

    def across(self, mask):
        return (self.chip_at(mask), self.core)

    def twin(self):
        return (self.chip, 1 - self.core)

    def peers(self):
        return [self.across(1), self.across(2), self.across(3), self.twin()]


def meet(place):
    barrier = pltpu.get_barrier_semaphore()
    for device in place.peers():
        pl.semaphore_signal(barrier, inc=1, device_id=device, device_id_type=MESH)
    pl.semaphore_wait(barrier, 4)


def remote(src, dst, send_sem, recv_sem, device):
    return pltpu.make_async_remote_copy(
        src_ref=src, dst_ref=dst, send_sem=send_sem, recv_sem=recv_sem, device_id=device, device_id_type=MESH
    )


class Stream:
    def __init__(self, place, own_in, own_out, kept_in, kept_out, got_in, got_out, twin_in, twin_out, sems):
        self.place = place
        self.own_in, self.own_out, self.kept_in, self.kept_out = own_in, own_out, kept_in, kept_out
        self.got_in, self.got_out, self.twin_in, self.twin_out = got_in, got_out, twin_in, twin_out
        (self.in_send, self.in_recv, self.out_send, self.out_recv) = sems[:4]
        (self.twin_in_send, self.twin_in_recv, self.twin_out_send, self.twin_out_recv) = sems[4:]
        self.blocks = own_in.shape[1] // CHIPS

    def mine_in(self, n, mask, block, count):
        slot, rows = lax.rem(n, 2), pl.ds(block, count)
        if mask == 0:
            return self.own_in.at[n, rows]
        if mask == 1:
            return self.kept_in.at[n, rows]
        return self.got_in.at[slot, mask - 2, rows]

    def mine_out(self, n, mask):
        slot = lax.rem(n, 2)
        if mask == 0:
            return self.own_out.at[n]
        if mask == 2:
            return self.kept_out.at[n]
        return self.got_out.at[slot, (mask - 1) // 2]

    def push_in(self, n, mask, unit, block):
        src = self.own_in.at[n, pl.ds(block, self.blocks)]
        dst = self.mine_in(n, mask, block, self.blocks)
        recv = self.in_recv.at[lax.rem(n, 2), mask - 1, unit]
        return remote(src, dst, self.in_send.at[mask - 1, unit], recv, self.place.across(mask))

    def push_out(self, n, mask):
        recv = self.out_recv.at[lax.rem(n, 2), mask - 1]
        return remote(self.own_out.at[n], self.mine_out(n, mask), self.out_send.at[mask - 1], recv, self.place.across(mask))

    def pushes(self, n):
        copies = []
        for unit in range(CHIPS):
            for mask in (1, 2, 3):
                copies.append(self.push_in(n, mask, unit, self.place.chip_at(mask ^ unit) * self.blocks))
            if unit:
                copies.append(self.push_out(n, unit))
        return copies

    def push(self, n):
        for copy in self.pushes(n):
            copy.start()

    def push_sent(self, n):
        for copy in self.pushes(n):
            copy.wait_send()

    def twin_copies(self, n, unit):
        slot, block = lax.rem(n, 2), self.place.chip_at(unit) * self.blocks
        return [
            remote(
                self.mine_in(n, mask, block, self.blocks),
                self.twin_in.at[slot, mask, pl.ds(block, self.blocks)],
                self.twin_in_send.at[mask, unit],
                self.twin_in_recv.at[slot, mask, unit],
                self.place.twin(),
            )
            for mask in range(CHIPS)
        ]

    def twin_out_copy(self, n, mask, unit):
        slot = lax.rem(n, 2)
        return remote(
            self.mine_out(n, mask),
            self.twin_out.at[slot, unit],
            self.twin_out_send.at[unit],
            self.twin_out_recv.at[slot, unit],
            self.place.twin(),
        )

    def forward(self, n, unit):
        block = self.place.chip_at(unit) * self.blocks
        for mask in (1, 2, 3):
            self.push_in(n, mask, unit, block).wait_recv()
        for copy in self.twin_copies(n, unit):
            copy.start()
        for mask in range(CHIPS):

            @pl.when(unit == mask)
            def _():
                if mask:
                    self.push_out(n, mask).wait_recv()
                self.twin_out_copy(n, mask, unit).start()

    def forward_sent(self, n, unit):
        for copy in self.twin_copies(n, unit):
            copy.wait_send()
        self.twin_out_copy(n, 0, unit).wait_send()

    def arrive(self, n, unit):
        for copy in self.twin_copies(n, unit):
            copy.wait_recv()
        self.twin_out_copy(n, 0, unit).wait_recv()

    def load_in(self, n, unit, parity, w_in_v, v, sem):
        count, depth = self.blocks // 2, self.own_in.shape[2]
        block = self.place.chip_at(unit) * self.blocks + parity * count
        copies = []
        for mask in range(CHIPS):
            for which in range(2):
                shard = 2 * self.place.chip_at(mask) + (self.place.core if which == 0 else 1 - self.place.core)
                src = self.mine_in(n, mask, block, count) if which == 0 else self.twin_in.at[lax.rem(n, 2), mask, pl.ds(block, count)]
                row = pl.ds(pl.multiple_of(shard * depth, depth), depth)
                copies.append(pltpu.make_async_copy(src, w_in_v.at[v, :, row], sem.at[v, 2 * mask + which]))
        return copies

    def load(self, n, unit, other, w_in_v, w_out_v, v, sem):
        parity = self.place.core + other - 2 * self.place.core * other
        for copy in self.load_in(n, unit, parity, w_in_v, v, sem):
            copy.start()
        last = sem.at[v, 2 * CHIPS]

        @pl.when(other == 1)
        def _():
            pltpu.make_async_copy(self.twin_out.at[lax.rem(n, 2), unit], w_out_v.at[v], last).start()

        for mask in range(CHIPS):

            @pl.when((other == 0) & (unit == mask))
            def _():
                pltpu.make_async_copy(self.mine_out(n, mask), w_out_v.at[v], last).start()

    def loaded(self, w_in_v, w_out_v, v, sem):
        for copy in self.load_in(0, 0, 0, w_in_v, v, sem):
            copy.wait()
        pltpu.make_async_copy(self.own_out.at[0], w_out_v.at[v], sem.at[v, 2 * CHIPS]).wait()


def tile_of(ref, rows):
    return jnp.concatenate([ref[b, rows, :] for b in range(ref.shape[0])], axis=1)


def put_tile(ref, rows, value):
    for b in range(ref.shape[0]):
        ref[b, rows, :] = value[:, b * LANES : (b + 1) * LANES]


def forward_stack_kernel(layers, x_ref, own_in, own_out, *refs):
    xs_ref, kept_in, kept_out, got_in, got_out, twin_in, twin_out = refs[:7]
    x_v, unit_v, total_v, w_in_v, w_out_v = refs[7:12]
    x_sem, load_sem, credit = refs[12:15]
    sems = refs[15:]
    place = Place()
    stream = Stream(place, own_in, own_out, kept_in, kept_out, got_in, got_out, twin_in, twin_out, sems)
    tokens, width = x_v.shape
    tiles = tokens // TOK_TILE
    chunks = 2 * CHIPS

    meet(place)
    stream.push(0)
    fetch = pltpu.make_async_copy(x_ref, x_v, x_sem)
    fetch.start()
    fetch.wait()

    def first_unit(t, carry):
        rows = pl.ds(pl.multiple_of(t * TOK_TILE, TOK_TILE), TOK_TILE)
        x_wide, inv_rms = unit_rows_of(x_v[rows, :])
        put_tile(unit_v, rows, (x_wide * inv_rms).astype(BF16))
        total_v[rows, :] = jnp.zeros((TOK_TILE, width), F32)
        return carry

    lax.fori_loop(0, tiles, first_unit, 0)
    stream.forward(0, 0)
    stream.arrive(0, 0)
    stream.load(0, 0, 0, w_in_v, w_out_v, 0, load_sem)
    stream.forward_sent(0, 0)

    def save(n):
        return pltpu.make_async_copy(x_v, xs_ref.at[n], x_sem)

    def compute(v, last):
        w_in = lane_join(w_in_v.at[v], 0, w_in_v.shape[1])
        w_out = lane_join(w_out_v.at[v], 0, w_out_v.shape[1])
        pending = []

        def finish():
            t, hidden = pending.pop(0)
            rows = pl.ds(t * TOK_TILE, TOK_TILE)
            total = total_v[rows, :] + jnp.dot(hidden, w_out, preferred_element_type=F32)
            if not last:
                total_v[rows, :] = total
                return
            x_next = (x_v[rows, :].astype(F32) + total).astype(BF16)
            x_v[rows, :] = x_next
            total_v[rows, :] = jnp.zeros((TOK_TILE, width), F32)
            x_wide, inv_rms = unit_rows_of(x_next)
            put_tile(unit_v, rows, (x_wide * inv_rms).astype(BF16))

        for t in range(tiles):
            unit = tile_of(unit_v, pl.ds(t * TOK_TILE, TOK_TILE))
            pre = jnp.dot(unit, w_in, preferred_element_type=F32).astype(BF16).astype(F32)
            tanh = jnp.tanh(pre * (GELU_A + GELU_B * (pre * pre)))
            pending.append((t, (pre * (0.5 * tanh + 0.5)).astype(BF16)))
            if len(pending) > 1:
                finish()
        while pending:
            finish()

    def chunk_step(n, step):
        unit, other, v = lax.div(step, 2), lax.rem(step, 2), lax.rem(step, 2)
        more = n + 1 < layers

        @pl.when(step == 0)
        def _():
            stream.push_sent(n)

            @pl.when(more)
            def _():
                for q, device in enumerate(place.peers()):
                    pl.semaphore_signal(credit.at[q], inc=1, device_id=device, device_id_type=MESH)
                for q in range(CHIPS):
                    pl.semaphore_wait(credit.at[q], 1)
                stream.push(n + 1)

        sends = [
            ((other == 0) & (unit >= 2) & more, n + 1, unit - 2),
            ((other == 0) & (unit < 2) & (n > 0), n, unit + 2),
            ((other == 1) & (unit < 3) & (n == 0), n, unit + 1),
        ]
        for condition, layer, which in sends:

            @pl.when(condition)
            def _():
                stream.forward(layer, which)

        @pl.when(other == 0)
        def _():
            stream.load(n, unit, 1, w_in_v, w_out_v, 1, load_sem)

        @pl.when((other == 1) & (unit < 3))
        def _():
            stream.arrive(n, unit + 1)
            stream.load(n, unit + 1, 0, w_in_v, w_out_v, 0, load_sem)

        @pl.when((step == chunks - 1) & more)
        def _():
            stream.arrive(n + 1, 0)
            stream.load(n + 1, 0, 0, w_in_v, w_out_v, 0, load_sem)

        stream.loaded(w_in_v, w_out_v, v, load_sem)

        @pl.when(step < chunks - 1)
        def _():
            compute(v, False)

        @pl.when(step == chunks - 1)
        def _():
            @pl.when(n > 0)
            def _():
                save(n - 1).wait()

            compute(v, True)
            save(n).start()

        for condition, layer, which in sends:

            @pl.when(condition)
            def _():
                stream.forward_sent(layer, which)

    def layer_step(n, carry):
        lax.fori_loop(0, chunks, lambda step, c: (chunk_step(n, step), c)[1], 0)
        return carry

    lax.fori_loop(0, layers, layer_step, 0)
    save(layers - 1).wait()


def stream_semaphores():
    dma = pltpu.SemaphoreType.DMA
    return [dma((3, 4)), dma((2, 3, 4)), dma((3,)), dma((2, 3)), dma((4, 4)), dma((2, 4, 4)), dma((4,)), dma((2, 4))]


def stream_buffers(own_in, own_out):
    piece_in, piece_out = own_in.shape[1:], own_out.shape[1:]
    return [
        jax.ShapeDtypeStruct((2, 2) + piece_in, BF16),
        jax.ShapeDtypeStruct((2, 2) + piece_out, BF16),
        jax.ShapeDtypeStruct((2, CHIPS) + piece_in, BF16),
        jax.ShapeDtypeStruct((2, CHIPS) + piece_out, BF16),
    ]


def forward_stack(x_rows, own_in, own_out):
    layers = own_in.shape[0]
    tokens, width = x_rows.shape
    blocks_f, blocks_d = own_in.shape[1], own_out.shape[1]
    chunk_blocks, chunk = blocks_f // SHARDS, own_out.shape[2]
    anywhere = pl.BlockSpec(memory_space=pl.ANY)
    shapes = [
        jax.ShapeDtypeStruct((layers, tokens, width), BF16),
        jax.ShapeDtypeStruct(own_in.shape, BF16),
        jax.ShapeDtypeStruct(own_out.shape, BF16),
    ] + stream_buffers(own_in, own_out)
    flops = 4 * layers * tokens * width * blocks_f * LANES
    outs = pl.pallas_call(
        functools.partial(forward_stack_kernel, layers),
        in_specs=[anywhere] * 3,
        out_specs=[anywhere] * len(shapes),
        out_shape=shapes,
        scratch_shapes=[
            pltpu.VMEM((tokens, width), BF16),
            pltpu.VMEM((blocks_d, tokens, LANES), BF16),
            pltpu.VMEM((tokens, width), F32),
            pltpu.VMEM((2, chunk_blocks, width, LANES), BF16),
            pltpu.VMEM((2, blocks_d, chunk, LANES), BF16),
            pltpu.SemaphoreType.DMA,
            pltpu.SemaphoreType.DMA((2, 2 * CHIPS + 1)),
            pltpu.SemaphoreType.REGULAR((CHIPS,)),
        ]
        + stream_semaphores(),
        compiler_params=pltpu.CompilerParams(vmem_limit_bytes=VMEM_LIMIT, collective_id=0, has_side_effects=True),
        cost_estimate=pl.CostEstimate(flops=flops, bytes_accessed=100_000_000, transcendentals=0),
        name="forward_stack",
    )(x_rows, own_in, own_out)
    return outs[0], outs[1], outs[2]


def solution(mesh):
    row_spec = P(("local", "data"), None)
    weight_spec = P(None, ("local", "data"), None)
    swap_cores = [(0, 1), (1, 0)]
    swap_x = [(i, i ^ 1) for i in range(CHIPS)]
    swap_y = [(i, i ^ 2) for i in range(CHIPS)]

    def device_step(x_rows, grad_rows, w_in_part, w_out_part):
        layers = w_in_part.shape[0]
        core = lax.axis_index("data").astype(jnp.int32)
        chip = lax.axis_index("local").astype(jnp.int32)
        chip_x, chip_y = chip % 2, chip // 2
        mine, other = jnp.reshape(core, (1,)), jnp.reshape(1 - core, (1,))

        bwd_list = [(0, 0), (0, 1), (2, 0), (2, 1), (1, 0), (1, 1), (3, 0), (3, 1)]
        across = [chip, chip_y * 2 + 1 - chip_x, 2 - chip_y * 2 + chip_x, 3 - chip]
        in_chips = [across[0], across[1], across[2], across[3]]
        out_chips = [across[0], across[2], across[1], across[3]]

        def bwd_seq(chips):
            kept, got = chips[:2], chips[2:]
            return jnp.stack(
                [2 * c + core for c in kept] + [2 * c + 1 - core for c in kept] + [2 * c + core for c in got] + [2 * c + 1 - core for c in got]
            )

        order_bwd = jnp.stack([bwd_seq(in_chips), bwd_seq(out_chips)]).astype(jnp.int32)

        own_in = w_in_part.reshape(w_in_part.shape[:2] + (-1, LANES)).transpose(0, 2, 1, 3)
        own_out = w_out_part.reshape(w_out_part.shape[:2] + (-1, LANES)).transpose(0, 2, 1, 3)
        xs, kept_in, kept_out = forward_stack(x_rows, own_in, own_out)

        def exchange(n, grad_cur):
            keep_in, keep_out, grad_cur = lax.optimization_barrier(
                (jnp.stack([own_in[n], kept_in[n]]), jnp.stack([own_out[n], kept_out[n]]), grad_cur)
            )
            got_in = lax.ppermute(keep_in, "local", swap_y)
            got_out = lax.ppermute(keep_out, "local", swap_x)
            twin_in = lax.ppermute(keep_in, "data", swap_cores)
            twin_out = lax.ppermute(keep_out, "data", swap_cores)
            return [keep_in, got_in, twin_in], [keep_out, got_out, twin_out], grad_cur

        def swap_got(in_arrays, out_arrays):
            in_arrays.append(lax.ppermute(in_arrays[1], "data", swap_cores))
            out_arrays.append(lax.ppermute(out_arrays[1], "data", swap_cores))

        grad_cur = grad_rows
        grads_in, grads_out = [None] * layers, [None] * layers
        in_arrays, out_arrays, grad_cur = exchange(layers - 1, grad_cur)
        swap_got(in_arrays, out_arrays)
        for n in reversed(range(layers)):
            if n + 1 < layers:
                reduce(grads_in, grads_out, n + 1)
            unit, hidden, dpre, grad_next = layer_call(
                backward_kernel,
                order_bwd,
                [(xs, n - 1) if n else (x_rows[None], 0), (grad_cur[None], 0)],
                Pieces(in_arrays, bwd_list),
                Pieces(out_arrays, bwd_list),
                [x_rows.shape[1], w_out_part.shape[1] * SHARDS, w_out_part.shape[1] * SHARDS, "rows"],
                3,
            )
            if n > 0:
                in_arrays, out_arrays, grad_next = exchange(n - 1, grad_next)
            out_there = grad_w_out_half(other, hidden, grad_cur, None)
            out_arrived = lax.ppermute(out_there, "data", swap_cores)
            in_there = grad_w_in_half(other, unit, dpre, None)
            in_arrived = lax.ppermute(in_there, "data", swap_cores)
            grad_out_half = grad_w_out_half(mine, hidden, grad_cur, out_arrived)
            if n > 0:
                in_arrays[1], out_arrays[1], grad_out_half = lax.optimization_barrier((in_arrays[1], out_arrays[1], grad_out_half))
                swap_got(in_arrays, out_arrays)
            grad_in_half = grad_w_in_half(mine, unit, dpre, in_arrived)
            if n > 0:
                grad_next, grad_out_half, grad_in_half = lax.optimization_barrier((grad_next, grad_out_half, grad_in_half))
            grads_in[n], grads_out[n], grad_cur = grad_in_half, grad_out_half, grad_next
        reduce(grads_in, grads_out, 0)
        return xs[layers - 1], jnp.stack(grads_in), jnp.stack(grads_out), grad_cur

    def reduce(grads_in, grads_out, n):
        grads_out[n] = lax.psum_scatter(grads_out[n], "local", scatter_dimension=0, tiled=True)
        grads_in[n] = lax.psum_scatter(grads_in[n], "local", scatter_dimension=0, tiled=True)

    return jax.shard_map(
        device_step,
        mesh=mesh,
        in_specs=(row_spec, row_spec, weight_spec, weight_spec),
        out_specs=(row_spec, weight_spec, weight_spec, row_spec),
        check_vma=False,
    )
```

```python
import functools

import jax
import jax.numpy as jnp
from jax import lax
from jax.experimental import pallas as pl
from jax.experimental.pallas import tpu as pltpu
from jax.sharding import PartitionSpec as P

NORM_EPS = 1e-6
GELU_A = 0.7978845608028654
GELU_B = GELU_A * 0.044715
LAST_LAST = (((1,), (1,)), ((), ()))
FIRST_FIRST = (((0,), (0,)), ((), ()))
BF16 = jnp.bfloat16
F32 = jnp.float32
MESH = pl.DeviceIdType.MESH

CHIPS = 4
SHARDS = 8
LANES = 128
TOK_TILE = 256
VMEM_LIMIT = 67_000_000


def unit_rows_of(x_tile):
    x_wide = x_tile.astype(F32)
    inv_rms = lax.rsqrt(jnp.mean(x_wide * x_wide, axis=-1, keepdims=True) + NORM_EPS)
    return x_wide, inv_rms


def lane_join(ref):
    return jnp.concatenate([ref[b] for b in range(ref.shape[0])], axis=1)


def tile_of(ref, rows):
    return jnp.concatenate([ref[b, rows, :] for b in range(ref.shape[0])], axis=1)


def put_tile(ref, rows, value):
    for b in range(ref.shape[0]):
        ref[b, rows, :] = value[:, b * LANES : (b + 1) * LANES]


def tile_rows(t):
    return pl.ds(pl.multiple_of(t * TOK_TILE, TOK_TILE), TOK_TILE)


class Place:
    def __init__(self):
        self.chip = lax.axis_index("local")
        self.core = lax.axis_index("data")
        self.chip_x, self.chip_y = lax.rem(self.chip, 2), lax.div(self.chip, 2)

    def chip_at(self, mask):
        mask_x, mask_y = (mask % 2, mask // 2) if isinstance(mask, int) else (lax.rem(mask, 2), lax.div(mask, 2))
        return lax.rem(self.chip_x + mask_x, 2) + 2 * lax.rem(self.chip_y + mask_y, 2)

    def across(self, mask):
        return (self.chip_at(mask), self.core)

    def twin(self):
        return (self.chip, 1 - self.core)

    def peers(self):
        return [self.across(1), self.across(2), self.twin()]


def meet(place):
    barrier = pltpu.get_barrier_semaphore()
    for device in place.peers():
        pl.semaphore_signal(barrier, inc=1, device_id=device, device_id_type=MESH)
    pl.semaphore_wait(barrier, 3)


def remote(src, dst, send_sem, recv_sem, device):
    return pltpu.make_async_remote_copy(
        src_ref=src, dst_ref=dst, send_sem=send_sem, recv_sem=recv_sem, device_id=device, device_id_type=MESH
    )


class Stream:
    def __init__(self, place, order, own_in, own_out, kept_in, kept_out, got_in, got_out, twin_in, twin_out, sems):
        self.place, self.order = place, order
        self.own_in, self.own_out, self.kept_in, self.kept_out = own_in, own_out, kept_in, kept_out
        self.got_in, self.got_out, self.twin_in, self.twin_out = got_in, got_out, twin_in, twin_out
        (self.in_send, self.in_recv, self.out_send, self.out_recv) = sems[:4]
        (self.twin_in_send, self.twin_in_recv, self.twin_out_send, self.twin_out_recv) = sems[4:]
        self.blocks = own_in.shape[1] // CHIPS

    def mine_in(self, n, mask, block, count):
        rows = pl.ds(block, count)
        if mask == 0:
            return self.own_in.at[n, rows]
        if mask == 1:
            return self.kept_in.at[n, rows]
        return self.got_in.at[lax.rem(n, 2), mask - 2, rows]

    def mine_out(self, n, mask):
        if mask == 0:
            return self.own_out.at[n]
        if mask == 2:
            return self.kept_out.at[n]
        return self.got_out.at[lax.rem(n, 2), (mask - 1) // 2]

    def send_in(self, n, mask, unit):
        there = 1 if mask == 1 else 2
        block = self.place.chip_at(there ^ unit) * self.blocks
        src = self.mine_in(n, 1 if mask == 3 else 0, block, self.blocks)
        dst = self.mine_in(n, mask, block, self.blocks)
        recv = self.in_recv.at[lax.rem(n, 2), mask - 1, unit]
        return remote(src, dst, self.in_send.at[lax.rem(n, 2), mask - 1, unit], recv, self.place.across(there))

    def got_slice(self, n, mask, unit):
        dst = self.mine_in(n, mask, self.place.chip_at(unit) * self.blocks, self.blocks)
        recv = self.in_recv.at[lax.rem(n, 2), mask - 1, unit]
        return remote(dst, dst, self.in_send.at[lax.rem(n, 2), mask - 1, unit], recv, self.place.across(1))

    def send_out(self, n, mask):
        src, dst = self.mine_out(n, 2 if mask == 3 else 0), self.mine_out(n, mask)
        recv = self.out_recv.at[lax.rem(n, 2), mask - 1]
        return remote(src, dst, self.out_send.at[lax.rem(n, 2), mask - 1], recv, self.place.across(2 if mask == 2 else 1))

    def push(self, n, keep):
        for unit in self.order:
            for mask in (1, 2) if keep else (2, 3):
                self.send_in(n, mask, unit).start()
        for mask in (1, 2) if keep else (1, 3):
            self.send_out(n, mask).start()

    def relay_in(self, n):
        for unit in self.order:
            self.got_slice(n, 1, 2 ^ unit).wait_recv()
            self.send_in(n, 3, unit).start()

    def relay_out(self, n):
        self.send_out(n, 2).wait_recv()
        self.send_out(n, 3).start()

    def pushed(self, n, keep):
        for mask in (1, 2, 3) if keep else (2, 3):
            for unit in self.order:
                self.send_in(n, mask, unit).wait_send()
        for mask in (1, 2, 3) if keep else (1, 3):
            self.send_out(n, mask).wait_send()

    def twin_copies(self, n, unit):
        slot, block = lax.rem(n, 2), self.place.chip_at(unit) * self.blocks
        return [
            remote(
                self.mine_in(n, mask, block, self.blocks),
                self.twin_in.at[slot, mask, pl.ds(block, self.blocks)],
                self.twin_in_send.at[mask, unit],
                self.twin_in_recv.at[slot, mask, unit],
                self.place.twin(),
            )
            for mask in range(CHIPS)
        ]

    def twin_out_copy(self, n, mask, unit):
        slot = lax.rem(n, 2)
        recv = self.twin_out_recv.at[slot, unit]
        return remote(self.mine_out(n, mask), self.twin_out.at[slot, unit], self.twin_out_send.at[unit], recv, self.place.twin())

    def forward(self, n, unit):
        for mask in (2, 3):
            self.got_slice(n, mask, unit).wait_recv()
        for copy in self.twin_copies(n, unit):
            copy.start()
        for mask in range(CHIPS):

            @pl.when(unit == mask)
            def _():
                if mask in (1, 3):
                    self.send_out(n, mask).wait_recv()
                self.twin_out_copy(n, mask, unit).start()

    def forwarded(self, n, unit):
        for copy in self.twin_copies(n, unit):
            copy.wait_send()
        self.twin_out_copy(n, 0, unit).wait_send()

    def arrive(self, n, unit):
        for copy in self.twin_copies(n, unit):
            copy.wait_recv()
        self.twin_out_copy(n, 0, unit).wait_recv()

    def load_in(self, n, unit, parity, w_in_v, v, sem):
        count, depth = self.blocks // 2, self.own_in.shape[2]
        block = self.place.chip_at(unit) * self.blocks + parity * count
        copies = []
        for mask in range(CHIPS):
            for which in range(2):
                shard = 2 * self.place.chip_at(mask) + (self.place.core if which == 0 else 1 - self.place.core)
                src = self.mine_in(n, mask, block, count) if which == 0 else self.twin_in.at[lax.rem(n, 2), mask, pl.ds(block, count)]
                row = pl.ds(pl.multiple_of(shard * depth, depth), depth)
                copies.append(pltpu.make_async_copy(src, w_in_v.at[v, :, row], sem.at[v, 2 * mask + which]))
        return copies

    def load(self, n, unit, mine, w_in_v, w_out_v, v, sem):
        parity = 1 - self.place.core - mine + 2 * self.place.core * mine
        for copy in self.load_in(n, unit, parity, w_in_v, v, sem):
            copy.start()
        last = sem.at[v, 2 * CHIPS]

        @pl.when(mine == 0)
        def _():
            pltpu.make_async_copy(self.twin_out.at[lax.rem(n, 2), unit], w_out_v.at[v], last).start()

        for mask in range(CHIPS):

            @pl.when((mine == 1) & (unit == mask))
            def _():
                pltpu.make_async_copy(self.mine_out(n, mask), w_out_v.at[v], last).start()

    def loaded(self, w_in_v, w_out_v, v, sem):
        for copy in self.load_in(0, 0, 0, w_in_v, v, sem):
            copy.wait()
        pltpu.make_async_copy(self.own_out.at[0], w_out_v.at[v], sem.at[v, 2 * CHIPS]).wait()


class Pace:
    def __init__(self, place, stream, layers, layer_at, unit_at, keep, bufs, credit):
        self.place, self.stream, self.layers, self.layer_at, self.unit_at = place, stream, layers, layer_at, unit_at
        self.keep, self.credit = keep, credit
        self.w_in_v, self.w_out_v, self.load_sem = bufs

    def load(self, q, i, b):
        self.stream.load(self.layer_at(q), self.unit_at(i), b, self.w_in_v, self.w_out_v, b, self.load_sem)

    def head(self):
        self.stream.push(self.layer_at(0), self.keep)

    def head_end(self):
        if self.keep:
            self.stream.relay_in(self.layer_at(0))
        self.stream.forward(self.layer_at(0), self.unit_at(0))
        self.stream.arrive(self.layer_at(0), self.unit_at(0))
        self.load(0, 0, 0)
        self.stream.forwarded(self.layer_at(0), self.unit_at(0))

    def sends(self, q, s):
        i, b = lax.div(s, 2), lax.rem(s, 2)
        return [
            ((b == 0) & (i == 3) & (q + 1 < self.layers), q + 1, 0),
            ((b == 0) & (i < 3) & (q > 0), q, i + 1),
            ((b == 1) & (i < 3) & (q == 0), q, i + 1),
        ]

    def before(self, q, s):
        i, b = lax.div(s, 2), lax.rem(s, 2)
        more = q + 1 < self.layers

        @pl.when((s == 0) & (q > 0))
        def _():
            self.stream.pushed(self.layer_at(q - 1), self.keep)

        @pl.when((s == 0) & more)
        def _():
            for at, device in enumerate(self.place.peers()):
                pl.semaphore_signal(self.credit.at[at], inc=1, device_id=device, device_id_type=MESH)
            for at in range(3):
                pl.semaphore_wait(self.credit.at[at], 1)
            self.stream.push(self.layer_at(q + 1), self.keep)

        if self.keep:

            @pl.when((s == 2) & (q == 0))
            def _():
                self.stream.relay_out(self.layer_at(0))

            @pl.when(((s == 3) & (q > 0) | (s == 4) & (q == 0)) & more)
            def _():
                self.stream.relay_in(self.layer_at(q + 1))

            @pl.when(((s == 5) & (q > 0) | (s == 7) & (q == 0)) & more)
            def _():
                self.stream.relay_out(self.layer_at(q + 1))

        for condition, count, unit in self.sends(q, s):

            @pl.when(condition)
            def _():
                self.stream.forward(self.layer_at(count), self.unit_at(unit))

        @pl.when(b == 0)
        def _():
            self.load(q, i, 1)

        for condition, count, unit in (((b == 1) & (i < 3), q, i + 1), ((s == 7) & more, q + 1, 0)):

            @pl.when(condition)
            def _():
                self.stream.arrive(self.layer_at(count), self.unit_at(unit))
                self.load(count, unit, 0)

        self.stream.loaded(self.w_in_v, self.w_out_v, b, self.load_sem)

    def after(self, q, s):
        for condition, count, unit in self.sends(q, s):

            @pl.when(condition)
            def _():
                self.stream.forwarded(self.layer_at(count), self.unit_at(unit))


def when(condition):
    if isinstance(condition, bool):
        return lambda body: body() if condition else None
    return pl.when(condition)


def both(*conditions):
    kept = [c for c in conditions if not (isinstance(c, bool) and c)]
    if any(isinstance(c, bool) for c in kept):
        return False
    if not kept:
        return True
    return functools.reduce(lambda a, b: a & b, kept)


BACKWARD_UNITS = (1, 3, 2, 0)


def backward_mask(unit):
    if isinstance(unit, int):
        return BACKWARD_UNITS[unit]
    return (1 - lax.div(unit, 2)) + 2 * lax.rem(lax.div(unit + 1, 2), 2)


class Reduce:
    def __init__(self, place, layers, hbm, vmem, sems, outs):
        self.place, self.layers = place, layers
        self.p_out, self.o_a, self.o_b, self.u_out, self.q_in, self.i_a, self.s_in, self.i_b = hbm
        self.r_v, self.gt_v, self.gm_v, self.o_v, self.it_v, self.out_a, self.out_b, self.in_a, self.in_b = vmem
        (
            self.to_send,
            self.to_recv,
            self.ti_send,
            self.ti_recv,
            self.oa_send,
            self.oa_recv,
            self.ob_send,
            self.ob_recv,
            self.ia_send,
            self.ia_recv,
            self.ib_send,
            self.ib_recv,
            self.p_sem,
            self.q_sem,
            self.out_sem,
            self.in_sem,
            self.out_save,
            self.in_save,
            self.credit_o,
            self.credit_i,
        ) = sems
        self.gw_in, self.gw_out = outs
        self.half_out = self.out_a.shape[1]
        self.side = self.in_a.shape[0] // 2
        self.row = self.side // 2
        self.chunk = self.in_a.shape[1]

    def slot(self, q):
        return q % 2 if isinstance(q, int) else lax.rem(q, 2)

    def twin_out(self):
        return remote(self.r_v, self.o_v, self.to_send, self.to_recv, self.place.twin())

    def twin_in(self, b):
        return remote(self.gt_v, self.it_v.at[b], self.ti_send.at[b], self.ti_recv.at[b], self.place.twin())

    def across_x_out(self, q, i, h):
        s = self.slot(q)
        return remote(self.p_out.at[s, i, h], self.o_a.at[s, i, h], self.oa_send.at[i, h], self.oa_recv.at[s, i, h], self.place.across(1))

    def across_y_out(self, q, h):
        s = self.slot(q)
        return remote(self.u_out.at[s, h], self.o_b.at[s, h], self.ob_send.at[h], self.ob_recv.at[s, h], self.place.across(2))

    def across_y_in(self, q, i, b):
        s, far = self.slot(q), pl.ds(pl.multiple_of((1 - self.place.chip_y) * self.side, self.side), self.side)
        there = i + 1 - 2 * (i % 2)
        return remote(
            self.q_in.at[s, i, b, far], self.i_a.at[s, there, b], self.ia_send.at[i, b], self.ia_recv.at[s, there, b], self.place.across(2)
        )

    def across_x_in(self, q, i, b):
        s, far = self.slot(q), pl.ds(pl.multiple_of((1 - self.place.chip_x) * self.row, self.row), self.row)
        there = 3 - i
        return remote(
            self.s_in.at[s, i, b, far], self.i_b.at[s, there, b], self.ib_send.at[i, b], self.ib_recv.at[s, there, b], self.place.across(1)
        )

    def resend(self, q, copy_of):
        @when(q > 0)
        def _():
            copy_of(q).wait_send()

        copy_of(q).start()

    def save_p(self, q, i):
        s = self.slot(q)
        return [
            pltpu.make_async_copy(self.r_v.at[:, pl.ds(h * self.half_out, self.half_out)], self.p_out.at[s, i, h], self.p_sem.at[h])
            for h in range(2)
        ]

    def save_q(self, q, i, b, gm):
        return pltpu.make_async_copy(self.gm_v.at[gm], self.q_in.at[self.slot(q), i, b], self.q_sem.at[b])

    def out_loads(self, a, b):
        return [pltpu.make_async_copy(a, self.out_a, self.out_sem.at[0]), pltpu.make_async_copy(b, self.out_b, self.out_sem.at[1])]

    def out_first(self, q):
        return self.out_loads(self.o_a.at[self.slot(q), 0, 0], self.o_a.at[self.slot(q), 0, 1])

    def out_second(self, q, h):
        s = self.slot(q)
        return self.out_loads(self.p_out.at[s, 2, h], self.o_a.at[s, 1, h])

    def out_third(self, q, h):
        s = self.slot(q)
        return self.out_loads(self.p_out.at[s, 3, h], self.o_b.at[s, h])

    def out_second_save(self, q, h):
        return pltpu.make_async_copy(self.out_a, self.u_out.at[self.slot(q), h], self.out_save)

    def out_third_save(self, q, h):
        n = self.layers - 1 - q
        return pltpu.make_async_copy(self.out_a, self.gw_out.at[n, :, pl.ds(h * self.half_out, self.half_out)], self.out_save)

    def in_second(self, q, pair, b):
        s, near = self.slot(q), pl.ds(pl.multiple_of(self.place.chip_y * self.side, self.side), self.side)
        copies = []
        for at in range(2):
            i, rows = 2 * pair + at, pl.ds(at * self.side, self.side)
            copies.append(pltpu.make_async_copy(self.q_in.at[s, i, b, near], self.in_a.at[rows], self.in_sem.at[0, at]))
            copies.append(pltpu.make_async_copy(self.i_a.at[s, i, b], self.in_b.at[rows], self.in_sem.at[1, at]))
        return copies

    def in_third(self, q, b):
        s, near = self.slot(q), pl.ds(pl.multiple_of(self.place.chip_x * self.row, self.row), self.row)
        copies = []
        for i in range(CHIPS):
            rows = pl.ds(i * self.row, self.row)
            copies.append(pltpu.make_async_copy(self.s_in.at[s, i, b, near], self.in_a.at[rows], self.in_sem.at[0, i]))
            copies.append(pltpu.make_async_copy(self.i_b.at[s, i, b], self.in_b.at[rows], self.in_sem.at[1, i]))
        return copies

    def in_second_save(self, q, pair, b):
        s = self.slot(q)
        return [
            pltpu.make_async_copy(self.in_a.at[pl.ds(at * self.side, self.side)], self.s_in.at[s, 2 * pair + at, b], self.in_save.at[at])
            for at in range(2)
        ]

    def in_third_save(self, q, b):
        n = self.layers - 1 - q
        core = self.place.core
        copies = []
        for i in range(CHIPS):
            shard = 2 * self.place.chip_at(BACKWARD_UNITS[i]) + (core if b else 1 - core)
            columns = pl.ds(pl.multiple_of(shard * self.chunk, self.chunk), self.chunk)
            copies.append(pltpu.make_async_copy(self.in_a.at[pl.ds(i * self.row, self.row)], self.gw_in.at[n, :, columns], self.in_save.at[i]))
        return copies

    def add(self, a, b):
        for start in range(0, a.shape[0], 64):
            rows = pl.ds(start, 64)
            a[rows, :] = a[rows, :] + b[rows, :]

    def free(self, semaphore):
        pl.semaphore_signal(semaphore, inc=1, device_id=self.place.twin(), device_id_type=MESH)

    def start(self):
        for semaphore in (self.credit_o, self.credit_i.at[0], self.credit_i.at[1]):
            self.free(semaphore)

    def mid(self, q, s):
        here = q < self.layers
        older = q > 0

        for t in range(8):
            i, b = t // 2, t % 2
            layer = q if t < 7 else q - 1

            @when(both(s == (t + 1) % 8, here if t < 7 else older))
            def _():
                self.twin_in(b).wait_send()
                if b == 0:
                    self.twin_out().wait_send()
                else:
                    for copy in self.save_p(layer, i):
                        copy.wait()
                    self.save_q(layer, i, 1, 0).wait()
                    if i < 2:
                        for h in range(2):
                            self.resend(layer, lambda q, h=h: self.across_x_out(q, i, h))
                    self.resend(layer, lambda q: self.across_y_in(q, i, 1))

            layer = q if t < 5 else q - 1
            if b == 0:

                @when(both(s == (t + 3) % 8, here if t < 5 else older))
                def _():
                    self.save_q(layer, i, 0, 0).wait()
                    self.resend(layer, lambda q: self.across_y_in(q, i, 0))

        for step, pair, b, late in ((6, 0, 1, 0), (7, 0, 0, 0), (2, 1, 1, 1), (3, 1, 0, 1)):
            layer = q - late

            @when(both(s == step, older if late else here))
            def _():
                for copy in self.in_second_save(layer, pair, b):
                    copy.wait()
                for at in range(2):
                    self.resend(layer, lambda q, at=at: self.across_x_in(q, 2 * pair + at, b))

        for step, b in ((4, 1), (5, 0)):

            @when(both(s == step, older))
            def _():
                for copy in self.in_third_save(q - 1, b):
                    copy.wait()

        for step, pair, b, late in ((5, 0, 1, 0), (6, 0, 0, 0), (1, 1, 1, 1), (2, 1, 0, 1)):
            layer = q - late

            @when(both(s == step, older if late else here))
            def _():
                for at in range(2):
                    there = 2 * pair + 1 - at
                    self.across_y_in(layer, there, b).wait_recv()
                for copy in self.in_second(layer, pair, b):
                    copy.start()

        for step, b in ((3, 1), (4, 0)):

            @when(both(s == step, older))
            def _():
                for i in range(CHIPS):
                    self.across_x_in(q - 1, 3 - i, b).wait_recv()
                for copy in self.in_third(q - 1, b):
                    copy.start()

        for step, h in ((1, 0), (2, 1)):

            @when(both(s == step, older))
            def _():
                self.out_second_save(q - 1, h).wait()
                self.resend(q - 1, lambda q: self.across_y_out(q, h))

        for step, h in ((5, 0), (6, 1)):

            @when(both(s == step, older))
            def _():
                self.out_third_save(q - 1, h).wait()

        @when(both(s == 7, here))
        def _():
            for h in range(2):
                self.across_x_out(q, 0, h).wait_recv()
            for copy in self.out_first(q):
                copy.start()

        for step, h in ((0, 0), (1, 1)):

            @when(both(s == step, older))
            def _():
                self.across_x_out(q - 1, 1, h).wait_recv()
                for copy in self.out_second(q - 1, h):
                    copy.start()

        for step, h in ((4, 0), (5, 1)):

            @when(both(s == step, older))
            def _():
                self.across_y_out(q - 1, h).wait_recv()
                for copy in self.out_third(q - 1, h):
                    copy.start()

    def end(self, q, s, gm):
        here = q < self.layers
        older = q > 0
        final = q == self.layers - 1

        for t in range(8):
            i, b = t // 2, t % 2

            @when(both(s == t, here))
            def _():
                pl.semaphore_wait(self.credit_i.at[b], 1)
                self.twin_in(b).start()
                if b == 0:
                    pl.semaphore_wait(self.credit_o, 1)
                    self.twin_out().start()
                    return
                self.twin_out().wait_recv()
                self.add(self.r_v, self.o_v)

                @when(True if i < 3 else q < self.layers - 1)
                def _():
                    self.free(self.credit_o)

                if i == 3:
                    for copy in self.out_first(q):
                        copy.wait()
                    for start in range(0, self.r_v.shape[0], 64):
                        rows = pl.ds(start, 64)
                        for h, part in enumerate((self.out_a, self.out_b)):
                            columns = pl.ds(h * self.half_out, self.half_out)
                            self.r_v[rows, columns] = self.r_v[rows, columns] + part[rows, :]
                for copy in self.save_p(q, i):
                    copy.start()
                self.twin_in(0).wait_recv()
                self.add(self.gm_v.at[gm], self.it_v.at[0])

                @when(True if i < 3 else q < self.layers - 1)
                def _():
                    self.free(self.credit_i.at[0])

                self.save_q(q, i, 1, gm).start()

            if b == 0:
                layer = q if t < 6 else q - 1
                old = (gm + 1) % 3 if isinstance(gm, int) else lax.rem(gm + 1, 3)

                @when(both(s == (t + 2) % 8, here if t < 6 else older))
                def _():
                    self.twin_in(1).wait_recv()
                    self.add(self.gm_v.at[old], self.it_v.at[1])

                    @when(True if i < 3 else layer < self.layers - 1)
                    def _():
                        self.free(self.credit_i.at[1])

                    self.save_q(layer, i, 0, old).start()

        for step, pair, b, late in ((5, 0, 1, 0), (6, 0, 0, 0), (1, 1, 1, 1), (2, 1, 0, 1)):
            layer = q - late

            @when(both(s == step, older if late else here))
            def _():
                for copy in self.in_second(layer, pair, b):
                    copy.wait()
                self.add(self.in_a, self.in_b)
                for copy in self.in_second_save(layer, pair, b):
                    copy.start()

        for step, b in ((3, 1), (4, 0)):

            @when(both(s == step, older))
            def _():
                for copy in self.in_third(q - 1, b):
                    copy.wait()
                self.add(self.in_a, self.in_b)
                for copy in self.in_third_save(q - 1, b):
                    copy.start()

        for step, h in ((0, 0), (1, 1)):

            @when(both(s == step, older))
            def _():
                for copy in self.out_second(q - 1, h):
                    copy.wait()
                self.add(self.out_a, self.out_b)
                self.out_second_save(q - 1, h).start()

        for step, h in ((4, 0), (5, 1)):

            @when(both(s == step, older))
            def _():
                for copy in self.out_third(q - 1, h):
                    copy.wait()
                self.add(self.out_a, self.out_b)
                self.out_third_save(q - 1, h).start()

    def finish(self):
        q = self.layers
        for s in range(7):
            self.mid(q, s)
            if s < 6:
                self.end(q, s, (8 * q + s) % 3)
        last = q - 1
        for h in range(2):
            for i in range(2):
                self.across_x_out(last, i, h).wait_send()
            self.across_y_out(last, h).wait_send()
        for b in range(2):
            for i in range(CHIPS):
                self.across_y_in(last, i, b).wait_send()
                self.across_x_in(last, i, b).wait_send()


def forward_stack_kernel(layers, x_ref, w_in_ref, w_out_ref, *refs):
    xs_ref, own_in, own_out, kept_in, kept_out, got_in, got_out, twin_in, twin_out = refs[:9]
    x_v, unit_v, total_v, w_in_v, w_out_v, stage_in, stage_out = refs[9:16]
    x_sem, load_sem, stage_sem, credit = refs[16:20]
    place = Place()
    stream = Stream(place, (0, 1, 2, 3), own_in, own_out, kept_in, kept_out, got_in, got_out, twin_in, twin_out, refs[20:])
    pace = Pace(place, stream, layers, lambda q: q, lambda i: i, True, (w_in_v, w_out_v, load_sem), credit)
    tokens, width = x_v.shape
    tiles = tokens // TOK_TILE

    def to_lanes(n):
        pairs = ((w_in_ref, stage_in, own_in, 0), (w_out_ref, stage_out, own_out, 1))
        for src, stage, _, at in pairs:
            for b in range(stage.shape[0]):
                pltpu.make_async_copy(src.at[n, :, pl.ds(b * LANES, LANES)], stage.at[b], stage_sem.at[at]).start()
        for _, stage, own, at in pairs:
            pltpu.make_async_copy(own.at[n], stage, stage_sem.at[at]).wait()
            pltpu.make_async_copy(stage, own.at[n], stage_sem.at[at]).start()
        for _, stage, own, at in pairs:
            pltpu.make_async_copy(stage, own.at[n], stage_sem.at[at]).wait()

    fetch = pltpu.make_async_copy(x_ref, x_v, x_sem)
    fetch.start()
    to_lanes(0)
    meet(place)
    pace.head()

    def other_lanes(n, carry):
        to_lanes(n)
        return carry

    lax.fori_loop(1, layers, other_lanes, 0)
    fetch.wait()

    def first_unit(t, carry):
        rows = tile_rows(t)
        x_wide, inv_rms = unit_rows_of(x_v[rows, :])
        put_tile(unit_v, rows, (x_wide * inv_rms).astype(BF16))
        total_v[rows, :] = jnp.zeros((TOK_TILE, width), F32)
        return carry

    lax.fori_loop(0, tiles, first_unit, 0)
    pace.head_end()

    def save(n):
        return pltpu.make_async_copy(x_v, xs_ref.at[n], x_sem)

    def compute(v, last):
        w_in, w_out = lane_join(w_in_v.at[v]), lane_join(w_out_v.at[v])
        pending = []

        def finish():
            t, hidden = pending.pop(0)
            rows = pl.ds(t * TOK_TILE, TOK_TILE)
            total = total_v[rows, :] + jnp.dot(hidden, w_out, preferred_element_type=F32)
            if not last:
                total_v[rows, :] = total
                return
            x_next = (x_v[rows, :].astype(F32) + total).astype(BF16)
            x_v[rows, :] = x_next
            total_v[rows, :] = jnp.zeros((TOK_TILE, width), F32)
            x_wide, inv_rms = unit_rows_of(x_next)
            put_tile(unit_v, rows, (x_wide * inv_rms).astype(BF16))

        for t in range(tiles):
            unit = tile_of(unit_v, pl.ds(t * TOK_TILE, TOK_TILE))
            pre = jnp.dot(unit, w_in, preferred_element_type=F32).astype(BF16).astype(F32)
            tanh = jnp.tanh(pre * (GELU_A + GELU_B * (pre * pre)))
            pending.append((t, (pre * (0.5 * tanh + 0.5)).astype(BF16)))
            if len(pending) > 1:
                finish()
        while pending:
            finish()

    def step(n, s):
        v = lax.rem(s, 2)
        pace.before(n, s)

        @pl.when(s < 7)
        def _():
            compute(v, False)

        @pl.when(s == 7)
        def _():
            @pl.when(n > 0)
            def _():
                save(n - 1).wait()

            compute(v, True)
            save(n).start()

        pace.after(n, s)

    def layer_step(n, carry):
        lax.fori_loop(0, 8, lambda s, c: (step(n, s), c)[1], 0)
        return carry

    lax.fori_loop(0, layers, layer_step, 0)
    stream.pushed(layers - 1, True)
    save(layers - 1).wait()


def backward_stack_kernel(layers, x_ref, xs_ref, dy_ref, own_in, own_out, kept_in, kept_out, *refs):
    gw_in, gw_out, dx_ref, got_in, got_out, twin_in, twin_out = refs[:7]
    sums_hbm = refs[7:15]
    unit_v, dy_v, du_v, hidden_v, dpre_v, w_in_v, w_out_v, x_v = refs[15:23]
    sums_v = refs[23:32]
    row_sem, x_sem, load_sem, credit = refs[32:36]
    stream_sems, sum_sems = refs[36:44], refs[44:]
    place = Place()
    stream = Stream(place, BACKWARD_UNITS, own_in, own_out, kept_in, kept_out, got_in, got_out, twin_in, twin_out, stream_sems)
    pace = Pace(place, stream, layers, lambda q: layers - 1 - q, backward_mask, False, (w_in_v, w_out_v, load_sem), credit)
    sums = Reduce(place, layers, sums_hbm, sums_v, sum_sems, (gw_in, gw_out))
    r_v, gt_v, gm_v = sums_v[:3]
    blocks_d, tokens, _ = unit_v.shape
    width = blocks_d * LANES
    tiles = tokens // TOK_TILE

    meet(place)
    pace.head()
    sums.start()

    def rows_copies(to_vmem, ref):
        copies = []
        for b in range(blocks_d):
            pair = (ref.at[:, pl.ds(b * LANES, LANES)], dy_v.at[b])
            copies.append(pltpu.make_async_copy(*(pair if to_vmem else pair[::-1]), row_sem.at[b]))
        return copies

    dy_copies = rows_copies(True, dy_ref)
    for copy in dy_copies:
        copy.start()

    def fetch(n, which, t):
        dst, sem = x_v.at[which, lax.rem(t, 2)], x_sem.at[which, lax.rem(t, 2)]

        @pl.when(n > 0)
        def _():
            pltpu.make_async_copy(xs_ref.at[n - 1, tile_rows(t)], dst, sem).start()

        @pl.when(n == 0)
        def _():
            pltpu.make_async_copy(x_ref.at[tile_rows(t)], dst, sem).start()

    def fetched(which, t):
        at = lax.rem(t, 2)
        pltpu.make_async_copy(x_ref.at[tile_rows(0)], x_v.at[which, at], x_sem.at[which, at]).wait()
        return x_v[which, at]

    def first_unit(t, carry):
        @pl.when(t + 1 < tiles)
        def _():
            fetch(layers - 1, 1, t + 1)

        rows = tile_rows(t)
        x_wide, inv_rms = unit_rows_of(fetched(1, t))
        put_tile(unit_v, rows, (x_wide * inv_rms).astype(BF16))
        du_v[rows, :] = jnp.zeros((TOK_TILE, width), F32)
        return carry

    fetch(layers - 1, 1, 0)
    lax.fori_loop(0, tiles, first_unit, 0)
    for copy in dy_copies:
        copy.wait()
    pace.head_end()

    def hidden_part(v):
        w_in, w_out = lane_join(w_in_v.at[v]), lane_join(w_out_v.at[v])
        pending = []

        def finish():
            t, dpre = pending.pop(0)
            rows = pl.ds(t * TOK_TILE, TOK_TILE)
            du_v[rows, :] = du_v[rows, :] + lax.dot_general(dpre, w_in, LAST_LAST, preferred_element_type=F32)

        for t in range(tiles):
            rows = pl.ds(t * TOK_TILE, TOK_TILE)
            pre = jnp.dot(tile_of(unit_v, rows), w_in, preferred_element_type=F32).astype(BF16).astype(F32)
            dhidden = lax.dot_general(tile_of(dy_v, rows), w_out, LAST_LAST, preferred_element_type=F32)
            poly = GELU_A + GELU_B * (pre * pre)
            cdf = 0.5 * jnp.tanh(pre * poly) + 0.5
            hidden = pre * cdf
            slope = cdf + (hidden * (6.0 * poly - 4.0 * GELU_A)) * (1.0 - cdf)
            dpre = (slope * dhidden).astype(BF16)
            put_tile(hidden_v, rows, hidden.astype(BF16))
            put_tile(dpre_v, rows, dpre)
            pending.append((t, dpre))
            if len(pending) > 1:
                finish()
        while pending:
            finish()

    def gradient_part(gm):
        r_v[...] = lax.dot_general(lane_join(hidden_v), lane_join(dy_v), FIRST_FIRST, preferred_element_type=F32)
        dpre = lane_join(dpre_v)

        def unit_of(parity):
            per = blocks_d // SHARDS
            parts = [unit_v[(2 * c + parity) * per + b] for c in range(CHIPS) for b in range(per)]
            return jnp.concatenate(parts, axis=1)

        gt_v[...] = lax.dot_general(unit_of(1 - place.core), dpre, FIRST_FIRST, preferred_element_type=F32)
        gm_v[gm] = lax.dot_general(unit_of(place.core), dpre, FIRST_FIRST, preferred_element_type=F32)

    def step(q, s):
        gm = lax.rem(8 * q + s, 3)
        pace.before(q, s)
        hidden_part(lax.rem(s, 2))
        sums.mid(q, s)
        gradient_part(gm)
        sums.end(q, s, gm)
        pace.after(q, s)

    def layer_step(q, carry):
        n = layers - 1 - q
        lax.fori_loop(0, 8, lambda s, c: (step(q, s), c)[1], 0)
        fetch(n, 0, 0)

        @pl.when(n > 0)
        def _():
            fetch(n - 1, 1, 0)

        def close(t, carry):
            @pl.when(t + 1 < tiles)
            def _():
                fetch(n, 0, t + 1)

                @pl.when(n > 0)
                def _():
                    fetch(n - 1, 1, t + 1)

            rows = tile_rows(t)
            x_wide, inv_rms = unit_rows_of(fetched(0, t))
            value, du = x_wide * inv_rms, du_v[rows, :]
            row_mean = jnp.mean(du * value, axis=-1, keepdims=True)
            put_tile(dy_v, rows, (tile_of(dy_v, rows).astype(F32) + inv_rms * (du - value * row_mean)).astype(BF16))
            du_v[rows, :] = jnp.zeros((TOK_TILE, width), F32)

            @pl.when(n > 0)
            def _():
                x_wide, inv_rms = unit_rows_of(fetched(1, t))
                put_tile(unit_v, rows, (x_wide * inv_rms).astype(BF16))

            return carry

        lax.fori_loop(0, tiles, close, 0)
        return carry

    lax.fori_loop(0, layers, layer_step, 0)
    dx_copies = rows_copies(False, dx_ref)
    for copy in dx_copies:
        copy.start()
    sums.finish()
    stream.pushed(0, False)
    for copy in dx_copies:
        copy.wait()


def stream_semaphores():
    dma = pltpu.SemaphoreType.DMA
    return [dma((2, 3, 4)), dma((2, 3, 4)), dma((2, 3)), dma((2, 3)), dma((4, 4)), dma((2, 4, 4)), dma((4,)), dma((2, 4))]


def sum_semaphores():
    dma, regular = pltpu.SemaphoreType.DMA, pltpu.SemaphoreType.REGULAR
    return [
        dma,
        dma,
        dma((2,)),
        dma((2,)),
        dma((2, 2)),
        dma((2, 2, 2)),
        dma((2,)),
        dma((2, 2)),
        dma((4, 2)),
        dma((2, 4, 2)),
        dma((4, 2)),
        dma((2, 4, 2)),
        dma((2,)),
        dma((2,)),
        dma((2,)),
        dma((2, 4)),
        dma,
        dma((4,)),
        regular,
        regular((2,)),
    ]


def stream_buffers(piece_in, piece_out):
    return [
        jax.ShapeDtypeStruct((2, 2) + piece_in, BF16),
        jax.ShapeDtypeStruct((2, 2) + piece_out, BF16),
        jax.ShapeDtypeStruct((2, CHIPS) + piece_in, BF16),
        jax.ShapeDtypeStruct((2, CHIPS) + piece_out, BF16),
    ]


ANYWHERE = pl.BlockSpec(memory_space=pl.ANY)


def forward_stack(x_rows, w_in, w_out):
    layers, depth, hidden_size = w_in.shape
    tokens, width = x_rows.shape
    chunk = w_out.shape[1]
    piece_in, piece_out = (hidden_size // LANES, depth, LANES), (width // LANES, chunk, LANES)
    pieces = [jax.ShapeDtypeStruct((layers,) + piece, BF16) for piece in (piece_in, piece_out)]
    shapes = [jax.ShapeDtypeStruct((layers, tokens, width), BF16)] + pieces * 2 + stream_buffers(piece_in, piece_out)
    outs = pl.pallas_call(
        functools.partial(forward_stack_kernel, layers),
        in_specs=[ANYWHERE] * 3,
        out_specs=[ANYWHERE] * len(shapes),
        out_shape=shapes,
        scratch_shapes=[
            pltpu.VMEM((tokens, width), BF16),
            pltpu.VMEM((width // LANES, tokens, LANES), BF16),
            pltpu.VMEM((tokens, width), F32),
            pltpu.VMEM((2, chunk // LANES, width, LANES), BF16),
            pltpu.VMEM((2, width // LANES, chunk, LANES), BF16),
            pltpu.VMEM(piece_in, BF16),
            pltpu.VMEM(piece_out, BF16),
            pltpu.SemaphoreType.DMA,
            pltpu.SemaphoreType.DMA((2, 2 * CHIPS + 1)),
            pltpu.SemaphoreType.DMA((2,)),
            pltpu.SemaphoreType.REGULAR((3,)),
        ]
        + stream_semaphores(),
        compiler_params=pltpu.CompilerParams(vmem_limit_bytes=VMEM_LIMIT, collective_id=0, has_side_effects=True),
        cost_estimate=pl.CostEstimate(flops=4 * layers * tokens * width * hidden_size, bytes_accessed=100_000_000, transcendentals=0),
        name="forward_stack",
    )(x_rows, w_in, w_out)
    return outs[:5]


def backward_stack(x_rows, xs, grad_rows, own_in, own_out, kept_in, kept_out):
    layers, blocks_f, depth, _ = own_in.shape
    blocks_d, chunk = own_out.shape[1], own_out.shape[2]
    tokens, width = x_rows.shape
    half, quarter = width // 2, width // 4
    hidden_size = blocks_f * LANES

    def sums(*shape):
        return jax.ShapeDtypeStruct(shape, F32)

    shapes = (
        [sums(layers, depth, hidden_size), sums(layers, chunk, width), jax.ShapeDtypeStruct((tokens, width), BF16)]
        + stream_buffers(own_in.shape[1:], own_out.shape[1:])
        + [
            sums(2, 4, 2, chunk, half),
            sums(2, 2, 2, chunk, half),
            sums(2, 2, chunk, half),
            sums(2, 2, chunk, half),
            sums(2, 4, 2, half, chunk),
            sums(2, 4, 2, quarter, chunk),
            sums(2, 4, 2, quarter, chunk),
            sums(2, 4, 2, depth, chunk),
        ]
    )
    outs = pl.pallas_call(
        functools.partial(backward_stack_kernel, layers),
        in_specs=[ANYWHERE] * 7,
        out_specs=[ANYWHERE] * len(shapes),
        out_shape=shapes,
        scratch_shapes=[
            pltpu.VMEM((blocks_d, tokens, LANES), BF16),
            pltpu.VMEM((blocks_d, tokens, LANES), BF16),
            pltpu.VMEM((tokens, width), F32),
            pltpu.VMEM((chunk // LANES, tokens, LANES), BF16),
            pltpu.VMEM((chunk // LANES, tokens, LANES), BF16),
            pltpu.VMEM((2, chunk // LANES, width, LANES), BF16),
            pltpu.VMEM((2, blocks_d, chunk, LANES), BF16),
            pltpu.VMEM((2, 2, TOK_TILE, width), BF16),
            pltpu.VMEM((chunk, width), F32),
            pltpu.VMEM((half, chunk), F32),
            pltpu.VMEM((3, half, chunk), F32),
            pltpu.VMEM((chunk, width), F32),
            pltpu.VMEM((2, half, chunk), F32),
            pltpu.VMEM((chunk, half), F32),
            pltpu.VMEM((chunk, half), F32),
            pltpu.VMEM((half, chunk), F32),
            pltpu.VMEM((half, chunk), F32),
            pltpu.SemaphoreType.DMA((blocks_d,)),
            pltpu.SemaphoreType.DMA((2, 2)),
            pltpu.SemaphoreType.DMA((2, 2 * CHIPS + 1)),
            pltpu.SemaphoreType.REGULAR((3,)),
        ]
        + stream_semaphores()
        + sum_semaphores(),
        compiler_params=pltpu.CompilerParams(vmem_limit_bytes=VMEM_LIMIT, collective_id=1, has_side_effects=True),
        cost_estimate=pl.CostEstimate(flops=10 * layers * tokens * width * hidden_size, bytes_accessed=300_000_000, transcendentals=0),
        name="backward_stack",
    )(x_rows, xs, grad_rows, own_in, own_out, kept_in, kept_out)
    return outs[:3]


def solution(mesh):
    row_spec = P(("local", "data"), None)
    weight_spec = P(None, ("local", "data"), None)

    def device_step(x_rows, grad_rows, w_in, w_out):
        xs, own_in, own_out, kept_in, kept_out = forward_stack(x_rows, w_in, w_out)
        gw_in, gw_out, dx = backward_stack(x_rows, xs, grad_rows, own_in, own_out, kept_in, kept_out)
        return xs[w_in.shape[0] - 1], gw_in, gw_out, dx

    return jax.shard_map(
        device_step,
        mesh=mesh,
        in_specs=(row_spec, row_spec, weight_spec, weight_spec),
        out_specs=(row_spec, weight_spec, weight_spec, row_spec),
        check_vma=False,
    )
```

```python
import functools

import jax
import jax.numpy as jnp
from jax import lax
from jax.experimental import pallas as pl
from jax.experimental.pallas import tpu as pltpu
from jax.sharding import PartitionSpec as P

NORM_EPS = 1e-6
GELU_A = 0.7978845608028654
GELU_B = GELU_A * 0.044715
LAST_LAST = (((1,), (1,)), ((), ()))
FIRST_FIRST = (((0,), (0,)), ((), ()))
BF16 = jnp.bfloat16
F32 = jnp.float32
MESH = pl.DeviceIdType.MESH

TWO = 2
CHIPS = 4
STEPS = 8
SHARDS = 8
LANES = 128
TOK_TILE = 256
VMEM_LIMIT = 67_000_000
ADD_ROWS = 64


def unit_rows_of(x_tile):
    x_wide = x_tile.astype(F32)
    inv_rms = lax.rsqrt(jnp.mean(x_wide * x_wide, axis=-1, keepdims=True) + NORM_EPS)
    return x_wide, inv_rms


def lane_join(ref):
    return jnp.concatenate([ref[b] for b in range(ref.shape[0])], axis=1)


def tile_of(ref, rows):
    return jnp.concatenate([ref[b, rows, :] for b in range(ref.shape[0])], axis=1)


def put_tile(ref, rows, value):
    for b in range(ref.shape[0]):
        ref[b, rows, :] = value[:, b * LANES : (b + 1) * LANES]


def tile_rows(t):
    return pl.ds(pl.multiple_of(t * TOK_TILE, TOK_TILE), TOK_TILE)


def odd(x):
    return lax.rem(x, TWO)


def half(x):
    return lax.div(x, TWO)


def notify(semaphore, device):
    pl.semaphore_signal(semaphore, inc=1, device_id=device, device_id_type=MESH)


def await_one(semaphore):
    pl.semaphore_wait(semaphore, 1)


class Place:
    def __init__(self):
        self.chip = lax.axis_index("local")
        self.core = lax.axis_index("data")
        self.chip_x, self.chip_y = odd(self.chip), half(self.chip)

    def chip_at(self, mask):
        mask_x, mask_y = (mask % 2, mask // 2) if isinstance(mask, int) else (odd(mask), half(mask))
        return odd(self.chip_x + mask_x) + 2 * odd(self.chip_y + mask_y)

    def across(self, mask):
        return (self.chip_at(mask), self.core)

    def twin(self):
        return (self.chip, 1 - self.core)

    def peers(self):
        return [self.across(1), self.across(2), self.twin()]


def meet(place):
    barrier = pltpu.get_barrier_semaphore()
    for device in place.peers():
        notify(barrier, device)
    pl.semaphore_wait(barrier, 3)


def remote(src, dst, send_sem, recv_sem, device):
    return pltpu.make_async_remote_copy(
        src_ref=src, dst_ref=dst, send_sem=send_sem, recv_sem=recv_sem, device_id=device, device_id_type=MESH
    )


class Stream:
    def __init__(self, place, order, own_in, own_out, kept_in, kept_out, got_in, got_out, twin_in, twin_out, sems):
        self.place, self.order = place, order
        self.own_in, self.own_out, self.kept_in, self.kept_out = own_in, own_out, kept_in, kept_out
        self.got_in, self.got_out, self.twin_in, self.twin_out = got_in, got_out, twin_in, twin_out
        (self.in_send, self.in_recv, self.out_send, self.out_recv) = sems[:4]
        (self.twin_in_send, self.twin_in_recv, self.twin_out_send, self.twin_out_recv) = sems[4:]
        self.blocks = own_in.shape[1] // CHIPS

    def mine_in(self, n, mask, block, count):
        rows = pl.ds(block, count)
        if mask == 0:
            return self.own_in.at[n, rows]
        if mask == 1:
            return self.kept_in.at[n, rows]
        return self.got_in.at[odd(n), mask - 2, rows]

    def mine_out(self, n, mask):
        if mask == 0:
            return self.own_out.at[n]
        if mask == 2:
            return self.kept_out.at[n]
        return self.got_out.at[odd(n), (mask - 1) // 2]

    def send_in(self, n, mask, unit):
        there = 1 if mask == 1 else 2
        block = self.place.chip_at(there ^ unit) * self.blocks
        src = self.mine_in(n, 1 if mask == 3 else 0, block, self.blocks)
        dst = self.mine_in(n, mask, block, self.blocks)
        recv = self.in_recv.at[odd(n), mask - 1, unit]
        return remote(src, dst, self.in_send.at[odd(n), mask - 1, unit], recv, self.place.across(there))

    def got_slice(self, n, mask, unit):
        dst = self.mine_in(n, mask, self.place.chip_at(unit) * self.blocks, self.blocks)
        recv = self.in_recv.at[odd(n), mask - 1, unit]
        return remote(dst, dst, self.in_send.at[odd(n), mask - 1, unit], recv, self.place.across(1))

    def send_out(self, n, mask):
        src, dst = self.mine_out(n, 2 if mask == 3 else 0), self.mine_out(n, mask)
        recv = self.out_recv.at[odd(n), mask - 1]
        return remote(src, dst, self.out_send.at[odd(n), mask - 1], recv, self.place.across(2 if mask == 2 else 1))

    def push_in(self, n, masks, units):
        for unit in units:
            for mask in masks:
                self.send_in(n, mask, unit).start()

    def push_out(self, n, masks):
        for mask in masks:
            self.send_out(n, mask).start()

    def relay_in(self, n, unit):
        self.got_slice(n, 1, 2 ^ unit).wait_recv()
        self.send_in(n, 3, unit).start()

    def relay_out(self, n):
        self.send_out(n, 2).wait_recv()
        self.send_out(n, 3).start()

    def pushed(self, n, keep):
        for mask in (1, 2, 3) if keep else (2, 3):
            for unit in self.order:
                self.send_in(n, mask, unit).wait_send()
        for mask in (1, 2, 3) if keep else (1, 3):
            self.send_out(n, mask).wait_send()

    def twin_copies(self, n, unit):
        slot, block = odd(n), self.place.chip_at(unit) * self.blocks
        return [
            remote(
                self.mine_in(n, mask, block, self.blocks),
                self.twin_in.at[slot, mask, pl.ds(block, self.blocks)],
                self.twin_in_send.at[mask, unit],
                self.twin_in_recv.at[slot, mask, unit],
                self.place.twin(),
            )
            for mask in range(CHIPS)
        ]

    def twin_out_copy(self, n, mask, unit):
        slot = odd(n)
        recv = self.twin_out_recv.at[slot, unit]
        return remote(self.mine_out(n, mask), self.twin_out.at[slot, unit], self.twin_out_send.at[unit], recv, self.place.twin())

    def forward(self, n, unit):
        for mask in (2, 3):
            self.got_slice(n, mask, unit).wait_recv()
        for copy in self.twin_copies(n, unit):
            copy.start()
        for mask in range(CHIPS):

            @pl.when(unit == mask)
            def _():
                if mask in (1, 3):
                    self.send_out(n, mask).wait_recv()
                self.twin_out_copy(n, mask, unit).start()

    def forwarded(self, n, unit):
        for copy in self.twin_copies(n, unit):
            copy.wait_send()
        self.twin_out_copy(n, 0, unit).wait_send()

    def arrive(self, n, unit):
        for copy in self.twin_copies(n, unit):
            copy.wait_recv()
        self.twin_out_copy(n, 0, unit).wait_recv()

    def load_in(self, n, unit, parity, w_in_v, v, sem):
        count, depth = self.blocks // 2, self.own_in.shape[2]
        block = self.place.chip_at(unit) * self.blocks + parity * count
        copies = []
        for mask in range(CHIPS):
            for which in range(TWO):
                shard = 2 * self.place.chip_at(mask) + (self.place.core if which == 0 else 1 - self.place.core)
                src = self.mine_in(n, mask, block, count) if which == 0 else self.twin_in.at[odd(n), mask, pl.ds(block, count)]
                row = pl.ds(pl.multiple_of(shard * depth, depth), depth)
                copies.append(pltpu.make_async_copy(src, w_in_v.at[v, :, row], sem.at[v, 2 * mask + which]))
        return copies

    def load(self, n, unit, mine, w_in_v, w_out_v, v, sem):
        parity = 1 - self.place.core - mine + 2 * self.place.core * mine
        for copy in self.load_in(n, unit, parity, w_in_v, v, sem):
            copy.start()
        last = sem.at[v, SHARDS]

        @pl.when(mine == 0)
        def _():
            pltpu.make_async_copy(self.twin_out.at[odd(n), unit], w_out_v.at[v], last).start()

        for mask in range(CHIPS):

            @pl.when((mine == 1) & (unit == mask))
            def _():
                pltpu.make_async_copy(self.mine_out(n, mask), w_out_v.at[v], last).start()

    def loaded(self, w_in_v, w_out_v, v, sem):
        for copy in self.load_in(0, 0, 0, w_in_v, v, sem):
            copy.wait()
        pltpu.make_async_copy(self.own_out.at[0], w_out_v.at[v], sem.at[v, SHARDS]).wait()


class Pace:
    def __init__(self, place, stream, layers, layer_at, unit_at, keep, bufs, credit):
        self.place, self.stream, self.layers, self.layer_at, self.unit_at = place, stream, layers, layer_at, unit_at
        self.keep, self.credit = keep, credit
        self.w_in_v, self.w_out_v, self.load_sem = bufs

    def load(self, q, i, b):
        self.stream.load(self.layer_at(q), self.unit_at(i), b, self.w_in_v, self.w_out_v, b, self.load_sem)

    def head(self):
        n, units = self.layer_at(0), self.stream.order
        if not self.keep:
            self.stream.push_in(n, (2, 3), units)
            self.stream.push_out(n, (1, 3))
            return
        self.stream.push_in(n, (1,), [units[at] for at in (0, 2, 1, 3)])
        self.stream.push_in(n, (2,), units[:1])
        self.stream.push_out(n, (1,))

    def head_end(self):
        n, units = self.layer_at(0), self.stream.order
        if self.keep:
            for at, unit in enumerate(units):
                if at:
                    self.stream.push_in(n, (2,), (unit,))
                self.stream.relay_in(n, unit)
                if at == 1:
                    self.stream.push_out(n, (2,))
        self.first_chunk(0)

    def first_chunk(self, q):
        n, unit = self.layer_at(q), self.unit_at(0)
        self.stream.forward(n, unit)
        self.stream.arrive(n, unit)
        self.load(q, 0, 0)
        self.stream.forwarded(n, unit)

    def sends(self, q, s):
        i, b = half(s), odd(s)
        early = (q + 1 < self.layers) & (q > 0) if self.keep else q + 1 < self.layers
        return [
            ((b == 0) & (i == 3) & early, q + 1, 0),
            ((b == 0) & (i < 3) & (q > 0), q, i + 1),
            ((b == 1) & (i < 3) & (q == 0), q, i + 1),
        ]

    def push_parts(self, q, s):
        stream, units = self.stream, self.stream.order
        there, more = self.layer_at(q + 1), q + 1 < self.layers
        if not self.keep:

            @pl.when((s == 0) & more)
            def _():
                stream.push_in(there, (2, 3), units[:2])
                stream.push_out(there, (1,))

            @pl.when((s == 1) & more)
            def _():
                stream.push_out(there, (3,))

            @pl.when((s == 6) & more)
            def _():
                stream.push_in(there, (2, 3), units[2:])

            return

        @pl.when((s == 0) & (q > 0) | (s == 3) & (q == 0))
        def _():
            stream.relay_out(self.layer_at(q))

        @pl.when((s == 0) & more)
        def _():
            stream.push_in(there, (1, 2), units)

        @pl.when(((s == 0) & (q > 0) | (s == 3) & (q == 0)) & more)
        def _():
            stream.push_out(there, (1, 2))

        @pl.when((s == 5) & more)
        def _():
            for unit in units:
                stream.relay_in(there, unit)

    def before(self, q, s):
        i, b = half(s), odd(s)
        more = q + 1 < self.layers

        @pl.when((s == 0) & (q > 0))
        def _():
            self.stream.pushed(self.layer_at(q - 1), self.keep)

        @pl.when((s == 0) & more)
        def _():
            for at, device in enumerate(self.place.peers()):
                notify(self.credit.at[at], device)
            for at in range(3):
                await_one(self.credit.at[at])

        self.push_parts(q, s)
        for condition, count, unit in self.sends(q, s):

            @pl.when(condition)
            def _():
                self.stream.forward(self.layer_at(count), self.unit_at(unit))

        @pl.when(b == 0)
        def _():
            self.load(q, i, 1)

        early = more & (q > 0) if self.keep else more
        for condition, count, unit in (((b == 1) & (i < 3), q, i + 1), ((s == 7) & early, q + 1, 0)):

            @pl.when(condition)
            def _():
                self.stream.arrive(self.layer_at(count), self.unit_at(unit))
                self.load(count, unit, 0)

        self.stream.loaded(self.w_in_v, self.w_out_v, b, self.load_sem)

    def after(self, q, s):
        for condition, count, unit in self.sends(q, s):

            @pl.when(condition)
            def _():
                self.stream.forwarded(self.layer_at(count), self.unit_at(unit))

        if self.keep:

            @pl.when((s == 7) & (q == 0) & (q + 1 < self.layers))
            def _():
                self.first_chunk(q + 1)


def when(condition):
    if isinstance(condition, bool):
        return lambda body: body() if condition else None
    return pl.when(condition)


def both(*conditions):
    kept = [c for c in conditions if not (isinstance(c, bool) and c)]
    if any(isinstance(c, bool) for c in kept):
        return False
    if not kept:
        return True
    return functools.reduce(lambda a, b: a & b, kept)


BACKWARD_UNITS = (1, 3, 2, 0)


def backward_mask(unit):
    if isinstance(unit, int):
        return BACKWARD_UNITS[unit]
    return (1 - half(unit)) + 2 * lax.rem(half(unit + 1), 2)


class Reduce:
    PARTS = ((0, 1), (0, 0), (1, 1), (1, 0))
    SECOND = (0, 1, 3, 4)

    def __init__(self, place, layers, hbm, vmem, sems, outs):
        self.place, self.layers = place, layers
        self.p_out, self.o_a, self.o_b, self.u_out, self.q_in, self.i_a, self.s_in, self.i_b = hbm
        self.r_v, self.gt_v, self.gm_v, self.o_v, self.it_v, self.out_a, self.out_b, self.in_a, self.in_b = vmem
        (
            self.to_send,
            self.to_recv,
            self.ti_send,
            self.ti_recv,
            self.oa_send,
            self.oa_recv,
            self.ob_send,
            self.ob_recv,
            self.ia_send,
            self.ia_recv,
            self.ib_send,
            self.ib_recv,
            self.p_sem,
            self.q_sem,
            self.out_sem,
            self.in_sem,
            self.out_save,
            self.in_save,
            self.credit_o,
            self.credit_i,
        ) = sems
        self.gw_in, self.gw_out = outs
        self.half_out = self.out_a.shape[1]
        self.side = self.in_a.shape[0] // 2
        self.row = self.side // 2
        self.chunk = self.in_a.shape[1]

    def slot(self, q):
        return q % 2 if isinstance(q, int) else odd(q)

    def twin_out(self):
        return remote(self.r_v, self.o_v, self.to_send, self.to_recv, self.place.twin())

    def twin_in(self, b):
        return remote(self.gt_v, self.it_v.at[b], self.ti_send.at[b], self.ti_recv.at[b], self.place.twin())

    def across_x_out(self, q, i, h):
        s = self.slot(q)
        return remote(self.p_out.at[s, i, h], self.o_a.at[s, i, h], self.oa_send.at[i, h], self.oa_recv.at[s, i, h], self.place.across(1))

    def across_y_out(self, q, h):
        s = self.slot(q)
        return remote(self.u_out.at[s, h], self.o_b.at[s, h], self.ob_send.at[h], self.ob_recv.at[s, h], self.place.across(2))

    def across_y_in(self, q, i, b):
        s, far = self.slot(q), pl.ds(pl.multiple_of((1 - self.place.chip_y) * self.side, self.side), self.side)
        there = i + 1 - 2 * (i % 2)
        return remote(
            self.q_in.at[s, i, b, far], self.i_a.at[s, there, b], self.ia_send.at[i, b], self.ia_recv.at[s, there, b], self.place.across(2)
        )

    def across_x_in(self, q, i, b):
        s, far = self.slot(q), pl.ds(pl.multiple_of((1 - self.place.chip_x) * self.row, self.row), self.row)
        there = 3 - i
        return remote(
            self.s_in.at[s, i, b, far], self.i_b.at[s, there, b], self.ib_send.at[i, b], self.ib_recv.at[s, there, b], self.place.across(1)
        )

    def resend(self, q, copy_of):
        @when(q > 0)
        def _():
            copy_of(q).wait_send()

        copy_of(q).start()

    def save_p(self, q, i):
        s = self.slot(q)
        return [
            pltpu.make_async_copy(self.r_v.at[:, pl.ds(h * self.half_out, self.half_out)], self.p_out.at[s, i, h], self.p_sem.at[h])
            for h in range(TWO)
        ]

    def save_q(self, q, i, b, gm):
        return pltpu.make_async_copy(self.gm_v.at[gm], self.q_in.at[self.slot(q), i, b], self.q_sem.at[b])

    def out_loads(self, a, b):
        return [pltpu.make_async_copy(a, self.out_a, self.out_sem.at[0]), pltpu.make_async_copy(b, self.out_b, self.out_sem.at[1])]

    def out_first(self, q):
        return self.out_loads(self.o_a.at[self.slot(q), 0, 0], self.o_a.at[self.slot(q), 0, 1])

    def out_second(self, q, h):
        s = self.slot(q)
        return self.out_loads(self.p_out.at[s, 2, h], self.o_a.at[s, 1, h])

    def out_third(self, q, h):
        s = self.slot(q)
        return self.out_loads(self.p_out.at[s, 3, h], self.o_b.at[s, h])

    def out_second_save(self, q, h):
        return pltpu.make_async_copy(self.out_a, self.u_out.at[self.slot(q), h], self.out_save)

    def out_third_save(self, q, h):
        n = self.layers - 1 - q
        return pltpu.make_async_copy(self.out_a, self.gw_out.at[n, :, pl.ds(h * self.half_out, self.half_out)], self.out_save)

    def in_second(self, q, pair, b):
        s, near = self.slot(q), pl.ds(pl.multiple_of(self.place.chip_y * self.side, self.side), self.side)
        copies = []
        for at in range(TWO):
            i, rows = TWO * pair + at, pl.ds(at * self.side, self.side)
            copies.append(pltpu.make_async_copy(self.q_in.at[s, i, b, near], self.in_a.at[rows], self.in_sem.at[0, at]))
            copies.append(pltpu.make_async_copy(self.i_a.at[s, i, b], self.in_b.at[rows], self.in_sem.at[1, at]))
        return copies

    def in_third(self, q, b):
        s, near = self.slot(q), pl.ds(pl.multiple_of(self.place.chip_x * self.row, self.row), self.row)
        copies = []
        for i in range(CHIPS):
            rows = pl.ds(i * self.row, self.row)
            copies.append(pltpu.make_async_copy(self.s_in.at[s, i, b, near], self.in_a.at[rows], self.in_sem.at[0, i]))
            copies.append(pltpu.make_async_copy(self.i_b.at[s, i, b], self.in_b.at[rows], self.in_sem.at[1, i]))
        return copies

    def in_second_save(self, q, pair, b):
        s = self.slot(q)
        return [
            pltpu.make_async_copy(self.in_a.at[pl.ds(at * self.side, self.side)], self.s_in.at[s, TWO * pair + at, b], self.in_save.at[at])
            for at in range(TWO)
        ]

    def in_third_save(self, q, b):
        n = self.layers - 1 - q
        core = self.place.core
        copies = []
        for i in range(CHIPS):
            shard = 2 * self.place.chip_at(BACKWARD_UNITS[i]) + (core if b else 1 - core)
            columns = pl.ds(pl.multiple_of(shard * self.chunk, self.chunk), self.chunk)
            copies.append(pltpu.make_async_copy(self.in_a.at[pl.ds(i * self.row, self.row)], self.gw_in.at[n, :, columns], self.in_save.at[i]))
        return copies

    def add(self, a, b):
        for start in range(0, a.shape[0], ADD_ROWS):
            rows = pl.ds(start, ADD_ROWS)
            a[rows, :] = a[rows, :] + b[rows, :]

    def free(self, semaphore):
        notify(semaphore, self.place.twin())

    def start(self):
        for semaphore in (self.credit_o, self.credit_i.at[0], self.credit_i.at[1]):
            self.free(semaphore)

    def mid(self, q, s):
        here, older, prev = q < self.layers, q > 0, q - 1

        for t in range(STEPS):
            i, b = divmod(t, TWO)
            layer, real = (q, here) if t < 7 else (prev, older)

            @when(both(s == (t + 1) % STEPS, real))
            def _():
                self.twin_in(b).wait_send()
                if b == 0:
                    self.twin_out().wait_send()
                    return
                for copy in self.save_p(layer, i):
                    copy.wait()
                self.save_q(layer, i, 1, 0).wait()

            layer, real = (q, here) if t < 5 else (prev, older)
            if b == 0:

                @when(both(s == (t + 3) % STEPS, real))
                def _():
                    self.save_q(layer, i, 0, 0).wait()

        for (pair, b), step in zip(self.PARTS, self.SECOND):

            @when(both(s == step + 1, older))
            def _():
                for copy in self.in_second_save(prev, pair, b):
                    copy.wait()
                for at in range(TWO):
                    self.resend(prev, lambda q, at=at: self.across_x_in(q, TWO * pair + at, b))

        for i in range(CHIPS):
            layer, real = (q, here) if i < 3 else (prev, older)

            @when(both(s == (2 * i + 3) % STEPS, real))
            def _():
                for b in (1, 0):
                    self.resend(layer, lambda q, b=b: self.across_y_in(q, i, b))

        for at in range(CHIPS):

            @when(both(s == 3 + at, here))
            def _():
                i, h = divmod(at, TWO)
                self.resend(q, lambda q: self.across_x_out(q, i, h))

        for h in range(TWO):

            @when(both(s == 1 + h, older))
            def _():
                self.out_second_save(prev, h).wait()

            @when(both(s == 2 + 2 * h, older))
            def _():
                self.resend(prev, lambda q: self.across_y_out(q, h))

            @when(both(s == 5 + 2 * h, older))
            def _():
                self.out_third_save(prev, h).wait()

        @when(both(s == 7, older))
        def _():
            for copy in self.in_third_save(prev, 1):
                copy.wait()

        @when(both(s == 0, q > 1))
        def _():
            for copy in self.in_third_save(q - 2, 0):
                copy.wait()

        for (pair, b), step in zip(self.PARTS, self.SECOND):

            @when(both(s == step, older))
            def _():
                for at in range(TWO):
                    self.across_y_in(prev, TWO * pair + 1 - at, b).wait_recv()
                for copy in self.in_second(prev, pair, b):
                    copy.start()

        for b in range(TWO):

            @when(both(s == 7 - b, older))
            def _():
                for i in range(CHIPS):
                    self.across_x_in(prev, 3 - i, b).wait_recv()
                for copy in self.in_third(prev, b):
                    copy.start()

        @when(both(s == 7, here))
        def _():
            for h in range(TWO):
                self.across_x_out(q, 0, h).wait_recv()
            for copy in self.out_first(q):
                copy.start()

        for h in range(TWO):

            @when(both(s == h, older))
            def _():
                self.across_x_out(prev, 1, h).wait_recv()
                for copy in self.out_second(prev, h):
                    copy.start()

            @when(both(s == 4 + 2 * h, older))
            def _():
                self.across_y_out(prev, h).wait_recv()
                for copy in self.out_third(prev, h):
                    copy.start()

    def end(self, q, s, gm):
        here, older, prev = q < self.layers, q > 0, q - 1
        old = (gm + 1) % 3 if isinstance(gm, int) else lax.rem(gm + 1, 3)

        for t in range(STEPS):
            i, b = divmod(t, TWO)

            @when(both(s == t, here))
            def _():
                more = True if i < 3 else q < self.layers - 1
                await_one(self.credit_i.at[b])
                self.twin_in(b).start()
                if b == 0:
                    await_one(self.credit_o)
                    self.twin_out().start()
                    return
                self.twin_out().wait_recv()
                self.add(self.r_v, self.o_v)

                @when(more)
                def _():
                    self.free(self.credit_o)

                if i == 3:
                    for copy in self.out_first(q):
                        copy.wait()
                    for start in range(0, self.r_v.shape[0], ADD_ROWS):
                        rows = pl.ds(start, ADD_ROWS)
                        for h, part in enumerate((self.out_a, self.out_b)):
                            columns = pl.ds(h * self.half_out, self.half_out)
                            self.r_v[rows, columns] = self.r_v[rows, columns] + part[rows, :]
                for copy in self.save_p(q, i):
                    copy.start()
                self.twin_in(0).wait_recv()
                self.add(self.gm_v.at[gm], self.it_v.at[0])

                @when(more)
                def _():
                    self.free(self.credit_i.at[0])

                self.save_q(q, i, 1, gm).start()

            if b == 0:
                layer, real = (q, here) if t < 6 else (prev, older)

                @when(both(s == (t + 2) % STEPS, real))
                def _():
                    self.twin_in(1).wait_recv()
                    self.add(self.gm_v.at[old], self.it_v.at[1])

                    @when(True if i < 3 else layer < self.layers - 1)
                    def _():
                        self.free(self.credit_i.at[1])

                    self.save_q(layer, i, 0, old).start()

        def summed(parts, loads, saves):
            for copy in loads:
                copy.wait()
            self.add(*parts)
            for copy in saves:
                copy.start()

        ins, outs = (self.in_a, self.in_b), (self.out_a, self.out_b)
        for (pair, b), step in zip(self.PARTS, self.SECOND):

            @when(both(s == step, older))
            def _():
                summed(ins, self.in_second(prev, pair, b), self.in_second_save(prev, pair, b))

        for b in range(TWO):

            @when(both(s == 7 - b, older))
            def _():
                summed(ins, self.in_third(prev, b), self.in_third_save(prev, b))

            @when(both(s == b, older))
            def _():
                summed(outs, self.out_second(prev, b), [self.out_second_save(prev, b)])

            @when(both(s == 4 + 2 * b, older))
            def _():
                summed(outs, self.out_third(prev, b), [self.out_third_save(prev, b)])

    def finish(self):
        q = self.layers
        last = q - 1
        for s in range(STEPS):
            self.mid(q, s)
            self.end(q, s, (STEPS * q + s) % 3)
        for copy in self.in_third_save(last, 0):
            copy.wait()
        for h in range(TWO):
            for i in range(TWO):
                self.across_x_out(last, i, h).wait_send()
            self.across_y_out(last, h).wait_send()
        for b in range(TWO):
            for i in range(CHIPS):
                self.across_y_in(last, i, b).wait_send()
                self.across_x_in(last, i, b).wait_send()


def forward_stack_kernel(layers, x_ref, w_in_ref, w_out_ref, *refs):
    xs_ref, own_in, own_out, kept_in, kept_out, got_in, got_out, twin_in, twin_out = refs[:9]
    x_v, unit_v, total_v, w_in_v, w_out_v, stage_in, stage_out = refs[9:16]
    x_sem, load_sem, stage_sem, credit = refs[16:20]
    place = Place()
    stream = Stream(place, (0, 1, 2, 3), own_in, own_out, kept_in, kept_out, got_in, got_out, twin_in, twin_out, refs[20:])
    pace = Pace(place, stream, layers, lambda q: q, lambda i: i, True, (w_in_v, w_out_v, load_sem), credit)
    tokens, width = x_v.shape
    tiles = tokens // TOK_TILE

    pairs = ((w_in_ref, stage_in, own_in, 0), (w_out_ref, stage_out, own_out, 1))

    def to_lanes(n, phase):
        for src, stage, own, at in pairs:
            if phase == 0:
                for b in range(stage.shape[0]):
                    pltpu.make_async_copy(src.at[n, :, pl.ds(b * LANES, LANES)], stage.at[b], stage_sem.at[at]).start()
            elif phase == 1:
                pltpu.make_async_copy(own.at[n], stage, stage_sem.at[at]).wait()
                pltpu.make_async_copy(stage, own.at[n], stage_sem.at[at]).start()
            else:
                pltpu.make_async_copy(stage, own.at[n], stage_sem.at[at]).wait()

    fetch = pltpu.make_async_copy(x_ref, x_v, x_sem)
    for phase in range(3):
        to_lanes(0, phase)
    fetch.start()
    meet(place)
    pace.head()
    for phase in range(3):
        to_lanes(1, phase)
    fetch.wait()

    def first_unit(t, carry):
        rows = tile_rows(t)
        x_wide, inv_rms = unit_rows_of(x_v[rows, :])
        put_tile(unit_v, rows, (x_wide * inv_rms).astype(BF16))
        total_v[rows, :] = jnp.zeros((TOK_TILE, width), F32)
        return carry

    lax.fori_loop(0, tiles, first_unit, 0)
    pace.head_end()

    def save(n):
        return pltpu.make_async_copy(x_v, xs_ref.at[n], x_sem)

    def compute(v, last):
        w_in, w_out = lane_join(w_in_v.at[v]), lane_join(w_out_v.at[v])
        pending = []

        def finish():
            t, hidden = pending.pop(0)
            rows = pl.ds(t * TOK_TILE, TOK_TILE)
            total = total_v[rows, :] + jnp.dot(hidden, w_out, preferred_element_type=F32)
            if not last:
                total_v[rows, :] = total
                return
            x_next = (x_v[rows, :].astype(F32) + total).astype(BF16)
            x_v[rows, :] = x_next
            total_v[rows, :] = jnp.zeros((TOK_TILE, width), F32)
            x_wide, inv_rms = unit_rows_of(x_next)
            put_tile(unit_v, rows, (x_wide * inv_rms).astype(BF16))

        for t in range(tiles):
            unit = tile_of(unit_v, pl.ds(t * TOK_TILE, TOK_TILE))
            pre = jnp.dot(unit, w_in, preferred_element_type=F32).astype(BF16).astype(F32)
            tanh = jnp.tanh(pre * (GELU_A + GELU_B * (pre * pre)))
            pending.append((t, (pre * (0.5 * tanh + 0.5)).astype(BF16)))
            if len(pending) > 1:
                finish()
        while pending:
            finish()

    def step(n, s):
        v = odd(s)
        pace.before(n, s)
        for phase in range(3):

            @pl.when((s == 1 + phase) & (n + 2 < layers))
            def _():
                to_lanes(n + 2, phase)

        @pl.when(s < 7)
        def _():
            compute(v, False)

        @pl.when(s == 7)
        def _():
            @pl.when(n > 0)
            def _():
                save(n - 1).wait()

            compute(v, True)
            save(n).start()

        pace.after(n, s)

    def layer_step(n, carry):
        lax.fori_loop(0, STEPS, lambda s, c: (step(n, s), c)[1], 0)
        return carry

    lax.fori_loop(0, layers, layer_step, 0)
    stream.pushed(layers - 1, True)
    save(layers - 1).wait()


def backward_stack_kernel(layers, x_ref, xs_ref, dy_ref, own_in, own_out, kept_in, kept_out, *refs):
    gw_in, gw_out, dx_ref, got_in, got_out, twin_in, twin_out = refs[:7]
    sums_hbm = refs[7:15]
    unit_v, dy_v, du_v, hidden_v, dpre_v, w_in_v, w_out_v, x_v = refs[15:23]
    sums_v = refs[23:32]
    row_sem, x_sem, load_sem, credit = refs[32:36]
    stream_sems, sum_sems = refs[36:44], refs[44:]
    place = Place()
    stream = Stream(place, BACKWARD_UNITS, own_in, own_out, kept_in, kept_out, got_in, got_out, twin_in, twin_out, stream_sems)
    pace = Pace(place, stream, layers, lambda q: layers - 1 - q, backward_mask, False, (w_in_v, w_out_v, load_sem), credit)
    sums = Reduce(place, layers, sums_hbm, sums_v, sum_sems, (gw_in, gw_out))
    r_v, gt_v, gm_v = sums_v[:3]
    blocks_d, tokens, _ = unit_v.shape
    width = blocks_d * LANES
    tiles = tokens // TOK_TILE

    meet(place)
    pace.head()
    sums.start()

    def rows_copies(to_vmem, ref):
        copies = []
        for b in range(blocks_d):
            pair = (ref.at[:, pl.ds(b * LANES, LANES)], dy_v.at[b])
            copies.append(pltpu.make_async_copy(*(pair if to_vmem else pair[::-1]), row_sem.at[b]))
        return copies

    dy_copies = rows_copies(True, dy_ref)
    for copy in dy_copies:
        copy.start()

    def fetch(n, which, t):
        dst, sem = x_v.at[which, odd(t)], x_sem.at[which, odd(t)]

        @pl.when(n > 0)
        def _():
            pltpu.make_async_copy(xs_ref.at[n - 1, tile_rows(t)], dst, sem).start()

        @pl.when(n == 0)
        def _():
            pltpu.make_async_copy(x_ref.at[tile_rows(t)], dst, sem).start()

    def fetched(which, t):
        at = odd(t)
        pltpu.make_async_copy(x_ref.at[tile_rows(0)], x_v.at[which, at], x_sem.at[which, at]).wait()
        return x_v[which, at]

    def first_unit(t, carry):
        @pl.when(t + 1 < tiles)
        def _():
            fetch(layers - 1, 1, t + 1)

        rows = tile_rows(t)
        x_wide, inv_rms = unit_rows_of(fetched(1, t))
        put_tile(unit_v, rows, (x_wide * inv_rms).astype(BF16))
        du_v[rows, :] = jnp.zeros((TOK_TILE, width), F32)
        return carry

    fetch(layers - 1, 1, 0)
    lax.fori_loop(0, tiles, first_unit, 0)
    for copy in dy_copies:
        copy.wait()
    pace.head_end()

    def hidden_part(v):
        w_in, w_out = lane_join(w_in_v.at[v]), lane_join(w_out_v.at[v])
        pending = []

        def finish():
            t, dpre = pending.pop(0)
            rows = pl.ds(t * TOK_TILE, TOK_TILE)
            du_v[rows, :] = du_v[rows, :] + lax.dot_general(dpre, w_in, LAST_LAST, preferred_element_type=F32)

        for t in range(tiles):
            rows = pl.ds(t * TOK_TILE, TOK_TILE)
            pre = jnp.dot(tile_of(unit_v, rows), w_in, preferred_element_type=F32).astype(BF16).astype(F32)
            dhidden = lax.dot_general(tile_of(dy_v, rows), w_out, LAST_LAST, preferred_element_type=F32)
            poly = GELU_A + GELU_B * (pre * pre)
            cdf = 0.5 * jnp.tanh(pre * poly) + 0.5
            hidden = pre * cdf
            slope = cdf + (hidden * (6.0 * poly - 4.0 * GELU_A)) * (1.0 - cdf)
            dpre = (slope * dhidden).astype(BF16)
            put_tile(hidden_v, rows, hidden.astype(BF16))
            put_tile(dpre_v, rows, dpre)
            pending.append((t, dpre))
            if len(pending) > 1:
                finish()
        while pending:
            finish()

    def gradient_part(gm):
        r_v[...] = lax.dot_general(lane_join(hidden_v), lane_join(dy_v), FIRST_FIRST, preferred_element_type=F32)
        dpre = lane_join(dpre_v)

        def unit_of(parity):
            per = blocks_d // SHARDS
            parts = [unit_v[(2 * c + parity) * per + b] for c in range(CHIPS) for b in range(per)]
            return jnp.concatenate(parts, axis=1)

        gt_v[...] = lax.dot_general(unit_of(1 - place.core), dpre, FIRST_FIRST, preferred_element_type=F32)
        gm_v[gm] = lax.dot_general(unit_of(place.core), dpre, FIRST_FIRST, preferred_element_type=F32)

    def step(q, s):
        gm = lax.rem(STEPS * q + s, 3)
        pace.before(q, s)
        hidden_part(odd(s))
        sums.mid(q, s)
        gradient_part(gm)
        sums.end(q, s, gm)
        pace.after(q, s)

    def layer_step(q, carry):
        n = layers - 1 - q
        lax.fori_loop(0, STEPS, lambda s, c: (step(q, s), c)[1], 0)
        fetch(n, 0, 0)

        @pl.when(n > 0)
        def _():
            fetch(n - 1, 1, 0)

        def close(t, carry):
            @pl.when(t + 1 < tiles)
            def _():
                fetch(n, 0, t + 1)

                @pl.when(n > 0)
                def _():
                    fetch(n - 1, 1, t + 1)

            rows = tile_rows(t)
            x_wide, inv_rms = unit_rows_of(fetched(0, t))
            value, du = x_wide * inv_rms, du_v[rows, :]
            row_mean = jnp.mean(du * value, axis=-1, keepdims=True)
            put_tile(dy_v, rows, (tile_of(dy_v, rows).astype(F32) + inv_rms * (du - value * row_mean)).astype(BF16))
            du_v[rows, :] = jnp.zeros((TOK_TILE, width), F32)

            @pl.when(n > 0)
            def _():
                x_wide, inv_rms = unit_rows_of(fetched(1, t))
                put_tile(unit_v, rows, (x_wide * inv_rms).astype(BF16))

            return carry

        lax.fori_loop(0, tiles, close, 0)
        return carry

    lax.fori_loop(0, layers, layer_step, 0)
    dx_copies = rows_copies(False, dx_ref)
    for copy in dx_copies:
        copy.start()
    sums.finish()
    stream.pushed(0, False)
    for copy in dx_copies:
        copy.wait()


def stream_semaphores():
    dma = pltpu.SemaphoreType.DMA
    return [dma((TWO, 3, CHIPS))] * TWO + [dma((TWO, 3))] * TWO + [dma((CHIPS, CHIPS)), dma((TWO, CHIPS, CHIPS)), dma((CHIPS,)), dma((TWO, CHIPS))]


def sum_semaphores():
    dma, regular = pltpu.SemaphoreType.DMA, pltpu.SemaphoreType.REGULAR
    return [
        dma,
        dma,
        dma((TWO,)),
        dma((TWO,)),
        dma((TWO, TWO)),
        dma((TWO, TWO, TWO)),
        dma((TWO,)),
        dma((TWO, TWO)),
        dma((CHIPS, TWO)),
        dma((TWO, CHIPS, TWO)),
        dma((CHIPS, TWO)),
        dma((TWO, CHIPS, TWO)),
        dma((TWO,)),
        dma((TWO,)),
        dma((TWO,)),
        dma((TWO, CHIPS)),
        dma,
        dma((CHIPS,)),
        regular,
        regular((TWO,)),
    ]


def stream_buffers(piece_in, piece_out):
    return [
        jax.ShapeDtypeStruct((TWO, TWO) + piece_in, BF16),
        jax.ShapeDtypeStruct((TWO, TWO) + piece_out, BF16),
        jax.ShapeDtypeStruct((TWO, CHIPS) + piece_in, BF16),
        jax.ShapeDtypeStruct((TWO, CHIPS) + piece_out, BF16),
    ]


ANYWHERE = pl.BlockSpec(memory_space=pl.ANY)


def forward_stack(x_rows, w_in, w_out):
    layers, depth, hidden_size = w_in.shape
    tokens, width = x_rows.shape
    chunk = w_out.shape[1]
    piece_in, piece_out = (hidden_size // LANES, depth, LANES), (width // LANES, chunk, LANES)
    pieces = [jax.ShapeDtypeStruct((layers,) + piece, BF16) for piece in (piece_in, piece_out)]
    shapes = [jax.ShapeDtypeStruct((layers, tokens, width), BF16)] + pieces * 2 + stream_buffers(piece_in, piece_out)
    outs = pl.pallas_call(
        functools.partial(forward_stack_kernel, layers),
        in_specs=[ANYWHERE] * 3,
        out_specs=[ANYWHERE] * len(shapes),
        out_shape=shapes,
        scratch_shapes=[
            pltpu.VMEM((tokens, width), BF16),
            pltpu.VMEM((width // LANES, tokens, LANES), BF16),
            pltpu.VMEM((tokens, width), F32),
            pltpu.VMEM((TWO, chunk // LANES, width, LANES), BF16),
            pltpu.VMEM((TWO, width // LANES, chunk, LANES), BF16),
            pltpu.VMEM(piece_in, BF16),
            pltpu.VMEM(piece_out, BF16),
            pltpu.SemaphoreType.DMA,
            pltpu.SemaphoreType.DMA((TWO, SHARDS + 1)),
            pltpu.SemaphoreType.DMA((TWO,)),
            pltpu.SemaphoreType.REGULAR((3,)),
        ]
        + stream_semaphores(),
        compiler_params=pltpu.CompilerParams(vmem_limit_bytes=VMEM_LIMIT, collective_id=0, has_side_effects=True),
        cost_estimate=pl.CostEstimate(flops=4 * layers * tokens * width * hidden_size, bytes_accessed=100_000_000, transcendentals=0),
        name="forward_stack",
    )(x_rows, w_in, w_out)
    return outs[:5]


def backward_stack(x_rows, xs, grad_rows, own_in, own_out, kept_in, kept_out):
    layers, blocks_f, depth, _ = own_in.shape
    blocks_d, chunk = own_out.shape[1], own_out.shape[2]
    tokens, width = x_rows.shape
    half, quarter = width // 2, width // 4
    hidden_size = blocks_f * LANES

    def sums(*shape):
        return jax.ShapeDtypeStruct(shape, F32)

    shapes = (
        [sums(layers, depth, hidden_size), sums(layers, chunk, width), jax.ShapeDtypeStruct((tokens, width), BF16)]
        + stream_buffers(own_in.shape[1:], own_out.shape[1:])
        + [
            sums(TWO, CHIPS, TWO, chunk, half),
            sums(TWO, TWO, TWO, chunk, half),
            sums(TWO, TWO, chunk, half),
            sums(TWO, TWO, chunk, half),
            sums(TWO, CHIPS, TWO, half, chunk),
            sums(TWO, CHIPS, TWO, quarter, chunk),
            sums(TWO, CHIPS, TWO, quarter, chunk),
            sums(TWO, CHIPS, TWO, depth, chunk),
        ]
    )
    outs = pl.pallas_call(
        functools.partial(backward_stack_kernel, layers),
        in_specs=[ANYWHERE] * 7,
        out_specs=[ANYWHERE] * len(shapes),
        out_shape=shapes,
        scratch_shapes=[
            pltpu.VMEM((blocks_d, tokens, LANES), BF16),
            pltpu.VMEM((blocks_d, tokens, LANES), BF16),
            pltpu.VMEM((tokens, width), F32),
            pltpu.VMEM((chunk // LANES, tokens, LANES), BF16),
            pltpu.VMEM((chunk // LANES, tokens, LANES), BF16),
            pltpu.VMEM((TWO, chunk // LANES, width, LANES), BF16),
            pltpu.VMEM((TWO, blocks_d, chunk, LANES), BF16),
            pltpu.VMEM((TWO, TWO, TOK_TILE, width), BF16),
            pltpu.VMEM((chunk, width), F32),
            pltpu.VMEM((half, chunk), F32),
            pltpu.VMEM((3, half, chunk), F32),
            pltpu.VMEM((chunk, width), F32),
            pltpu.VMEM((TWO, half, chunk), F32),
            pltpu.VMEM((chunk, half), F32),
            pltpu.VMEM((chunk, half), F32),
            pltpu.VMEM((half, chunk), F32),
            pltpu.VMEM((half, chunk), F32),
            pltpu.SemaphoreType.DMA((blocks_d,)),
            pltpu.SemaphoreType.DMA((TWO, TWO)),
            pltpu.SemaphoreType.DMA((TWO, SHARDS + 1)),
            pltpu.SemaphoreType.REGULAR((3,)),
        ]
        + stream_semaphores()
        + sum_semaphores(),
        compiler_params=pltpu.CompilerParams(vmem_limit_bytes=VMEM_LIMIT, collective_id=1, has_side_effects=True),
        cost_estimate=pl.CostEstimate(flops=10 * layers * tokens * width * hidden_size, bytes_accessed=300_000_000, transcendentals=0),
        name="backward_stack",
    )(x_rows, xs, grad_rows, own_in, own_out, kept_in, kept_out)
    return outs[:3]


def solution(mesh):
    row_spec = P(("local", "data"), None)
    weight_spec = P(None, ("local", "data"), None)

    def device_step(x_rows, grad_rows, w_in, w_out):
        xs, own_in, own_out, kept_in, kept_out = forward_stack(x_rows, w_in, w_out)
        gw_in, gw_out, dx = backward_stack(x_rows, xs, grad_rows, own_in, own_out, kept_in, kept_out)
        return xs[w_in.shape[0] - 1], gw_in, gw_out, dx

    return jax.shard_map(
        device_step,
        mesh=mesh,
        in_specs=(row_spec, row_spec, weight_spec, weight_spec),
        out_specs=(row_spec, weight_spec, weight_spec, row_spec),
        check_vma=False,
    )
```

```python
import functools

import jax
import jax.numpy as jnp
from jax import lax
from jax.experimental import pallas as pl
from jax.experimental.pallas import tpu as pltpu
from jax.sharding import PartitionSpec as P

NORM_EPS = 1e-6
GELU_A = 0.7978845608028654
GELU_B = GELU_A * 0.044715
LAST_LAST = (((1,), (1,)), ((), ()))
FIRST_FIRST = (((0,), (0,)), ((), ()))
BF16 = jnp.bfloat16
F32 = jnp.float32
MESH = pl.DeviceIdType.MESH

TWO = 2
CHIPS = 4
STEPS = 8
SHARDS = 8
LANES = 128
TOK_TILE = 256
VMEM_LIMIT = 67_000_000
ADD_ROWS = 64


def unit_rows_of(x_tile):
    x_wide = x_tile.astype(F32)
    inv_rms = lax.rsqrt(jnp.mean(x_wide * x_wide, axis=-1, keepdims=True) + NORM_EPS)
    return x_wide, inv_rms


def lane_join(ref):
    return jnp.concatenate([ref[b] for b in range(ref.shape[0])], axis=1)


def tile_of(ref, rows):
    return jnp.concatenate([ref[b, rows, :] for b in range(ref.shape[0])], axis=1)


def put_tile(ref, rows, value):
    for b in range(ref.shape[0]):
        ref[b, rows, :] = value[:, b * LANES : (b + 1) * LANES]


def tile_rows(t):
    return pl.ds(pl.multiple_of(t * TOK_TILE, TOK_TILE), TOK_TILE)


def odd(x):
    return x % TWO if isinstance(x, int) else lax.rem(x, TWO)


def half(x):
    return x // TWO if isinstance(x, int) else lax.div(x, TWO)


def when(condition):
    if isinstance(condition, bool):
        return lambda body: body() if condition else None
    return pl.when(condition)


def both(*conditions):
    kept = [c for c in conditions if not (isinstance(c, bool) and c)]
    if any(isinstance(c, bool) for c in kept):
        return False
    if not kept:
        return True
    return functools.reduce(lambda a, b: a & b, kept)


def by_step(s, body):
    for k in range(STEPS):

        @pl.when(s == k)
        def _():
            body(k)


def notify(semaphore, device):
    pl.semaphore_signal(semaphore, inc=1, device_id=device, device_id_type=MESH)


def await_one(semaphore):
    pl.semaphore_wait(semaphore, 1)


class Place:
    def __init__(self):
        self.chip = lax.axis_index("local")
        self.core = lax.axis_index("data")
        self.chip_x, self.chip_y = odd(self.chip), half(self.chip)

    def chip_at(self, mask):
        mask_x, mask_y = (mask % 2, mask // 2) if isinstance(mask, int) else (odd(mask), half(mask))
        return odd(self.chip_x + mask_x) + 2 * odd(self.chip_y + mask_y)

    def across(self, mask):
        return (self.chip_at(mask), self.core)

    def twin(self):
        return (self.chip, 1 - self.core)

    def peers(self):
        return [self.across(1), self.across(2), self.twin()]


def meet(place):
    barrier = pltpu.get_barrier_semaphore()
    for device in place.peers():
        notify(barrier, device)
    pl.semaphore_wait(barrier, 3)


def remote(src, dst, send_sem, recv_sem, device):
    return pltpu.make_async_remote_copy(
        src_ref=src, dst_ref=dst, send_sem=send_sem, recv_sem=recv_sem, device_id=device, device_id_type=MESH
    )


class Stream:
    def __init__(self, place, order, own_in, own_out, kept_in, kept_out, got_in, got_out, twin_in, twin_out, sems):
        self.place, self.order = place, order
        self.own_in, self.own_out, self.kept_in, self.kept_out = own_in, own_out, kept_in, kept_out
        self.got_in, self.got_out, self.twin_in, self.twin_out = got_in, got_out, twin_in, twin_out
        (self.in_send, self.in_recv, self.out_send, self.out_recv) = sems[:4]
        (self.twin_in_send, self.twin_in_recv, self.twin_out_send, self.twin_out_recv) = sems[4:]
        self.blocks = own_in.shape[1] // CHIPS

    def mine_in(self, n, mask, block, count):
        rows = pl.ds(block, count)
        if mask == 0:
            return self.own_in.at[n, rows]
        if mask == 1:
            return self.kept_in.at[n, rows]
        return self.got_in.at[odd(n), mask - 2, rows]

    def mine_out(self, n, mask):
        if mask == 0:
            return self.own_out.at[n]
        if mask == 2:
            return self.kept_out.at[n]
        return self.got_out.at[odd(n), (mask - 1) // 2]

    def send_in(self, n, mask, unit):
        there = 1 if mask == 1 else 2
        block = self.place.chip_at(there ^ unit) * self.blocks
        src = self.mine_in(n, 1 if mask == 3 else 0, block, self.blocks)
        dst = self.mine_in(n, mask, block, self.blocks)
        recv = self.in_recv.at[odd(n), mask - 1, unit]
        return remote(src, dst, self.in_send.at[odd(n), mask - 1, unit], recv, self.place.across(there))

    def got_slice(self, n, mask, unit):
        dst = self.mine_in(n, mask, self.place.chip_at(unit) * self.blocks, self.blocks)
        recv = self.in_recv.at[odd(n), mask - 1, unit]
        return remote(dst, dst, self.in_send.at[odd(n), mask - 1, unit], recv, self.place.across(1))

    def send_out(self, n, mask):
        src, dst = self.mine_out(n, 2 if mask == 3 else 0), self.mine_out(n, mask)
        recv = self.out_recv.at[odd(n), mask - 1]
        return remote(src, dst, self.out_send.at[odd(n), mask - 1], recv, self.place.across(2 if mask == 2 else 1))

    def push_in(self, n, masks, units):
        for unit in units:
            for mask in masks:
                self.send_in(n, mask, unit).start()

    def push_out(self, n, masks):
        for mask in masks:
            self.send_out(n, mask).start()

    def relay_in(self, n, unit):
        self.got_slice(n, 1, 2 ^ unit).wait_recv()
        self.send_in(n, 3, unit).start()

    def relay_out(self, n):
        self.send_out(n, 2).wait_recv()
        self.send_out(n, 3).start()

    def pushed(self, n, keep):
        for mask in (1, 2, 3) if keep else (2, 3):
            for unit in self.order:
                self.send_in(n, mask, unit).wait_send()
        for mask in (1, 2, 3) if keep else (1, 3):
            self.send_out(n, mask).wait_send()

    def twin_copies(self, n, unit):
        slot, block = odd(n), self.place.chip_at(unit) * self.blocks
        return [
            remote(
                self.mine_in(n, mask, block, self.blocks),
                self.twin_in.at[slot, mask, pl.ds(block, self.blocks)],
                self.twin_in_send.at[mask, unit],
                self.twin_in_recv.at[slot, mask, unit],
                self.place.twin(),
            )
            for mask in range(CHIPS)
        ]

    def twin_out_copy(self, n, mask, unit):
        slot = odd(n)
        recv = self.twin_out_recv.at[slot, unit]
        return remote(self.mine_out(n, mask), self.twin_out.at[slot, unit], self.twin_out_send.at[unit], recv, self.place.twin())

    def forward(self, n, unit):
        for mask in (2, 3):
            self.got_slice(n, mask, unit).wait_recv()
        for copy in self.twin_copies(n, unit):
            copy.start()
        for mask in range(CHIPS):

            @when(unit == mask)
            def _():
                if mask in (1, 3):
                    self.send_out(n, mask).wait_recv()
                self.twin_out_copy(n, mask, unit).start()

    def forwarded(self, n, unit):
        for copy in self.twin_copies(n, unit):
            copy.wait_send()
        self.twin_out_copy(n, 0, unit).wait_send()

    def arrive(self, n, unit):
        for copy in self.twin_copies(n, unit):
            copy.wait_recv()
        self.twin_out_copy(n, 0, unit).wait_recv()

    def load_in(self, n, unit, parity, w_in_v, v, sem):
        count, depth = self.blocks // 2, self.own_in.shape[2]
        block = self.place.chip_at(unit) * self.blocks + parity * count
        copies = []
        for mask in range(CHIPS):
            for which in range(TWO):
                shard = 2 * self.place.chip_at(mask) + (self.place.core if which == 0 else 1 - self.place.core)
                src = self.mine_in(n, mask, block, count) if which == 0 else self.twin_in.at[odd(n), mask, pl.ds(block, count)]
                row = pl.ds(pl.multiple_of(shard * depth, depth), depth)
                copies.append(pltpu.make_async_copy(src, w_in_v.at[v, :, row], sem.at[v, 2 * mask + which]))
        return copies

    def load(self, n, unit, mine, w_in_v, w_out_v, v, sem):
        parity = 1 - self.place.core - mine + 2 * self.place.core * mine
        for copy in self.load_in(n, unit, parity, w_in_v, v, sem):
            copy.start()
        last = sem.at[v, SHARDS]

        @when(mine == 0)
        def _():
            pltpu.make_async_copy(self.twin_out.at[odd(n), unit], w_out_v.at[v], last).start()

        for mask in range(CHIPS):

            @when(both(mine == 1, unit == mask))
            def _():
                pltpu.make_async_copy(self.mine_out(n, mask), w_out_v.at[v], last).start()

    def loaded(self, w_in_v, w_out_v, v, sem):
        for copy in self.load_in(0, 0, 0, w_in_v, v, sem):
            copy.wait()
        pltpu.make_async_copy(self.own_out.at[0], w_out_v.at[v], sem.at[v, SHARDS]).wait()


class Pace:
    def __init__(self, place, stream, layers, layer_at, unit_at, keep, bufs, credit):
        self.place, self.stream, self.layers, self.layer_at, self.unit_at = place, stream, layers, layer_at, unit_at
        self.keep, self.credit = keep, credit
        self.w_in_v, self.w_out_v, self.load_sem = bufs

    def load(self, q, i, b):
        self.stream.load(self.layer_at(q), self.unit_at(i), b, self.w_in_v, self.w_out_v, b, self.load_sem)

    def head(self):
        n, units = self.layer_at(0), self.stream.order
        if not self.keep:
            self.stream.push_in(n, (2, 3), units)
            self.stream.push_out(n, (3, 1))
            return
        self.stream.push_in(n, (1,), [units[at] for at in (0, 2, 3, 1)])
        self.stream.push_in(n, (2,), units[:1])
        self.stream.push_out(n, (1,))

    def head_end(self):
        n, units = self.layer_at(0), self.stream.order
        if not self.keep:
            self.first_chunk(0)
            return
        for at, unit in enumerate(units):
            if at:
                self.stream.push_in(n, (2,), (unit,))
            if at == 3:
                self.first_chunk(0)
            self.stream.relay_in(n, unit)
            if at == 1:
                self.stream.push_out(n, (2,))

    def first_chunk(self, q):
        n, unit = self.layer_at(q), self.unit_at(0)
        self.stream.forward(n, unit)
        self.stream.arrive(n, unit)
        self.load(q, 0, 0)
        self.stream.forwarded(n, unit)

    def sends(self, q, s):
        i, b = half(s), odd(s)
        early = (q + 1 < self.layers) & (q > 0) if self.keep else q + 1 < self.layers
        return [
            (both(s == 6, early), q + 1, 0),
            (both(b == 0 and i < 3, q > 0), q, i + 1),
            (both(b == 1 and i < 3, q == 0), q, i + 1),
        ]

    def push_parts(self, q, s):
        stream, units = self.stream, self.stream.order
        there, more = self.layer_at(q + 1), q + 1 < self.layers
        if not self.keep:

            for at, (step, mask) in enumerate(((1, 3), (4, 1))):

                @when(both(s == 3 * at, more))
                def _():
                    stream.push_in(there, (2, 3), units[TWO * at : TWO * at + TWO])

                @when(both(s == step, more))
                def _():
                    stream.push_out(there, (mask,))

            return

        turn = q > 0 if s == 0 else q == 0

        @when(both(s in (0, 3), turn))
        def _():
            stream.relay_out(self.layer_at(q))

        @when(both(s == 0, more))
        def _():
            stream.push_in(there, (1, 2), units)

        @when(both(s in (0, 3), turn, more))
        def _():
            stream.push_out(there, (1, 2))

        @when(both(s == 5, more))
        def _():
            for unit in units:
                stream.relay_in(there, unit)

    def before(self, q, s):
        i, b = half(s), odd(s)
        more = q + 1 < self.layers

        @when(both(s == 0, q > 0))
        def _():
            self.stream.pushed(self.layer_at(q - 1), self.keep)

        @when(both(s == 0, more))
        def _():
            for at, device in enumerate(self.place.peers()):
                notify(self.credit.at[at], device)
            for at in range(3):
                await_one(self.credit.at[at])

        self.push_parts(q, s)
        for condition, count, unit in self.sends(q, s):

            @when(condition)
            def _():
                self.stream.forward(self.layer_at(count), self.unit_at(unit))

        @when(b == 0)
        def _():
            self.load(q, i, 1)

        early = more & (q > 0) if self.keep else more
        for condition, count, unit in ((both(b == 1 and i < 3, q > 0), q, i + 1), (both(s == 7, early), q + 1, 0)):

            @when(condition)
            def _():
                self.stream.arrive(self.layer_at(count), self.unit_at(unit))
                self.load(count, unit, 0)

        self.stream.loaded(self.w_in_v, self.w_out_v, b, self.load_sem)

    def late(self, q, s):
        i, b = half(s), odd(s)

        @when(both(b == 1 and i < 3, q == 0))
        def _():
            self.stream.arrive(self.layer_at(q), self.unit_at(i + 1))
            self.load(q, i + 1, 0)

    def after(self, q, s):
        for condition, count, unit in self.sends(q, s):

            @when(condition)
            def _():
                self.stream.forwarded(self.layer_at(count), self.unit_at(unit))

        if self.keep:

            @when(both(s == 7, (q == 0) & (q + 1 < self.layers)))
            def _():
                self.first_chunk(q + 1)


BACKWARD_UNITS = (3, 2, 1, 0)


class Reduce:
    PARTS = ((0, 1), (0, 0), (1, 1), (1, 0))
    SECOND = (0, 1, 2, 4)
    THIRD = (7, 5)
    OUT = (4, 7)
    SENT = ((5, 5), (0, 1))
    NEXT = (1, 5)
    LAST = (3, 6)

    def __init__(self, place, layers, hbm, vmem, sems, outs):
        self.place, self.layers = place, layers
        self.p_out, self.o_a, self.o_b, self.u_out, self.q_in, self.i_a, self.s_in, self.i_b = hbm
        self.r_v, self.gt_v, self.gm_v, self.o_v, self.it_v, self.out_a, self.out_b, self.in_a, self.in_b = vmem
        (
            self.to_send,
            self.to_recv,
            self.ti_send,
            self.ti_recv,
            self.oa_send,
            self.oa_recv,
            self.ob_send,
            self.ob_recv,
            self.ia_send,
            self.ia_recv,
            self.ib_send,
            self.ib_recv,
            self.p_sem,
            self.q_sem,
            self.out_sem,
            self.in_sem,
            self.out_save,
            self.in_save,
            self.credit_o,
            self.credit_i,
        ) = sems
        self.gw_in, self.gw_out = outs
        self.half_out = self.out_a.shape[1]
        self.side = self.in_a.shape[0] // 2
        self.row = self.side // 2
        self.chunk = self.in_a.shape[1]

    def slot(self, q):
        return q % 2 if isinstance(q, int) else odd(q)

    def twin_out(self):
        return remote(self.r_v, self.o_v, self.to_send, self.to_recv, self.place.twin())

    def twin_in(self, b):
        return remote(self.gt_v, self.it_v.at[b], self.ti_send.at[b], self.ti_recv.at[b], self.place.twin())

    def across_x_out(self, q, i, h):
        s = self.slot(q)
        at = i // TWO
        return remote(
            self.p_out.at[s, i, h], self.o_a.at[s, at, h], self.oa_send.at[at, h], self.oa_recv.at[s, at, h], self.place.across(1)
        )

    def across_y_out(self, q, h):
        s = self.slot(q)
        return remote(self.u_out.at[s, h], self.o_b.at[s, h], self.ob_send.at[h], self.ob_recv.at[s, h], self.place.across(2))

    def across_y_in(self, q, i, b):
        s, far = self.slot(q), pl.ds(pl.multiple_of((1 - self.place.chip_y) * self.side, self.side), self.side)
        there = (i + TWO) % CHIPS
        return remote(
            self.q_in.at[s, i, b, far], self.i_a.at[s, there, b], self.ia_send.at[i, b], self.ia_recv.at[s, there, b], self.place.across(2)
        )

    def across_x_in(self, q, i, b):
        s, far = self.slot(q), pl.ds(pl.multiple_of((1 - self.place.chip_x) * self.row, self.row), self.row)
        there = i ^ 1
        return remote(
            self.s_in.at[s, i, b, far], self.i_b.at[s, there, b], self.ib_send.at[i, b], self.ib_recv.at[s, there, b], self.place.across(1)
        )

    def resend(self, q, copy_of):
        @when(q > 0)
        def _():
            copy_of(q).wait_send()

        copy_of(q).start()

    def save_p(self, q, i):
        s = self.slot(q)
        return [
            pltpu.make_async_copy(self.r_v.at[:, pl.ds(h * self.half_out, self.half_out)], self.p_out.at[s, i, h], self.p_sem.at[h])
            for h in range(TWO)
        ]

    def save_q(self, q, i, b, gm):
        return pltpu.make_async_copy(self.gm_v.at[gm], self.q_in.at[self.slot(q), i, b], self.q_sem.at[b])

    def out_loads(self, a, b):
        return [pltpu.make_async_copy(a, self.out_a, self.out_sem.at[0]), pltpu.make_async_copy(b, self.out_b, self.out_sem.at[1])]

    def out_second(self, q, h):
        s = self.slot(q)
        return self.out_loads(self.p_out.at[s, 1, h], self.o_a.at[s, 0, h])

    def out_third(self, q, h):
        s = self.slot(q)
        return self.out_loads(self.p_out.at[s, 3, h], self.o_a.at[s, 1, h])

    def out_last(self, q, h):
        return [pltpu.make_async_copy(self.o_b.at[self.slot(q), h], self.out_b, self.out_sem.at[1])]

    def out_second_save(self, q, h):
        return pltpu.make_async_copy(self.out_a, self.u_out.at[self.slot(q), h], self.out_save)

    def out_third_save(self, q, h):
        n = self.layers - 1 - q
        return pltpu.make_async_copy(self.out_a, self.gw_out.at[n, :, pl.ds(h * self.half_out, self.half_out)], self.out_save)

    def in_second(self, q, pair, b):
        s, near = self.slot(q), pl.ds(pl.multiple_of(self.place.chip_y * self.side, self.side), self.side)
        copies = []
        for at in range(TWO):
            i, rows = pair + TWO * at, pl.ds(at * self.side, self.side)
            copies.append(pltpu.make_async_copy(self.q_in.at[s, i, b, near], self.in_a.at[rows], self.in_sem.at[0, at]))
            copies.append(pltpu.make_async_copy(self.i_a.at[s, i, b], self.in_b.at[rows], self.in_sem.at[1, at]))
        return copies

    def in_third(self, q, b):
        s, near = self.slot(q), pl.ds(pl.multiple_of(self.place.chip_x * self.row, self.row), self.row)
        copies = []
        for i in range(CHIPS):
            rows = pl.ds(i * self.row, self.row)
            copies.append(pltpu.make_async_copy(self.s_in.at[s, i, b, near], self.in_a.at[rows], self.in_sem.at[0, i]))
            copies.append(pltpu.make_async_copy(self.i_b.at[s, i, b], self.in_b.at[rows], self.in_sem.at[1, i]))
        return copies

    def in_second_save(self, q, pair, b):
        s = self.slot(q)
        return [
            pltpu.make_async_copy(self.in_a.at[pl.ds(at * self.side, self.side)], self.s_in.at[s, pair + TWO * at, b], self.in_save.at[at])
            for at in range(TWO)
        ]

    def in_third_save(self, q, b):
        n = self.layers - 1 - q
        core = self.place.core
        copies = []
        for i in range(CHIPS):
            shard = 2 * self.place.chip_at(BACKWARD_UNITS[i]) + (core if b else 1 - core)
            columns = pl.ds(pl.multiple_of(shard * self.chunk, self.chunk), self.chunk)
            copies.append(pltpu.make_async_copy(self.in_a.at[pl.ds(i * self.row, self.row)], self.gw_in.at[n, :, columns], self.in_save.at[i]))
        return copies

    def add(self, a, b):
        for start in range(0, a.shape[0], ADD_ROWS):
            rows = pl.ds(start, ADD_ROWS)
            a[rows, :] = a[rows, :] + b[rows, :]

    def free(self, semaphore):
        notify(semaphore, self.place.twin())

    def start(self):
        for semaphore in (self.credit_o, self.credit_i.at[0], self.credit_i.at[1]):
            self.free(semaphore)

    def mid(self, q, s):
        here, older, prev = q < self.layers, q > 0, q - 1

        for (pair, b), step in zip(self.PARTS, self.SECOND):

            @when(both(s == step + 1, older))
            def _():
                for copy in self.in_second_save(prev, pair, b):
                    copy.wait()
                for at in range(TWO):
                    self.resend(prev, lambda q, at=at: self.across_x_in(q, pair + TWO * at, b))

        for t in range(STEPS):
            i, b = divmod(t, TWO)
            layer, real = (q, here) if t < 7 else (prev, older)

            @when(both(s == (t + 1) % STEPS, real))
            def _():
                self.twin_in(b).wait_send()
                if b == 0:
                    self.twin_out().wait_send()
                    return
                for copy in self.save_p(layer, i):
                    copy.wait()
                self.save_q(layer, i, 1, 0).wait()
                self.resend(layer, lambda q: self.across_y_in(q, i, 1))

            layer, real = (q, here) if t < 5 else (prev, older)
            if b == 0:

                @when(both(s == (t + 3) % STEPS, real))
                def _():
                    self.save_q(layer, i, 0, 0).wait()
                    self.resend(layer, lambda q: self.across_y_in(q, i, 0))

        for h in range(TWO):

            @when(both(s == TWO + h, here))
            def _():
                self.resend(q, lambda q: self.across_x_out(q, 0, h))

            @when(both(s == 6, here))
            def _():
                self.resend(q, lambda q: self.across_x_out(q, 2, h))

            layer, real = (prev, older) if h else (q, here)
            saved, sent = self.SENT[h]

            @when(both(s == saved, real))
            def _():
                self.out_second_save(layer, h).wait()

            @when(both(s == sent, real))
            def _():
                self.resend(layer, lambda q: self.across_y_out(q, h))

            @when(both(s == self.LAST[h] + 1, older))
            def _():
                self.out_third_save(prev, h).wait()

        @when(both(s == 6, older))
        def _():
            for copy in self.in_third_save(prev, 1):
                copy.wait()

        @when(both(s == 0, q > 1))
        def _():
            for copy in self.in_third_save(q - 2, 0):
                copy.wait()

        for (pair, b), step in zip(self.PARTS, self.SECOND):

            @when(both(s == step, older))
            def _():
                for at in range(TWO):
                    self.across_y_in(prev, (pair + TWO * at + TWO) % CHIPS, b).wait_recv()
                for copy in self.in_second(prev, pair, b):
                    copy.start()

        for b, step in enumerate(self.THIRD):

            @when(both(s == step, older))
            def _():
                for i in range(CHIPS):
                    self.across_x_in(prev, i ^ 1, b).wait_recv()
                for copy in self.in_third(prev, b):
                    copy.start()

        for h in range(TWO):

            @when(both(s == self.OUT[h], here))
            def _():
                self.across_x_out(q, 0, h).wait_recv()
                for copy in self.out_second(q, h):
                    copy.start()

            @when(both(s == self.NEXT[h], older))
            def _():
                self.across_x_out(prev, 2, h).wait_recv()
                for copy in self.out_third(prev, h):
                    copy.start()

            @when(both(s == self.LAST[h], older))
            def _():
                self.across_y_out(prev, h).wait_recv()
                for copy in self.out_last(prev, h):
                    copy.start()

    def end(self, q, s, gm):
        here, older, prev = q < self.layers, q > 0, q - 1
        old = (gm + 1) % 3 if isinstance(gm, int) else lax.rem(gm + 1, 3)

        for t in range(STEPS):
            i, b = divmod(t, TWO)

            @when(both(s == t, here))
            def _():
                more = True if i < 3 else q < self.layers - 1
                await_one(self.credit_i.at[b])
                self.twin_in(b).start()
                if b == 0:
                    await_one(self.credit_o)
                    self.twin_out().start()
                    return
                self.twin_out().wait_recv()
                self.add(self.r_v, self.o_v)

                @when(more)
                def _():
                    self.free(self.credit_o)

                for copy in self.save_p(q, i):
                    copy.start()
                self.twin_in(0).wait_recv()
                self.add(self.gm_v.at[gm], self.it_v.at[0])

                @when(more)
                def _():
                    self.free(self.credit_i.at[0])

                self.save_q(q, i, 1, gm).start()

            if b == 0:
                layer, real = (q, here) if t < 6 else (prev, older)

                @when(both(s == (t + 2) % STEPS, real))
                def _():
                    self.twin_in(1).wait_recv()
                    self.add(self.gm_v.at[old], self.it_v.at[1])

                    @when(True if i < 3 else layer < self.layers - 1)
                    def _():
                        self.free(self.credit_i.at[1])

                    self.save_q(layer, i, 0, old).start()

        def summed(parts, loads, saves):
            for copy in loads:
                copy.wait()
            self.add(*parts)
            for copy in saves:
                copy.start()

        ins, outs = (self.in_a, self.in_b), (self.out_a, self.out_b)
        for (pair, b), step in zip(self.PARTS, self.SECOND):

            @when(both(s == step, older))
            def _():
                summed(ins, self.in_second(prev, pair, b), self.in_second_save(prev, pair, b))

        for b in range(TWO):

            @when(both(s == self.THIRD[b], older))
            def _():
                summed(ins, self.in_third(prev, b), self.in_third_save(prev, b))

            @when(both(s == self.OUT[b], here))
            def _():
                summed(outs, self.out_second(q, b), [self.out_second_save(q, b)])

            @when(both(s == self.NEXT[b], older))
            def _():
                summed(outs, self.out_third(prev, b), [])

            @when(both(s == self.LAST[b], older))
            def _():
                summed(outs, self.out_last(prev, b), [self.out_third_save(prev, b)])

    def finish(self):
        q = self.layers
        last = q - 1
        for s in range(STEPS):
            self.mid(q, s)
            self.end(q, s, (STEPS * q + s) % 3)
        for copy in self.in_third_save(last, 0):
            copy.wait()
        for h in range(TWO):
            for i in (0, 2):
                self.across_x_out(last, i, h).wait_send()
            self.across_y_out(last, h).wait_send()
        for b in range(TWO):
            for i in range(CHIPS):
                self.across_y_in(last, i, b).wait_send()
                self.across_x_in(last, i, b).wait_send()


def forward_stack_kernel(layers, x_ref, w_in_ref, w_out_ref, *refs):
    xs_ref, own_in, own_out, kept_in, kept_out, got_in, got_out, twin_in, twin_out = refs[:9]
    x_v, unit_v, total_v, w_in_v, w_out_v, stage_in, stage_out = refs[9:16]
    x_sem, load_sem, stage_sem, credit = refs[16:20]
    place = Place()
    stream = Stream(place, (0, 1, 2, 3), own_in, own_out, kept_in, kept_out, got_in, got_out, twin_in, twin_out, refs[20:])
    pace = Pace(place, stream, layers, lambda q: q, lambda i: i, True, (w_in_v, w_out_v, load_sem), credit)
    tokens, width = x_v.shape
    tiles = tokens // TOK_TILE

    pairs = ((w_in_ref, stage_in, own_in, 0), (w_out_ref, stage_out, own_out, 1))

    def to_lanes(n, phase):
        for src, stage, own, at in pairs:
            if phase == 0:
                for b in range(stage.shape[0]):
                    pltpu.make_async_copy(src.at[n, :, pl.ds(b * LANES, LANES)], stage.at[b], stage_sem.at[at]).start()
            elif phase == 1:
                pltpu.make_async_copy(own.at[n], stage, stage_sem.at[at]).wait()
                pltpu.make_async_copy(stage, own.at[n], stage_sem.at[at]).start()
            else:
                pltpu.make_async_copy(stage, own.at[n], stage_sem.at[at]).wait()

    fetch = pltpu.make_async_copy(x_ref, x_v, x_sem)
    for phase in range(3):
        to_lanes(0, phase)
    fetch.start()
    meet(place)
    pace.head()
    for phase in range(3):
        to_lanes(1, phase)
    fetch.wait()

    def first_unit(t, carry):
        rows = tile_rows(t)
        x_wide, inv_rms = unit_rows_of(x_v[rows, :])
        put_tile(unit_v, rows, (x_wide * inv_rms).astype(BF16))
        total_v[rows, :] = jnp.zeros((TOK_TILE, width), F32)
        return carry

    lax.fori_loop(0, tiles, first_unit, 0)
    pace.head_end()

    def save(n):
        return pltpu.make_async_copy(x_v, xs_ref.at[n], x_sem)

    def compute(v, last):
        w_in, w_out = lane_join(w_in_v.at[v]), lane_join(w_out_v.at[v])
        pending = []

        def finish():
            t, hidden = pending.pop(0)
            rows = pl.ds(t * TOK_TILE, TOK_TILE)
            total = total_v[rows, :] + jnp.dot(hidden, w_out, preferred_element_type=F32)
            if not last:
                total_v[rows, :] = total
                return
            x_next = (x_v[rows, :].astype(F32) + total).astype(BF16)
            x_v[rows, :] = x_next
            total_v[rows, :] = jnp.zeros((TOK_TILE, width), F32)
            x_wide, inv_rms = unit_rows_of(x_next)
            put_tile(unit_v, rows, (x_wide * inv_rms).astype(BF16))

        for t in range(tiles):
            unit = tile_of(unit_v, pl.ds(t * TOK_TILE, TOK_TILE))
            pre = jnp.dot(unit, w_in, preferred_element_type=F32).astype(BF16).astype(F32)
            tanh = jnp.tanh(pre * (GELU_A + GELU_B * (pre * pre)))
            pending.append((t, (pre * (0.5 * tanh + 0.5)).astype(BF16)))
            if len(pending) > 1:
                finish()
        while pending:
            finish()

    def step(n, s):
        def before(k):
            pace.before(n, k)
            if 0 < k < 4:

                @pl.when(n + 2 < layers)
                def _():
                    to_lanes(n + 2, k - 1)

        def after(k):
            pace.late(n, k)
            pace.after(n, k)

        by_step(s, before)

        @pl.when(s < 7)
        def _():
            compute(odd(s), False)

        @pl.when(s == 7)
        def _():
            @pl.when(n > 0)
            def _():
                save(n - 1).wait()

            compute(1, True)
            save(n).start()

        by_step(s, after)

    def layer_step(n, carry):
        lax.fori_loop(0, STEPS, lambda s, c: (step(n, s), c)[1], 0)
        return carry

    lax.fori_loop(0, layers, layer_step, 0)
    stream.pushed(layers - 1, True)
    save(layers - 1).wait()


def backward_stack_kernel(layers, x_ref, xs_ref, dy_ref, own_in, own_out, kept_in, kept_out, *refs):
    gw_in, gw_out, dx_ref, got_in, got_out, twin_in, twin_out = refs[:7]
    sums_hbm = refs[7:15]
    unit_v, dy_v, du_v, hidden_v, dpre_v, w_in_v, w_out_v, x_v = refs[15:23]
    sums_v = refs[23:32]
    row_sem, x_sem, load_sem, credit = refs[32:36]
    stream_sems, sum_sems = refs[36:44], refs[44:]
    place = Place()
    stream = Stream(place, BACKWARD_UNITS, own_in, own_out, kept_in, kept_out, got_in, got_out, twin_in, twin_out, stream_sems)
    pace = Pace(place, stream, layers, lambda q: layers - 1 - q, lambda i: CHIPS - 1 - i, False, (w_in_v, w_out_v, load_sem), credit)
    sums = Reduce(place, layers, sums_hbm, sums_v, sum_sems, (gw_in, gw_out))
    r_v, gt_v, gm_v = sums_v[:3]
    blocks_d, tokens, _ = unit_v.shape
    width = blocks_d * LANES
    tiles = tokens // TOK_TILE

    meet(place)
    pace.head()
    sums.start()

    def rows_copies(to_vmem, ref):
        copies = []
        for b in range(blocks_d):
            pair = (ref.at[:, pl.ds(b * LANES, LANES)], dy_v.at[b])
            copies.append(pltpu.make_async_copy(*(pair if to_vmem else pair[::-1]), row_sem.at[b]))
        return copies

    dy_copies = rows_copies(True, dy_ref)
    for copy in dy_copies:
        copy.start()

    def fetch(n, which, t):
        dst, sem = x_v.at[which, odd(t)], x_sem.at[which, odd(t)]

        @pl.when(n > 0)
        def _():
            pltpu.make_async_copy(xs_ref.at[n - 1, tile_rows(t)], dst, sem).start()

        @pl.when(n == 0)
        def _():
            pltpu.make_async_copy(x_ref.at[tile_rows(t)], dst, sem).start()

    def fetched(which, t):
        at = odd(t)
        pltpu.make_async_copy(x_ref.at[tile_rows(0)], x_v.at[which, at], x_sem.at[which, at]).wait()
        return x_v[which, at]

    def first_unit(t, carry):
        @pl.when(t + 1 < tiles)
        def _():
            fetch(layers - 1, 1, t + 1)

        rows = tile_rows(t)
        x_wide, inv_rms = unit_rows_of(fetched(1, t))
        put_tile(unit_v, rows, (x_wide * inv_rms).astype(BF16))
        du_v[rows, :] = jnp.zeros((TOK_TILE, width), F32)
        return carry

    fetch(layers - 1, 1, 0)
    lax.fori_loop(0, tiles, first_unit, 0)
    for copy in dy_copies:
        copy.wait()
    pace.head_end()

    def hidden_part(v):
        w_in, w_out = lane_join(w_in_v.at[v]), lane_join(w_out_v.at[v])
        pending = []

        def finish():
            t, dpre = pending.pop(0)
            rows = pl.ds(t * TOK_TILE, TOK_TILE)
            du_v[rows, :] = du_v[rows, :] + lax.dot_general(dpre, w_in, LAST_LAST, preferred_element_type=F32)

        for t in range(tiles):
            rows = pl.ds(t * TOK_TILE, TOK_TILE)
            pre = jnp.dot(tile_of(unit_v, rows), w_in, preferred_element_type=F32).astype(BF16).astype(F32)
            dhidden = lax.dot_general(tile_of(dy_v, rows), w_out, LAST_LAST, preferred_element_type=F32)
            poly = GELU_A + GELU_B * (pre * pre)
            cdf = 0.5 * jnp.tanh(pre * poly) + 0.5
            hidden = pre * cdf
            slope = cdf + (hidden * (6.0 * poly - 4.0 * GELU_A)) * (1.0 - cdf)
            dpre = (slope * dhidden).astype(BF16)
            put_tile(hidden_v, rows, hidden.astype(BF16))
            put_tile(dpre_v, rows, dpre)
            pending.append((t, dpre))
            if len(pending) > 1:
                finish()
        while pending:
            finish()

    def gradient_part(gm):
        r_v[...] = lax.dot_general(lane_join(hidden_v), lane_join(dy_v), FIRST_FIRST, preferred_element_type=F32)
        dpre = lane_join(dpre_v)

        def unit_of(parity):
            per = blocks_d // SHARDS
            parts = [unit_v[(2 * c + parity) * per + b] for c in range(CHIPS) for b in range(per)]
            return jnp.concatenate(parts, axis=1)

        gt_v[...] = lax.dot_general(unit_of(1 - place.core), dpre, FIRST_FIRST, preferred_element_type=F32)
        gm_v[gm] = lax.dot_general(unit_of(place.core), dpre, FIRST_FIRST, preferred_element_type=F32)

    def step(q, s):
        gm = lax.rem(STEPS * q + s, 3)

        def middle(k):
            pace.late(q, k)
            sums.mid(q, k)

        def after(k):
            sums.end(q, k, gm)
            pace.after(q, k)

        by_step(s, lambda k: pace.before(q, k))
        hidden_part(odd(s))
        by_step(s, middle)
        gradient_part(gm)
        by_step(s, after)

    def layer_step(q, carry):
        n = layers - 1 - q
        lax.fori_loop(0, STEPS, lambda s, c: (step(q, s), c)[1], 0)
        fetch(n, 0, 0)

        @pl.when(n > 0)
        def _():
            fetch(n - 1, 1, 0)

        def close(t, carry):
            @pl.when(t + 1 < tiles)
            def _():
                fetch(n, 0, t + 1)

                @pl.when(n > 0)
                def _():
                    fetch(n - 1, 1, t + 1)

            rows = tile_rows(t)
            x_wide, inv_rms = unit_rows_of(fetched(0, t))
            value, du = x_wide * inv_rms, du_v[rows, :]
            row_mean = jnp.mean(du * value, axis=-1, keepdims=True)
            put_tile(dy_v, rows, (tile_of(dy_v, rows).astype(F32) + inv_rms * (du - value * row_mean)).astype(BF16))
            du_v[rows, :] = jnp.zeros((TOK_TILE, width), F32)

            @pl.when(n > 0)
            def _():
                x_wide, inv_rms = unit_rows_of(fetched(1, t))
                put_tile(unit_v, rows, (x_wide * inv_rms).astype(BF16))

            return carry

        lax.fori_loop(0, tiles, close, 0)
        return carry

    lax.fori_loop(0, layers, layer_step, 0)
    dx_copies = rows_copies(False, dx_ref)
    for copy in dx_copies:
        copy.start()
    sums.finish()
    stream.pushed(0, False)
    for copy in dx_copies:
        copy.wait()


def stream_semaphores():
    dma = pltpu.SemaphoreType.DMA
    return [dma((TWO, 3, CHIPS))] * TWO + [dma((TWO, 3))] * TWO + [dma((CHIPS, CHIPS)), dma((TWO, CHIPS, CHIPS)), dma((CHIPS,)), dma((TWO, CHIPS))]


def sum_semaphores():
    dma, regular = pltpu.SemaphoreType.DMA, pltpu.SemaphoreType.REGULAR
    return [
        dma,
        dma,
        dma((TWO,)),
        dma((TWO,)),
        dma((TWO, TWO)),
        dma((TWO, TWO, TWO)),
        dma((TWO,)),
        dma((TWO, TWO)),
        dma((CHIPS, TWO)),
        dma((TWO, CHIPS, TWO)),
        dma((CHIPS, TWO)),
        dma((TWO, CHIPS, TWO)),
        dma((TWO,)),
        dma((TWO,)),
        dma((TWO,)),
        dma((TWO, CHIPS)),
        dma,
        dma((CHIPS,)),
        regular,
        regular((TWO,)),
    ]


def stream_buffers(piece_in, piece_out):
    return [
        jax.ShapeDtypeStruct((TWO, TWO) + piece_in, BF16),
        jax.ShapeDtypeStruct((TWO, TWO) + piece_out, BF16),
        jax.ShapeDtypeStruct((TWO, CHIPS) + piece_in, BF16),
        jax.ShapeDtypeStruct((TWO, CHIPS) + piece_out, BF16),
    ]


ANYWHERE = pl.BlockSpec(memory_space=pl.ANY)


def forward_stack(x_rows, w_in, w_out):
    layers, depth, hidden_size = w_in.shape
    tokens, width = x_rows.shape
    chunk = w_out.shape[1]
    piece_in, piece_out = (hidden_size // LANES, depth, LANES), (width // LANES, chunk, LANES)
    pieces = [jax.ShapeDtypeStruct((layers,) + piece, BF16) for piece in (piece_in, piece_out)]
    shapes = [jax.ShapeDtypeStruct((layers, tokens, width), BF16)] + pieces * 2 + stream_buffers(piece_in, piece_out)
    outs = pl.pallas_call(
        functools.partial(forward_stack_kernel, layers),
        in_specs=[ANYWHERE] * 3,
        out_specs=[ANYWHERE] * len(shapes),
        out_shape=shapes,
        scratch_shapes=[
            pltpu.VMEM((tokens, width), BF16),
            pltpu.VMEM((width // LANES, tokens, LANES), BF16),
            pltpu.VMEM((tokens, width), F32),
            pltpu.VMEM((TWO, chunk // LANES, width, LANES), BF16),
            pltpu.VMEM((TWO, width // LANES, chunk, LANES), BF16),
            pltpu.VMEM(piece_in, BF16),
            pltpu.VMEM(piece_out, BF16),
            pltpu.SemaphoreType.DMA,
            pltpu.SemaphoreType.DMA((TWO, SHARDS + 1)),
            pltpu.SemaphoreType.DMA((TWO,)),
            pltpu.SemaphoreType.REGULAR((3,)),
        ]
        + stream_semaphores(),
        compiler_params=pltpu.CompilerParams(vmem_limit_bytes=VMEM_LIMIT, collective_id=0, has_side_effects=True),
        cost_estimate=pl.CostEstimate(flops=4 * layers * tokens * width * hidden_size, bytes_accessed=100_000_000, transcendentals=0),
        name="forward_stack",
    )(x_rows, w_in, w_out)
    return outs[:5]


def backward_stack(x_rows, xs, grad_rows, own_in, own_out, kept_in, kept_out):
    layers, blocks_f, depth, _ = own_in.shape
    blocks_d, chunk = own_out.shape[1], own_out.shape[2]
    tokens, width = x_rows.shape
    half, quarter = width // 2, width // 4
    hidden_size = blocks_f * LANES

    def sums(*shape):
        return jax.ShapeDtypeStruct(shape, F32)

    shapes = (
        [sums(layers, depth, hidden_size), sums(layers, chunk, width), jax.ShapeDtypeStruct((tokens, width), BF16)]
        + stream_buffers(own_in.shape[1:], own_out.shape[1:])
        + [
            sums(TWO, CHIPS, TWO, chunk, half),
            sums(TWO, TWO, TWO, chunk, half),
            sums(TWO, TWO, chunk, half),
            sums(TWO, TWO, chunk, half),
            sums(TWO, CHIPS, TWO, half, chunk),
            sums(TWO, CHIPS, TWO, quarter, chunk),
            sums(TWO, CHIPS, TWO, quarter, chunk),
            sums(TWO, CHIPS, TWO, depth, chunk),
        ]
    )
    outs = pl.pallas_call(
        functools.partial(backward_stack_kernel, layers),
        in_specs=[ANYWHERE] * 7,
        out_specs=[ANYWHERE] * len(shapes),
        out_shape=shapes,
        scratch_shapes=[
            pltpu.VMEM((blocks_d, tokens, LANES), BF16),
            pltpu.VMEM((blocks_d, tokens, LANES), BF16),
            pltpu.VMEM((tokens, width), F32),
            pltpu.VMEM((chunk // LANES, tokens, LANES), BF16),
            pltpu.VMEM((chunk // LANES, tokens, LANES), BF16),
            pltpu.VMEM((TWO, chunk // LANES, width, LANES), BF16),
            pltpu.VMEM((TWO, blocks_d, chunk, LANES), BF16),
            pltpu.VMEM((TWO, TWO, TOK_TILE, width), BF16),
            pltpu.VMEM((chunk, width), F32),
            pltpu.VMEM((half, chunk), F32),
            pltpu.VMEM((3, half, chunk), F32),
            pltpu.VMEM((chunk, width), F32),
            pltpu.VMEM((TWO, half, chunk), F32),
            pltpu.VMEM((chunk, half), F32),
            pltpu.VMEM((chunk, half), F32),
            pltpu.VMEM((half, chunk), F32),
            pltpu.VMEM((half, chunk), F32),
            pltpu.SemaphoreType.DMA((blocks_d,)),
            pltpu.SemaphoreType.DMA((TWO, TWO)),
            pltpu.SemaphoreType.DMA((TWO, SHARDS + 1)),
            pltpu.SemaphoreType.REGULAR((3,)),
        ]
        + stream_semaphores()
        + sum_semaphores(),
        compiler_params=pltpu.CompilerParams(vmem_limit_bytes=VMEM_LIMIT, collective_id=1, has_side_effects=True),
        cost_estimate=pl.CostEstimate(flops=10 * layers * tokens * width * hidden_size, bytes_accessed=300_000_000, transcendentals=0),
        name="backward_stack",
    )(x_rows, xs, grad_rows, own_in, own_out, kept_in, kept_out)
    return outs[:3]


def solution(mesh):
    row_spec = P(("local", "data"), None)
    weight_spec = P(None, ("local", "data"), None)

    def device_step(x_rows, grad_rows, w_in, w_out):
        xs, own_in, own_out, kept_in, kept_out = forward_stack(x_rows, w_in, w_out)
        gw_in, gw_out, dx = backward_stack(x_rows, xs, grad_rows, own_in, own_out, kept_in, kept_out)
        return xs[w_in.shape[0] - 1], gw_in, gw_out, dx

    return jax.shard_map(
        device_step,
        mesh=mesh,
        in_specs=(row_spec, row_spec, weight_spec, weight_spec),
        out_specs=(row_spec, weight_spec, weight_spec, row_spec),
        check_vma=False,
    )
```

```python
import functools

import jax
import jax.numpy as jnp
from jax import lax
from jax.experimental import pallas as pl
from jax.experimental.pallas import tpu as pltpu
from jax.sharding import PartitionSpec as P

NORM_EPS = 1e-6
GELU_A = 0.7978845608028654
GELU_B = GELU_A * 0.044715
LAST_LAST = (((1,), (1,)), ((), ()))
FIRST_FIRST = (((0,), (0,)), ((), ()))
BF16 = jnp.bfloat16
F32 = jnp.float32
MESH = pl.DeviceIdType.MESH

TWO = 2
CHIPS = 4
STEPS = 8
SHARDS = 8
LANES = 128
TOK_TILE = 256
VMEM_LIMIT = 67_000_000
ADD_ROWS = 64


def unit_rows_of(x_tile):
    x_wide = x_tile.astype(F32)
    inv_rms = lax.rsqrt(jnp.mean(x_wide * x_wide, axis=-1, keepdims=True) + NORM_EPS)
    return x_wide, inv_rms


def lane_join(ref):
    return jnp.concatenate([ref[b] for b in range(ref.shape[0])], axis=1)


def tile_of(ref, rows):
    return jnp.concatenate([ref[b, rows, :] for b in range(ref.shape[0])], axis=1)


def put_tile(ref, rows, value):
    for b in range(ref.shape[0]):
        ref[b, rows, :] = value[:, b * LANES : (b + 1) * LANES]


def tile_rows(t):
    return pl.ds(pl.multiple_of(t * TOK_TILE, TOK_TILE), TOK_TILE)


def odd(x):
    return x % TWO if isinstance(x, int) else lax.rem(x, TWO)


def half(x):
    return x // TWO if isinstance(x, int) else lax.div(x, TWO)


def when(condition):
    if isinstance(condition, bool):
        return lambda body: body() if condition else None
    return pl.when(condition)


def both(*conditions):
    kept = [c for c in conditions if not (isinstance(c, bool) and c)]
    if any(isinstance(c, bool) for c in kept):
        return False
    if not kept:
        return True
    return functools.reduce(lambda a, b: a & b, kept)


def by_step(s, body):
    for k in range(STEPS):

        @pl.when(s == k)
        def _():
            body(k)


def notify(semaphore, device):
    pl.semaphore_signal(semaphore, inc=1, device_id=device, device_id_type=MESH)


def await_one(semaphore):
    pl.semaphore_wait(semaphore, 1)


class Place:
    def __init__(self):
        self.chip = lax.axis_index("local")
        self.core = lax.axis_index("data")
        self.chip_x, self.chip_y = odd(self.chip), half(self.chip)

    def chip_at(self, mask):
        mask_x, mask_y = (mask % 2, mask // 2) if isinstance(mask, int) else (odd(mask), half(mask))
        return odd(self.chip_x + mask_x) + 2 * odd(self.chip_y + mask_y)

    def across(self, mask):
        return (self.chip_at(mask), self.core)

    def twin(self):
        return (self.chip, 1 - self.core)

    def peers(self):
        return [self.across(1), self.across(2), self.twin()]


def meet(place):
    barrier = pltpu.get_barrier_semaphore()
    for device in place.peers():
        notify(barrier, device)
    pl.semaphore_wait(barrier, 3)


def remote(src, dst, send_sem, recv_sem, device):
    return pltpu.make_async_remote_copy(
        src_ref=src, dst_ref=dst, send_sem=send_sem, recv_sem=recv_sem, device_id=device, device_id_type=MESH
    )


class Stream:
    def __init__(self, place, order, own_in, own_out, kept_in, kept_out, got_in, got_out, twin_in, twin_out, sems):
        self.place, self.order = place, order
        self.own_in, self.own_out, self.kept_in, self.kept_out = own_in, own_out, kept_in, kept_out
        self.got_in, self.got_out, self.twin_in, self.twin_out = got_in, got_out, twin_in, twin_out
        (self.in_send, self.in_recv, self.out_send, self.out_recv) = sems[:4]
        (self.twin_in_send, self.twin_in_recv, self.twin_out_send, self.twin_out_recv) = sems[4:]
        self.blocks = own_in.shape[1] // CHIPS

    def mine_in(self, n, mask, block, count):
        rows = pl.ds(block, count)
        if mask == 0:
            return self.own_in.at[n, rows]
        if mask == 1:
            return self.kept_in.at[n, rows]
        return self.got_in.at[odd(n), mask - 2, rows]

    def mine_out(self, n, mask):
        if mask == 0:
            return self.own_out.at[n]
        if mask == 2:
            return self.kept_out.at[n]
        return self.got_out.at[odd(n), (mask - 1) // 2]

    def send_in(self, n, mask, unit):
        there = 1 if mask == 1 else 2
        block = self.place.chip_at(there ^ unit) * self.blocks
        src = self.mine_in(n, 1 if mask == 3 else 0, block, self.blocks)
        dst = self.mine_in(n, mask, block, self.blocks)
        recv = self.in_recv.at[odd(n), mask - 1, unit]
        return remote(src, dst, self.in_send.at[odd(n), mask - 1, unit], recv, self.place.across(there))

    def got_slice(self, n, mask, unit):
        dst = self.mine_in(n, mask, self.place.chip_at(unit) * self.blocks, self.blocks)
        recv = self.in_recv.at[odd(n), mask - 1, unit]
        return remote(dst, dst, self.in_send.at[odd(n), mask - 1, unit], recv, self.place.across(1))

    def send_out(self, n, mask):
        src, dst = self.mine_out(n, 2 if mask == 3 else 0), self.mine_out(n, mask)
        recv = self.out_recv.at[odd(n), mask - 1]
        return remote(src, dst, self.out_send.at[odd(n), mask - 1], recv, self.place.across(2 if mask == 2 else 1))

    def push_in(self, n, masks, units):
        for unit in units:
            for mask in masks:
                self.send_in(n, mask, unit).start()

    def push_out(self, n, masks):
        for mask in masks:
            self.send_out(n, mask).start()

    def relay_in(self, n, units):
        for unit in units:
            self.got_slice(n, 1, 2 ^ unit).wait_recv()
            self.send_in(n, 3, unit).start()

    def relay_out(self, n):
        self.send_out(n, 2).wait_recv()
        self.send_out(n, 3).start()

    def pushed(self, n, keep):
        for mask in (1, 2, 3) if keep else (2, 3):
            for unit in self.order:
                self.send_in(n, mask, unit).wait_send()
        for mask in (1, 2, 3) if keep else (1, 3):
            self.send_out(n, mask).wait_send()

    def twin_copies(self, n, unit):
        slot, block = odd(n), self.place.chip_at(unit) * self.blocks
        return [
            remote(
                self.mine_in(n, mask, block, self.blocks),
                self.twin_in.at[slot, mask, pl.ds(block, self.blocks)],
                self.twin_in_send.at[mask, unit],
                self.twin_in_recv.at[slot, mask, unit],
                self.place.twin(),
            )
            for mask in range(CHIPS)
        ]

    def twin_out_copy(self, n, mask, unit):
        slot = odd(n)
        recv = self.twin_out_recv.at[slot, unit]
        return remote(self.mine_out(n, mask), self.twin_out.at[slot, unit], self.twin_out_send.at[unit], recv, self.place.twin())

    def forward(self, n, unit):
        for mask in (2, 3):
            self.got_slice(n, mask, unit).wait_recv()
        for copy in self.twin_copies(n, unit):
            copy.start()
        for mask in range(CHIPS):

            @when(unit == mask)
            def _():
                if mask in (1, 3):
                    self.send_out(n, mask).wait_recv()
                self.twin_out_copy(n, mask, unit).start()

    def forwarded(self, n, unit):
        for copy in self.twin_copies(n, unit):
            copy.wait_send()
        self.twin_out_copy(n, 0, unit).wait_send()

    def arrive(self, n, unit):
        for copy in self.twin_copies(n, unit):
            copy.wait_recv()
        self.twin_out_copy(n, 0, unit).wait_recv()

    def load_in(self, n, unit, parity, w_in_v, v, sem):
        count, depth = self.blocks // 2, self.own_in.shape[2]
        block = self.place.chip_at(unit) * self.blocks + parity * count
        copies = []
        for mask in range(CHIPS):
            for which in range(TWO):
                shard = 2 * self.place.chip_at(mask) + (self.place.core if which == 0 else 1 - self.place.core)
                src = self.mine_in(n, mask, block, count) if which == 0 else self.twin_in.at[odd(n), mask, pl.ds(block, count)]
                row = pl.ds(pl.multiple_of(shard * depth, depth), depth)
                copies.append(pltpu.make_async_copy(src, w_in_v.at[v, :, row], sem.at[v, 2 * mask + which]))
        return copies

    def load(self, n, unit, mine, w_in_v, w_out_v, v, sem):
        parity = 1 - self.place.core - mine + 2 * self.place.core * mine
        for copy in self.load_in(n, unit, parity, w_in_v, v, sem):
            copy.start()
        last = sem.at[v, SHARDS]

        @when(mine == 0)
        def _():
            pltpu.make_async_copy(self.twin_out.at[odd(n), unit], w_out_v.at[v], last).start()

        for mask in range(CHIPS):

            @when(both(mine == 1, unit == mask))
            def _():
                pltpu.make_async_copy(self.mine_out(n, mask), w_out_v.at[v], last).start()

    def loaded(self, w_in_v, w_out_v, v, sem):
        for copy in self.load_in(0, 0, 0, w_in_v, v, sem):
            copy.wait()
        pltpu.make_async_copy(self.own_out.at[0], w_out_v.at[v], sem.at[v, SHARDS]).wait()


class Pace:
    LATE = ((1, 0, 0, 1), (1, 0, 1, 1), (0, 0, 0, 0))
    PUSH = ((1, 1, 0, 1, 5, 6, 7), (2, 0, 4, 2, 3, 1, 7), (0, 1, 1, 3, 4, 5, 6))

    def __init__(self, place, stream, layers, layer_at, unit_at, keep, bufs, credit):
        self.place, self.stream, self.layers, self.layer_at, self.unit_at = place, stream, layers, layer_at, unit_at
        self.keep, self.credit = keep, credit
        self.w_in_v, self.w_out_v, self.load_sem = bufs

    def load(self, q, i, b):
        self.stream.load(self.layer_at(q), self.unit_at(i), b, self.w_in_v, self.w_out_v, b, self.load_sem)

    def head(self):
        n, stream = self.layer_at(0), self.stream
        if not self.keep:
            stream.push_in(n, (2, 3), stream.order)
            stream.push_out(n, (3, 1))
            return
        stream.push_in(n, (1,), (2, 3, 1, 0))
        stream.push_out(n, (1,))
        stream.push_in(n, (2,), (0, 1))

    def head_end(self):
        n, stream = self.layer_at(0), self.stream
        if not self.keep:
            self.first_chunk(0)
            return
        stream.relay_in(n, (0, 1))
        stream.push_out(n, (2,))
        stream.relay_in(n, (2,))
        self.first_chunk(0)
        stream.push_in(n, (2,), (2, 3))
        stream.relay_in(n, (3,))

    def first_chunk(self, q):
        n, unit = self.layer_at(q), self.unit_at(0)
        self.stream.forward(n, unit)
        self.stream.arrive(n, unit)
        self.load(q, 0, 0)
        self.stream.forwarded(n, unit)

    def turns(self, q):
        return [q == 0, q == 1, q > 1] if self.keep else [q == 0, q > 0]

    def units(self, q, late):
        units = []
        for turn, flags in zip(self.turns(q), self.LATE if self.keep else ((1, 1, 1, 0), (0, 0, 0, 0))):
            for i, flag in enumerate(flags):
                if flag == late:
                    count, real = (q, True) if i < 3 else (q + 1, q + 1 < self.layers)
                    units.append((2 * i, both(turn, real), count, (i + 1) % CHIPS))
        return units

    def sends(self, q, s):
        return [(both(s == step + late, turn), count, unit) for late in range(TWO) for step, turn, count, unit in self.units(q, late)]

    def push_parts(self, q, s):
        stream, units = self.stream, self.stream.order
        there, more = self.layer_at(q + 1), q + 1 < self.layers
        if not self.keep:
            for at, (step, mask) in enumerate(((1, 3), (4, 1))):

                @when(both(s == 3 * at, more))
                def _():
                    stream.push_in(there, (2, 3), units[TWO * at : TWO * at + TWO])

                @when(both(s == step, more))
                def _():
                    stream.push_out(there, (mask,))

            return

        parts = (
            (True, lambda: stream.relay_out(self.layer_at(q))),
            (more, lambda: stream.push_in(there, (1,), (2, 3, 0, 1))),
            (more, lambda: stream.push_in(there, (2,), units)),
            (more, lambda: stream.push_out(there, (1,))),
            (more, lambda: stream.relay_in(there, (0, 1))),
            (more, lambda: stream.push_out(there, (2,))),
            (more, lambda: stream.relay_in(there, (2, 3))),
        )
        for at, (real, part) in enumerate(parts):
            for turn, steps in zip(self.turns(q), self.PUSH):

                @when(both(s == steps[at], turn, real))
                def _():
                    part()

    def before(self, q, s):
        i, b = half(s), odd(s)
        more = q + 1 < self.layers

        @when(both(s == 0, q > 0))
        def _():
            self.stream.pushed(self.layer_at(q - 1), self.keep)

        @when(both(s == 0, more))
        def _():
            for at, device in enumerate(self.place.peers()):
                notify(self.credit.at[at], device)
            for at in range(3):
                await_one(self.credit.at[at])

        self.push_parts(q, s)
        for condition, count, unit in self.sends(q, s):

            @when(condition)
            def _():
                self.stream.forward(self.layer_at(count), self.unit_at(unit))

        @when(b == 0)
        def _():
            self.load(q, i, 1)

        self.fetch_unit(q, s, 0)
        self.stream.loaded(self.w_in_v, self.w_out_v, b, self.load_sem)

    def fetch_unit(self, q, s, late):
        for step, turn, count, unit in self.units(q, late):

            @when(both(s == step + 1, turn))
            def _():
                self.stream.arrive(self.layer_at(count), self.unit_at(unit))
                self.load(count, unit, 0)

    def late(self, q, s):
        self.fetch_unit(q, s, 1)

    def after(self, q, s):
        for condition, count, unit in self.sends(q, s):

            @when(condition)
            def _():
                self.stream.forwarded(self.layer_at(count), self.unit_at(unit))


BACKWARD_UNITS = (3, 2, 1, 0)


class Reduce:
    PARTS = ((0, 1), (0, 0), (1, 1), (1, 0))
    SECOND = (0, 1, 2, 4)
    THIRD = (7, 5)
    OUT = (4, 7)
    SENT = ((5, 5), (0, 1))
    NEXT = (1, 5)
    LAST = (3, 6)

    def __init__(self, place, layers, hbm, vmem, sems, outs):
        self.place, self.layers = place, layers
        self.p_out, self.o_a, self.o_b, self.u_out, self.q_in, self.i_a, self.s_in, self.i_b = hbm
        self.r_v, self.gt_v, self.gm_v, self.o_v, self.it_v, self.out_a, self.out_b, self.in_a, self.in_b = vmem
        (
            self.to_send,
            self.to_recv,
            self.ti_send,
            self.ti_recv,
            self.oa_send,
            self.oa_recv,
            self.ob_send,
            self.ob_recv,
            self.ia_send,
            self.ia_recv,
            self.ib_send,
            self.ib_recv,
            self.p_sem,
            self.q_sem,
            self.out_sem,
            self.in_sem,
            self.out_save,
            self.in_save,
            self.credit_o,
            self.credit_i,
        ) = sems
        self.gw_in, self.gw_out = outs
        self.half_out = self.out_a.shape[1]
        self.side = self.in_a.shape[0] // 2
        self.row = self.side // 2
        self.chunk = self.in_a.shape[1]

    def slot(self, q):
        return q % 2 if isinstance(q, int) else odd(q)

    def twin_out(self):
        return remote(self.r_v, self.o_v, self.to_send, self.to_recv, self.place.twin())

    def twin_in(self, b):
        return remote(self.gt_v, self.it_v.at[b], self.ti_send.at[b], self.ti_recv.at[b], self.place.twin())

    def across_x_out(self, q, i, h):
        s = self.slot(q)
        at = i // TWO
        return remote(
            self.p_out.at[s, i, h], self.o_a.at[s, at, h], self.oa_send.at[at, h], self.oa_recv.at[s, at, h], self.place.across(1)
        )

    def across_y_out(self, q, h):
        s = self.slot(q)
        return remote(self.u_out.at[s, h], self.o_b.at[s, h], self.ob_send.at[h], self.ob_recv.at[s, h], self.place.across(2))

    def across_y_in(self, q, i, b):
        s, far = self.slot(q), pl.ds(pl.multiple_of((1 - self.place.chip_y) * self.side, self.side), self.side)
        there = (i + TWO) % CHIPS
        return remote(
            self.q_in.at[s, i, b, far], self.i_a.at[s, there, b], self.ia_send.at[i, b], self.ia_recv.at[s, there, b], self.place.across(2)
        )

    def across_x_in(self, q, i, b):
        s, far = self.slot(q), pl.ds(pl.multiple_of((1 - self.place.chip_x) * self.row, self.row), self.row)
        there = i ^ 1
        return remote(
            self.s_in.at[s, i, b, far], self.i_b.at[s, there, b], self.ib_send.at[i, b], self.ib_recv.at[s, there, b], self.place.across(1)
        )

    def resend(self, q, copy_of):
        @when(q > 0)
        def _():
            copy_of(q).wait_send()

        copy_of(q).start()

    def save_p(self, q, i):
        s = self.slot(q)
        return [
            pltpu.make_async_copy(self.r_v.at[:, pl.ds(h * self.half_out, self.half_out)], self.p_out.at[s, i, h], self.p_sem.at[h])
            for h in range(TWO)
        ]

    def save_q(self, q, i, b, gm):
        return pltpu.make_async_copy(self.gm_v.at[gm], self.q_in.at[self.slot(q), i, b], self.q_sem.at[b])

    def out_loads(self, a, b):
        return [pltpu.make_async_copy(a, self.out_a, self.out_sem.at[0]), pltpu.make_async_copy(b, self.out_b, self.out_sem.at[1])]

    def out_second(self, q, h):
        s = self.slot(q)
        return self.out_loads(self.p_out.at[s, 1, h], self.o_a.at[s, 0, h])

    def out_third(self, q, h):
        s = self.slot(q)
        return self.out_loads(self.p_out.at[s, 3, h], self.o_a.at[s, 1, h])

    def out_last(self, q, h):
        return [pltpu.make_async_copy(self.o_b.at[self.slot(q), h], self.out_b, self.out_sem.at[1])]

    def out_second_save(self, q, h):
        return pltpu.make_async_copy(self.out_a, self.u_out.at[self.slot(q), h], self.out_save)

    def out_third_save(self, q, h):
        n = self.layers - 1 - q
        return pltpu.make_async_copy(self.out_a, self.gw_out.at[n, :, pl.ds(h * self.half_out, self.half_out)], self.out_save)

    def in_second(self, q, pair, b):
        s, near = self.slot(q), pl.ds(pl.multiple_of(self.place.chip_y * self.side, self.side), self.side)
        copies = []
        for at in range(TWO):
            i, rows = pair + TWO * at, pl.ds(at * self.side, self.side)
            copies.append(pltpu.make_async_copy(self.q_in.at[s, i, b, near], self.in_a.at[rows], self.in_sem.at[0, at]))
            copies.append(pltpu.make_async_copy(self.i_a.at[s, i, b], self.in_b.at[rows], self.in_sem.at[1, at]))
        return copies

    def in_third(self, q, b):
        s, near = self.slot(q), pl.ds(pl.multiple_of(self.place.chip_x * self.row, self.row), self.row)
        copies = []
        for i in range(CHIPS):
            rows = pl.ds(i * self.row, self.row)
            copies.append(pltpu.make_async_copy(self.s_in.at[s, i, b, near], self.in_a.at[rows], self.in_sem.at[0, i]))
            copies.append(pltpu.make_async_copy(self.i_b.at[s, i, b], self.in_b.at[rows], self.in_sem.at[1, i]))
        return copies

    def in_second_save(self, q, pair, b):
        s = self.slot(q)
        return [
            pltpu.make_async_copy(self.in_a.at[pl.ds(at * self.side, self.side)], self.s_in.at[s, pair + TWO * at, b], self.in_save.at[at])
            for at in range(TWO)
        ]

    def in_third_save(self, q, b):
        n = self.layers - 1 - q
        core = self.place.core
        copies = []
        for i in range(CHIPS):
            shard = 2 * self.place.chip_at(BACKWARD_UNITS[i]) + (core if b else 1 - core)
            columns = pl.ds(pl.multiple_of(shard * self.chunk, self.chunk), self.chunk)
            copies.append(pltpu.make_async_copy(self.in_a.at[pl.ds(i * self.row, self.row)], self.gw_in.at[n, :, columns], self.in_save.at[i]))
        return copies

    def add(self, a, b):
        for start in range(0, a.shape[0], ADD_ROWS):
            rows = pl.ds(start, ADD_ROWS)
            a[rows, :] = a[rows, :] + b[rows, :]

    def free(self, semaphore):
        notify(semaphore, self.place.twin())

    def start(self):
        for semaphore in (self.credit_o, self.credit_i.at[0], self.credit_i.at[1]):
            self.free(semaphore)

    def mid(self, q, s):
        here, older, prev = q < self.layers, q > 0, q - 1

        for (pair, b), step in zip(self.PARTS, self.SECOND):

            @when(both(s == step + 1, older))
            def _():
                for copy in self.in_second_save(prev, pair, b):
                    copy.wait()
                for at in range(TWO):
                    self.resend(prev, lambda q, at=at: self.across_x_in(q, pair + TWO * at, b))

        for t in range(STEPS):
            i, b = divmod(t, TWO)
            layer, real = (q, here) if t < 7 else (prev, older)

            @when(both(s == (t + 1) % STEPS, real))
            def _():
                self.twin_in(b).wait_send()
                if b == 0:
                    self.twin_out().wait_send()
                    return
                for copy in self.save_p(layer, i):
                    copy.wait()
                self.save_q(layer, i, 1, 0).wait()
                self.resend(layer, lambda q: self.across_y_in(q, i, 1))

            layer, real = (q, here) if t < 5 else (prev, older)
            if b == 0:

                @when(both(s == (t + 3) % STEPS, real))
                def _():
                    self.save_q(layer, i, 0, 0).wait()
                    self.resend(layer, lambda q: self.across_y_in(q, i, 0))

        for h in range(TWO):

            @when(both(s == TWO + h, here))
            def _():
                self.resend(q, lambda q: self.across_x_out(q, 0, h))

            @when(both(s == 6, here))
            def _():
                self.resend(q, lambda q: self.across_x_out(q, 2, h))

            layer, real = (prev, older) if h else (q, here)
            saved, sent = self.SENT[h]

            @when(both(s == saved, real))
            def _():
                self.out_second_save(layer, h).wait()

            @when(both(s == sent, real))
            def _():
                self.resend(layer, lambda q: self.across_y_out(q, h))

            @when(both(s == self.LAST[h] + 1, older))
            def _():
                self.out_third_save(prev, h).wait()

        @when(both(s == 6, older))
        def _():
            for copy in self.in_third_save(prev, 1):
                copy.wait()

        @when(both(s == 0, q > 1))
        def _():
            for copy in self.in_third_save(q - 2, 0):
                copy.wait()

        for (pair, b), step in zip(self.PARTS, self.SECOND):

            @when(both(s == step, older))
            def _():
                for at in range(TWO):
                    self.across_y_in(prev, (pair + TWO * at + TWO) % CHIPS, b).wait_recv()
                for copy in self.in_second(prev, pair, b):
                    copy.start()

        for b, step in enumerate(self.THIRD):

            @when(both(s == step, older))
            def _():
                for i in range(CHIPS):
                    self.across_x_in(prev, i ^ 1, b).wait_recv()
                for copy in self.in_third(prev, b):
                    copy.start()

        for h in range(TWO):

            @when(both(s == self.OUT[h], here))
            def _():
                self.across_x_out(q, 0, h).wait_recv()
                for copy in self.out_second(q, h):
                    copy.start()

            @when(both(s == self.NEXT[h], older))
            def _():
                self.across_x_out(prev, 2, h).wait_recv()
                for copy in self.out_third(prev, h):
                    copy.start()

            @when(both(s == self.LAST[h], older))
            def _():
                self.across_y_out(prev, h).wait_recv()
                for copy in self.out_last(prev, h):
                    copy.start()

    def end(self, q, s, gm):
        here, older, prev = q < self.layers, q > 0, q - 1
        old = (gm + 1) % 3 if isinstance(gm, int) else lax.rem(gm + 1, 3)

        for t in range(STEPS):
            i, b = divmod(t, TWO)

            @when(both(s == t, here))
            def _():
                more = True if i < 3 else q < self.layers - 1
                await_one(self.credit_i.at[b])
                self.twin_in(b).start()
                if b == 0:
                    await_one(self.credit_o)
                    self.twin_out().start()
                    return
                self.twin_out().wait_recv()
                self.add(self.r_v, self.o_v)

                @when(more)
                def _():
                    self.free(self.credit_o)

                for copy in self.save_p(q, i):
                    copy.start()
                self.twin_in(0).wait_recv()
                self.add(self.gm_v.at[gm], self.it_v.at[0])

                @when(more)
                def _():
                    self.free(self.credit_i.at[0])

                self.save_q(q, i, 1, gm).start()

            if b == 0:
                layer, real = (q, here) if t < 6 else (prev, older)

                @when(both(s == (t + 2) % STEPS, real))
                def _():
                    self.twin_in(1).wait_recv()
                    self.add(self.gm_v.at[old], self.it_v.at[1])

                    @when(True if i < 3 else layer < self.layers - 1)
                    def _():
                        self.free(self.credit_i.at[1])

                    self.save_q(layer, i, 0, old).start()

        def summed(parts, loads, saves):
            for copy in loads:
                copy.wait()
            self.add(*parts)
            for copy in saves:
                copy.start()

        ins, outs = (self.in_a, self.in_b), (self.out_a, self.out_b)
        for (pair, b), step in zip(self.PARTS, self.SECOND):

            @when(both(s == step, older))
            def _():
                summed(ins, self.in_second(prev, pair, b), self.in_second_save(prev, pair, b))

        for b in range(TWO):

            @when(both(s == self.THIRD[b], older))
            def _():
                summed(ins, self.in_third(prev, b), self.in_third_save(prev, b))

            @when(both(s == self.OUT[b], here))
            def _():
                summed(outs, self.out_second(q, b), [self.out_second_save(q, b)])

            @when(both(s == self.NEXT[b], older))
            def _():
                summed(outs, self.out_third(prev, b), [])

            @when(both(s == self.LAST[b], older))
            def _():
                summed(outs, self.out_last(prev, b), [self.out_third_save(prev, b)])

    def finish(self):
        q = self.layers
        last = q - 1
        for s in range(STEPS):
            self.mid(q, s)
            self.end(q, s, (STEPS * q + s) % 3)
        for copy in self.in_third_save(last, 0):
            copy.wait()
        for h in range(TWO):
            for i in (0, 2):
                self.across_x_out(last, i, h).wait_send()
            self.across_y_out(last, h).wait_send()
        for b in range(TWO):
            for i in range(CHIPS):
                self.across_y_in(last, i, b).wait_send()
                self.across_x_in(last, i, b).wait_send()


def forward_stack_kernel(layers, x_ref, w_in_ref, w_out_ref, *refs):
    xs_ref, own_in, own_out, kept_in, kept_out, got_in, got_out, twin_in, twin_out = refs[:9]
    x_v, unit_v, total_v, w_in_v, w_out_v, stage_in, stage_out = refs[9:16]
    x_sem, load_sem, stage_sem, credit = refs[16:20]
    place = Place()
    stream = Stream(place, (0, 1, 2, 3), own_in, own_out, kept_in, kept_out, got_in, got_out, twin_in, twin_out, refs[20:])
    pace = Pace(place, stream, layers, lambda q: q, lambda i: i, True, (w_in_v, w_out_v, load_sem), credit)
    tokens, width = x_v.shape
    tiles = tokens // TOK_TILE

    pairs = ((w_in_ref, stage_in, own_in, 0), (w_out_ref, stage_out, own_out, 1))

    def to_lanes(n, phase):
        for src, stage, own, at in pairs:
            if phase == 0:
                for b in range(stage.shape[0]):
                    pltpu.make_async_copy(src.at[n, :, pl.ds(b * LANES, LANES)], stage.at[b], stage_sem.at[at]).start()
            elif phase == 1:
                pltpu.make_async_copy(own.at[n], stage, stage_sem.at[at]).wait()
                pltpu.make_async_copy(stage, own.at[n], stage_sem.at[at]).start()
            else:
                pltpu.make_async_copy(stage, own.at[n], stage_sem.at[at]).wait()

    fetch = pltpu.make_async_copy(x_ref, x_v, x_sem)
    for phase in range(3):
        to_lanes(0, phase)
    fetch.start()
    meet(place)
    pace.head()
    for phase in range(3):
        to_lanes(1, phase)
    fetch.wait()

    def first_unit(t, carry):
        rows = tile_rows(t)
        x_wide, inv_rms = unit_rows_of(x_v[rows, :])
        put_tile(unit_v, rows, (x_wide * inv_rms).astype(BF16))
        total_v[rows, :] = jnp.zeros((TOK_TILE, width), F32)
        return carry

    lax.fori_loop(0, tiles, first_unit, 0)
    pace.head_end()

    def save(n):
        return pltpu.make_async_copy(x_v, xs_ref.at[n], x_sem)

    def compute(v, last):
        w_in, w_out = lane_join(w_in_v.at[v]), lane_join(w_out_v.at[v])
        pending = []

        def finish():
            t, hidden = pending.pop(0)
            rows = pl.ds(t * TOK_TILE, TOK_TILE)
            total = total_v[rows, :] + jnp.dot(hidden, w_out, preferred_element_type=F32)
            if not last:
                total_v[rows, :] = total
                return
            x_next = (x_v[rows, :].astype(F32) + total).astype(BF16)
            x_v[rows, :] = x_next
            total_v[rows, :] = jnp.zeros((TOK_TILE, width), F32)
            x_wide, inv_rms = unit_rows_of(x_next)
            put_tile(unit_v, rows, (x_wide * inv_rms).astype(BF16))

        for t in range(tiles):
            unit = tile_of(unit_v, pl.ds(t * TOK_TILE, TOK_TILE))
            pre = jnp.dot(unit, w_in, preferred_element_type=F32).astype(BF16).astype(F32)
            tanh = jnp.tanh(pre * (GELU_A + GELU_B * (pre * pre)))
            pending.append((t, (pre * (0.5 * tanh + 0.5)).astype(BF16)))
            if len(pending) > 1:
                finish()
        while pending:
            finish()

    def step(n, s):
        def before(k):
            pace.before(n, k)
            if 0 < k < 4:

                @pl.when(n + 2 < layers)
                def _():
                    to_lanes(n + 2, k - 1)

        def after(k):
            pace.late(n, k)
            pace.after(n, k)

        by_step(s, before)

        @pl.when(s < 7)
        def _():
            compute(odd(s), False)

        @pl.when(s == 7)
        def _():
            @pl.when(n > 0)
            def _():
                save(n - 1).wait()

            compute(1, True)
            save(n).start()

        by_step(s, after)

    def layer_step(n, carry):
        lax.fori_loop(0, STEPS, lambda s, c: (step(n, s), c)[1], 0)
        return carry

    lax.fori_loop(0, layers, layer_step, 0)
    stream.pushed(layers - 1, True)
    save(layers - 1).wait()


def backward_stack_kernel(layers, x_ref, xs_ref, dy_ref, own_in, own_out, kept_in, kept_out, *refs):
    gw_in, gw_out, dx_ref, got_in, got_out, twin_in, twin_out = refs[:7]
    sums_hbm = refs[7:15]
    unit_v, dy_v, du_v, hidden_v, dpre_v, w_in_v, w_out_v, x_v = refs[15:23]
    sums_v = refs[23:32]
    row_sem, x_sem, load_sem, credit = refs[32:36]
    stream_sems, sum_sems = refs[36:44], refs[44:]
    place = Place()
    stream = Stream(place, BACKWARD_UNITS, own_in, own_out, kept_in, kept_out, got_in, got_out, twin_in, twin_out, stream_sems)
    pace = Pace(place, stream, layers, lambda q: layers - 1 - q, lambda i: CHIPS - 1 - i, False, (w_in_v, w_out_v, load_sem), credit)
    sums = Reduce(place, layers, sums_hbm, sums_v, sum_sems, (gw_in, gw_out))
    r_v, gt_v, gm_v = sums_v[:3]
    blocks_d, tokens, _ = unit_v.shape
    width = blocks_d * LANES
    tiles = tokens // TOK_TILE

    meet(place)
    pace.head()
    sums.start()

    def rows_copies(to_vmem, ref):
        copies = []
        for b in range(blocks_d):
            pair = (ref.at[:, pl.ds(b * LANES, LANES)], dy_v.at[b])
            copies.append(pltpu.make_async_copy(*(pair if to_vmem else pair[::-1]), row_sem.at[b]))
        return copies

    dy_copies = rows_copies(True, dy_ref)
    for copy in dy_copies:
        copy.start()

    def fetch(n, which, t):
        dst, sem = x_v.at[which, odd(t)], x_sem.at[which, odd(t)]

        @pl.when(n > 0)
        def _():
            pltpu.make_async_copy(xs_ref.at[n - 1, tile_rows(t)], dst, sem).start()

        @pl.when(n == 0)
        def _():
            pltpu.make_async_copy(x_ref.at[tile_rows(t)], dst, sem).start()

    def fetched(which, t):
        at = odd(t)
        pltpu.make_async_copy(x_ref.at[tile_rows(0)], x_v.at[which, at], x_sem.at[which, at]).wait()
        return x_v[which, at]

    def first_unit(t, carry):
        @pl.when(t + 1 < tiles)
        def _():
            fetch(layers - 1, 1, t + 1)

        rows = tile_rows(t)
        x_wide, inv_rms = unit_rows_of(fetched(1, t))
        put_tile(unit_v, rows, (x_wide * inv_rms).astype(BF16))
        du_v[rows, :] = jnp.zeros((TOK_TILE, width), F32)
        return carry

    fetch(layers - 1, 1, 0)
    lax.fori_loop(0, tiles, first_unit, 0)
    for copy in dy_copies:
        copy.wait()
    pace.head_end()

    def hidden_part(v):
        w_in, w_out = lane_join(w_in_v.at[v]), lane_join(w_out_v.at[v])
        pending = []

        def finish():
            t, dpre = pending.pop(0)
            rows = pl.ds(t * TOK_TILE, TOK_TILE)
            du_v[rows, :] = du_v[rows, :] + lax.dot_general(dpre, w_in, LAST_LAST, preferred_element_type=F32)

        for t in range(tiles):
            rows = pl.ds(t * TOK_TILE, TOK_TILE)
            pre = jnp.dot(tile_of(unit_v, rows), w_in, preferred_element_type=F32).astype(BF16).astype(F32)
            dhidden = lax.dot_general(tile_of(dy_v, rows), w_out, LAST_LAST, preferred_element_type=F32)
            poly = GELU_A + GELU_B * (pre * pre)
            cdf = 0.5 * jnp.tanh(pre * poly) + 0.5
            hidden = pre * cdf
            slope = cdf + (hidden * (6.0 * poly - 4.0 * GELU_A)) * (1.0 - cdf)
            dpre = (slope * dhidden).astype(BF16)
            put_tile(hidden_v, rows, hidden.astype(BF16))
            put_tile(dpre_v, rows, dpre)
            pending.append((t, dpre))
            if len(pending) > 1:
                finish()
        while pending:
            finish()

    def gradient_part(gm):
        r_v[...] = lax.dot_general(lane_join(hidden_v), lane_join(dy_v), FIRST_FIRST, preferred_element_type=F32)
        dpre = lane_join(dpre_v)

        def unit_of(parity):
            per = blocks_d // SHARDS
            parts = [unit_v[(2 * c + parity) * per + b] for c in range(CHIPS) for b in range(per)]
            return jnp.concatenate(parts, axis=1)

        gt_v[...] = lax.dot_general(unit_of(1 - place.core), dpre, FIRST_FIRST, preferred_element_type=F32)
        gm_v[gm] = lax.dot_general(unit_of(place.core), dpre, FIRST_FIRST, preferred_element_type=F32)

    def step(q, s):
        gm = lax.rem(STEPS * q + s, 3)

        def middle(k):
            pace.late(q, k)
            sums.mid(q, k)

        def after(k):
            sums.end(q, k, gm)
            pace.after(q, k)

        by_step(s, lambda k: pace.before(q, k))
        hidden_part(odd(s))
        by_step(s, middle)
        gradient_part(gm)
        by_step(s, after)

    def layer_step(q, carry):
        n = layers - 1 - q
        lax.fori_loop(0, STEPS, lambda s, c: (step(q, s), c)[1], 0)
        fetch(n, 0, 0)

        @pl.when(n > 0)
        def _():
            fetch(n - 1, 1, 0)

        def close(t, carry):
            @pl.when(t + 1 < tiles)
            def _():
                fetch(n, 0, t + 1)

                @pl.when(n > 0)
                def _():
                    fetch(n - 1, 1, t + 1)

            rows = tile_rows(t)
            x_wide, inv_rms = unit_rows_of(fetched(0, t))
            value, du = x_wide * inv_rms, du_v[rows, :]
            row_mean = jnp.mean(du * value, axis=-1, keepdims=True)
            put_tile(dy_v, rows, (tile_of(dy_v, rows).astype(F32) + inv_rms * (du - value * row_mean)).astype(BF16))
            du_v[rows, :] = jnp.zeros((TOK_TILE, width), F32)

            @pl.when(n > 0)
            def _():
                x_wide, inv_rms = unit_rows_of(fetched(1, t))
                put_tile(unit_v, rows, (x_wide * inv_rms).astype(BF16))

            return carry

        lax.fori_loop(0, tiles, close, 0)
        return carry

    lax.fori_loop(0, layers, layer_step, 0)
    dx_copies = rows_copies(False, dx_ref)
    for copy in dx_copies:
        copy.start()
    sums.finish()
    stream.pushed(0, False)
    for copy in dx_copies:
        copy.wait()


def stream_semaphores():
    dma = pltpu.SemaphoreType.DMA
    return [dma((TWO, 3, CHIPS))] * TWO + [dma((TWO, 3))] * TWO + [dma((CHIPS, CHIPS)), dma((TWO, CHIPS, CHIPS)), dma((CHIPS,)), dma((TWO, CHIPS))]


def sum_semaphores():
    dma, regular = pltpu.SemaphoreType.DMA, pltpu.SemaphoreType.REGULAR
    return [
        dma,
        dma,
        dma((TWO,)),
        dma((TWO,)),
        dma((TWO, TWO)),
        dma((TWO, TWO, TWO)),
        dma((TWO,)),
        dma((TWO, TWO)),
        dma((CHIPS, TWO)),
        dma((TWO, CHIPS, TWO)),
        dma((CHIPS, TWO)),
        dma((TWO, CHIPS, TWO)),
        dma((TWO,)),
        dma((TWO,)),
        dma((TWO,)),
        dma((TWO, CHIPS)),
        dma,
        dma((CHIPS,)),
        regular,
        regular((TWO,)),
    ]


def stream_buffers(piece_in, piece_out):
    return [
        jax.ShapeDtypeStruct((TWO, TWO) + piece_in, BF16),
        jax.ShapeDtypeStruct((TWO, TWO) + piece_out, BF16),
        jax.ShapeDtypeStruct((TWO, CHIPS) + piece_in, BF16),
        jax.ShapeDtypeStruct((TWO, CHIPS) + piece_out, BF16),
    ]


ANYWHERE = pl.BlockSpec(memory_space=pl.ANY)


def forward_stack(x_rows, w_in, w_out):
    layers, depth, hidden_size = w_in.shape
    tokens, width = x_rows.shape
    chunk = w_out.shape[1]
    piece_in, piece_out = (hidden_size // LANES, depth, LANES), (width // LANES, chunk, LANES)
    pieces = [jax.ShapeDtypeStruct((layers,) + piece, BF16) for piece in (piece_in, piece_out)]
    shapes = [jax.ShapeDtypeStruct((layers, tokens, width), BF16)] + pieces * 2 + stream_buffers(piece_in, piece_out)
    outs = pl.pallas_call(
        functools.partial(forward_stack_kernel, layers),
        in_specs=[ANYWHERE] * 3,
        out_specs=[ANYWHERE] * len(shapes),
        out_shape=shapes,
        scratch_shapes=[
            pltpu.VMEM((tokens, width), BF16),
            pltpu.VMEM((width // LANES, tokens, LANES), BF16),
            pltpu.VMEM((tokens, width), F32),
            pltpu.VMEM((TWO, chunk // LANES, width, LANES), BF16),
            pltpu.VMEM((TWO, width // LANES, chunk, LANES), BF16),
            pltpu.VMEM(piece_in, BF16),
            pltpu.VMEM(piece_out, BF16),
            pltpu.SemaphoreType.DMA,
            pltpu.SemaphoreType.DMA((TWO, SHARDS + 1)),
            pltpu.SemaphoreType.DMA((TWO,)),
            pltpu.SemaphoreType.REGULAR((3,)),
        ]
        + stream_semaphores(),
        compiler_params=pltpu.CompilerParams(vmem_limit_bytes=VMEM_LIMIT, collective_id=0, has_side_effects=True),
        cost_estimate=pl.CostEstimate(flops=4 * layers * tokens * width * hidden_size, bytes_accessed=100_000_000, transcendentals=0),
        name="forward_stack",
    )(x_rows, w_in, w_out)
    return outs[:5]


def backward_stack(x_rows, xs, grad_rows, own_in, own_out, kept_in, kept_out):
    layers, blocks_f, depth, _ = own_in.shape
    blocks_d, chunk = own_out.shape[1], own_out.shape[2]
    tokens, width = x_rows.shape
    half, quarter = width // 2, width // 4
    hidden_size = blocks_f * LANES

    def sums(*shape):
        return jax.ShapeDtypeStruct(shape, F32)

    shapes = (
        [sums(layers, depth, hidden_size), sums(layers, chunk, width), jax.ShapeDtypeStruct((tokens, width), BF16)]
        + stream_buffers(own_in.shape[1:], own_out.shape[1:])
        + [
            sums(TWO, CHIPS, TWO, chunk, half),
            sums(TWO, TWO, TWO, chunk, half),
            sums(TWO, TWO, chunk, half),
            sums(TWO, TWO, chunk, half),
            sums(TWO, CHIPS, TWO, half, chunk),
            sums(TWO, CHIPS, TWO, quarter, chunk),
            sums(TWO, CHIPS, TWO, quarter, chunk),
            sums(TWO, CHIPS, TWO, depth, chunk),
        ]
    )
    outs = pl.pallas_call(
        functools.partial(backward_stack_kernel, layers),
        in_specs=[ANYWHERE] * 7,
        out_specs=[ANYWHERE] * len(shapes),
        out_shape=shapes,
        scratch_shapes=[
            pltpu.VMEM((blocks_d, tokens, LANES), BF16),
            pltpu.VMEM((blocks_d, tokens, LANES), BF16),
            pltpu.VMEM((tokens, width), F32),
            pltpu.VMEM((chunk // LANES, tokens, LANES), BF16),
            pltpu.VMEM((chunk // LANES, tokens, LANES), BF16),
            pltpu.VMEM((TWO, chunk // LANES, width, LANES), BF16),
            pltpu.VMEM((TWO, blocks_d, chunk, LANES), BF16),
            pltpu.VMEM((TWO, TWO, TOK_TILE, width), BF16),
            pltpu.VMEM((chunk, width), F32),
            pltpu.VMEM((half, chunk), F32),
            pltpu.VMEM((3, half, chunk), F32),
            pltpu.VMEM((chunk, width), F32),
            pltpu.VMEM((TWO, half, chunk), F32),
            pltpu.VMEM((chunk, half), F32),
            pltpu.VMEM((chunk, half), F32),
            pltpu.VMEM((half, chunk), F32),
            pltpu.VMEM((half, chunk), F32),
            pltpu.SemaphoreType.DMA((blocks_d,)),
            pltpu.SemaphoreType.DMA((TWO, TWO)),
            pltpu.SemaphoreType.DMA((TWO, SHARDS + 1)),
            pltpu.SemaphoreType.REGULAR((3,)),
        ]
        + stream_semaphores()
        + sum_semaphores(),
        compiler_params=pltpu.CompilerParams(vmem_limit_bytes=VMEM_LIMIT, collective_id=1, has_side_effects=True),
        cost_estimate=pl.CostEstimate(flops=10 * layers * tokens * width * hidden_size, bytes_accessed=300_000_000, transcendentals=0),
        name="backward_stack",
    )(x_rows, xs, grad_rows, own_in, own_out, kept_in, kept_out)
    return outs[:3]


def solution(mesh):
    row_spec = P(("local", "data"), None)
    weight_spec = P(None, ("local", "data"), None)

    def device_step(x_rows, grad_rows, w_in, w_out):
        xs, own_in, own_out, kept_in, kept_out = forward_stack(x_rows, w_in, w_out)
        gw_in, gw_out, dx = backward_stack(x_rows, xs, grad_rows, own_in, own_out, kept_in, kept_out)
        return xs[w_in.shape[0] - 1], gw_in, gw_out, dx

    return jax.shard_map(
        device_step,
        mesh=mesh,
        in_specs=(row_spec, row_spec, weight_spec, weight_spec),
        out_specs=(row_spec, weight_spec, weight_spec, row_spec),
        check_vma=False,
    )
```

```python
import functools

import jax
import jax.numpy as jnp
from jax import lax
from jax.experimental import pallas as pl
from jax.experimental.pallas import tpu as pltpu
from jax.sharding import PartitionSpec as P

NORM_EPS = 1e-6
GELU_A = 0.7978845608028654
GELU_B = GELU_A * 0.044715
LAST_LAST = (((1,), (1,)), ((), ()))
FIRST_FIRST = (((0,), (0,)), ((), ()))
BF16 = jnp.bfloat16
F32 = jnp.float32
MESH = pl.DeviceIdType.MESH

TWO = 2
CHIPS = 4
STEPS = 8
SHARDS = 8
LANES = 128
TOK_TILE = 256
VMEM_LIMIT = 67_000_000
ADD_ROWS = 64


def unit_rows_of(x_tile):
    x_wide = x_tile.astype(F32)
    inv_rms = lax.rsqrt(jnp.mean(x_wide * x_wide, axis=-1, keepdims=True) + NORM_EPS)
    return x_wide, inv_rms


def lane_join(ref):
    return jnp.concatenate([ref[b] for b in range(ref.shape[0])], axis=1)


def tile_of(ref, rows):
    return jnp.concatenate([ref[b, rows, :] for b in range(ref.shape[0])], axis=1)


def put_tile(ref, rows, value):
    for b in range(ref.shape[0]):
        ref[b, rows, :] = value[:, b * LANES : (b + 1) * LANES]


def tile_rows(t):
    return pl.ds(pl.multiple_of(t * TOK_TILE, TOK_TILE), TOK_TILE)


def odd(x):
    return x % TWO if isinstance(x, int) else lax.rem(x, TWO)


def half(x):
    return x // TWO if isinstance(x, int) else lax.div(x, TWO)


def when(condition):
    if isinstance(condition, bool):
        return lambda body: body() if condition else None
    return pl.when(condition)


def both(*conditions):
    kept = [c for c in conditions if not (isinstance(c, bool) and c)]
    if any(isinstance(c, bool) for c in kept):
        return False
    if not kept:
        return True
    return functools.reduce(lambda a, b: a & b, kept)


def by_step(s, body):
    for k in range(STEPS):

        @pl.when(s == k)
        def _():
            body(k)


def notify(semaphore, device):
    pl.semaphore_signal(semaphore, inc=1, device_id=device, device_id_type=MESH)


def await_one(semaphore):
    pl.semaphore_wait(semaphore, 1)


class Place:
    def __init__(self):
        self.chip = lax.axis_index("local")
        self.core = lax.axis_index("data")
        self.chip_x, self.chip_y = odd(self.chip), half(self.chip)

    def chip_at(self, mask):
        mask_x, mask_y = (mask % 2, mask // 2) if isinstance(mask, int) else (odd(mask), half(mask))
        return odd(self.chip_x + mask_x) + 2 * odd(self.chip_y + mask_y)

    def across(self, mask):
        return (self.chip_at(mask), self.core)

    def twin(self):
        return (self.chip, 1 - self.core)

    def peers(self):
        return [self.across(1), self.across(2), self.twin()]


def meet(place):
    barrier = pltpu.get_barrier_semaphore()
    for device in place.peers():
        notify(barrier, device)
    pl.semaphore_wait(barrier, 3)


def remote(src, dst, send_sem, recv_sem, device):
    return pltpu.make_async_remote_copy(
        src_ref=src, dst_ref=dst, send_sem=send_sem, recv_sem=recv_sem, device_id=device, device_id_type=MESH
    )


class Stream:
    def __init__(self, place, order, own_in, own_out, kept_in, kept_out, got_in, got_out, twin_in, twin_out, sems):
        self.place, self.order = place, order
        self.own_in, self.own_out, self.kept_in, self.kept_out = own_in, own_out, kept_in, kept_out
        self.got_in, self.got_out, self.twin_in, self.twin_out = got_in, got_out, twin_in, twin_out
        (self.in_send, self.in_recv, self.out_send, self.out_recv) = sems[:4]
        (self.twin_in_send, self.twin_in_recv, self.twin_out_send, self.twin_out_recv) = sems[4:]
        self.blocks = own_in.shape[1] // CHIPS

    def mine_in(self, n, mask, block, count):
        rows = pl.ds(block, count)
        if mask == 0:
            return self.own_in.at[n, rows]
        if mask == 1:
            return self.kept_in.at[n, rows]
        return self.got_in.at[odd(n), mask - 2, rows]

    def mine_out(self, n, mask):
        if mask == 0:
            return self.own_out.at[n]
        if mask == 2:
            return self.kept_out.at[n]
        return self.got_out.at[odd(n), (mask - 1) // 2]

    def send_in(self, n, mask, unit):
        there = 1 if mask == 1 else 2
        block = self.place.chip_at(there ^ unit) * self.blocks
        src = self.mine_in(n, 1 if mask == 3 else 0, block, self.blocks)
        dst = self.mine_in(n, mask, block, self.blocks)
        recv = self.in_recv.at[odd(n), mask - 1, unit]
        return remote(src, dst, self.in_send.at[odd(n), mask - 1, unit], recv, self.place.across(there))

    def got_slice(self, n, mask, unit):
        dst = self.mine_in(n, mask, self.place.chip_at(unit) * self.blocks, self.blocks)
        recv = self.in_recv.at[odd(n), mask - 1, unit]
        return remote(dst, dst, self.in_send.at[odd(n), mask - 1, unit], recv, self.place.across(1))

    def send_out(self, n, mask):
        src, dst = self.mine_out(n, 2 if mask == 3 else 0), self.mine_out(n, mask)
        recv = self.out_recv.at[odd(n), mask - 1]
        return remote(src, dst, self.out_send.at[odd(n), mask - 1], recv, self.place.across(2 if mask == 2 else 1))

    def push_in(self, n, masks, units):
        for unit in units:
            for mask in masks:
                self.send_in(n, mask, unit).start()

    def push_out(self, n, masks):
        for mask in masks:
            self.send_out(n, mask).start()

    def relay_in(self, n, units):
        for unit in units:
            self.got_slice(n, 1, 2 ^ unit).wait_recv()
            self.send_in(n, 3, unit).start()

    def relay_out(self, n):
        self.send_out(n, 2).wait_recv()
        self.send_out(n, 3).start()

    def pushed(self, n, keep):
        for mask in (1, 2, 3) if keep else (2, 3):
            for unit in self.order:
                self.send_in(n, mask, unit).wait_send()
        for mask in (1, 2, 3) if keep else (1, 3):
            self.send_out(n, mask).wait_send()

    def twin_copies(self, n, unit):
        slot, block = odd(n), self.place.chip_at(unit) * self.blocks
        return [
            remote(
                self.mine_in(n, mask, block, self.blocks),
                self.twin_in.at[slot, mask, pl.ds(block, self.blocks)],
                self.twin_in_send.at[mask, unit],
                self.twin_in_recv.at[slot, mask, unit],
                self.place.twin(),
            )
            for mask in range(CHIPS)
        ]

    def twin_out_copy(self, n, mask, unit):
        slot = odd(n)
        recv = self.twin_out_recv.at[slot, unit]
        return remote(self.mine_out(n, mask), self.twin_out.at[slot, unit], self.twin_out_send.at[unit], recv, self.place.twin())

    def forward(self, n, unit):
        for mask in (2, 3):
            self.got_slice(n, mask, unit).wait_recv()
        for copy in self.twin_copies(n, unit):
            copy.start()
        for mask in range(CHIPS):

            @when(unit == mask)
            def _():
                if mask in (1, 3):
                    self.send_out(n, mask).wait_recv()
                self.twin_out_copy(n, mask, unit).start()

    def forwarded(self, n, unit):
        for copy in self.twin_copies(n, unit):
            copy.wait_send()
        self.twin_out_copy(n, 0, unit).wait_send()

    def arrive(self, n, unit):
        for copy in self.twin_copies(n, unit):
            copy.wait_recv()
        self.twin_out_copy(n, 0, unit).wait_recv()

    def load_in(self, n, unit, parity, w_in_v, v, sem):
        count, depth = self.blocks // 2, self.own_in.shape[2]
        block = self.place.chip_at(unit) * self.blocks + parity * count
        copies = []
        for mask in range(CHIPS):
            for which in range(TWO):
                shard = 2 * self.place.chip_at(mask) + (self.place.core if which == 0 else 1 - self.place.core)
                src = self.mine_in(n, mask, block, count) if which == 0 else self.twin_in.at[odd(n), mask, pl.ds(block, count)]
                row = pl.ds(pl.multiple_of(shard * depth, depth), depth)
                copies.append(pltpu.make_async_copy(src, w_in_v.at[v, :, row], sem.at[v, 2 * mask + which]))
        return copies

    def load(self, n, unit, mine, w_in_v, w_out_v, v, sem):
        parity = 1 - self.place.core - mine + 2 * self.place.core * mine
        for copy in self.load_in(n, unit, parity, w_in_v, v, sem):
            copy.start()
        last = sem.at[v, SHARDS]

        @when(mine == 0)
        def _():
            pltpu.make_async_copy(self.twin_out.at[odd(n), unit], w_out_v.at[v], last).start()

        for mask in range(CHIPS):

            @when(both(mine == 1, unit == mask))
            def _():
                pltpu.make_async_copy(self.mine_out(n, mask), w_out_v.at[v], last).start()

    def loaded(self, w_in_v, w_out_v, v, sem):
        for copy in self.load_in(0, 0, 0, w_in_v, v, sem):
            copy.wait()
        pltpu.make_async_copy(self.own_out.at[0], w_out_v.at[v], sem.at[v, SHARDS]).wait()


class Pace:
    LATE = ((1, 0, 0, 1), (1, 0, 1, 1), (0, 0, 0, 0))
    PUSH = ((1, 1, 0, 1, 5, 6, 7), (2, 0, 4, 2, 3, 1, 7), (0, 1, 1, 3, 4, 5, 6))

    def __init__(self, place, stream, layers, layer_at, unit_at, keep, bufs, credit):
        self.place, self.stream, self.layers, self.layer_at, self.unit_at = place, stream, layers, layer_at, unit_at
        self.keep, self.credit = keep, credit
        self.w_in_v, self.w_out_v, self.load_sem = bufs

    def load(self, q, i, b):
        self.stream.load(self.layer_at(q), self.unit_at(i), b, self.w_in_v, self.w_out_v, b, self.load_sem)

    def head(self):
        n, stream = self.layer_at(0), self.stream
        if not self.keep:
            stream.push_in(n, (2, 3), stream.order)
            stream.push_out(n, (3, 1))
            return
        stream.push_in(n, (1,), (2, 3, 1, 0))
        stream.push_out(n, (1,))
        stream.push_in(n, (2,), (0, 1))

    def head_end(self):
        n, stream = self.layer_at(0), self.stream
        if not self.keep:
            self.first_chunk(0)
            return
        stream.relay_in(n, (0, 1))
        stream.push_out(n, (2,))
        stream.relay_in(n, (2,))
        self.first_chunk(0)
        stream.push_in(n, (2,), (2, 3))
        stream.relay_in(n, (3,))

    def first_chunk(self, q):
        n, unit = self.layer_at(q), self.unit_at(0)
        self.stream.forward(n, unit)
        self.stream.arrive(n, unit)
        self.load(q, 0, 0)
        self.stream.forwarded(n, unit)

    def turns(self, q):
        return [q == 0, q == 1, q > 1] if self.keep else [q == 0, q > 0]

    def units(self, q, late):
        units = []
        for turn, flags in zip(self.turns(q), self.LATE if self.keep else ((1, 1, 1, 0), (0, 0, 0, 0))):
            for i, flag in enumerate(flags):
                if flag == late:
                    count, real = (q, True) if i < 3 else (q + 1, q + 1 < self.layers)
                    units.append((2 * i, both(turn, real), count, (i + 1) % CHIPS))
        return units

    def sends(self, q, s):
        return [(both(s == step + late, turn), count, unit) for late in range(TWO) for step, turn, count, unit in self.units(q, late)]

    def push_parts(self, q, s):
        stream, units = self.stream, self.stream.order
        there, more = self.layer_at(q + 1), q + 1 < self.layers
        if not self.keep:
            for at, (step, mask) in enumerate(((1, 3), (4, 1))):

                @when(both(s == 3 * at, more))
                def _():
                    stream.push_in(there, (2, 3), units[TWO * at : TWO * at + TWO])

                @when(both(s == step, more))
                def _():
                    stream.push_out(there, (mask,))

            return

        parts = (
            (True, lambda: stream.relay_out(self.layer_at(q))),
            (more, lambda: stream.push_in(there, (1,), (2, 3, 0, 1))),
            (more, lambda: stream.push_in(there, (2,), units)),
            (more, lambda: stream.push_out(there, (1,))),
            (more, lambda: stream.relay_in(there, (0, 1))),
            (more, lambda: stream.push_out(there, (2,))),
            (more, lambda: stream.relay_in(there, (2, 3))),
        )
        for at, (real, part) in enumerate(parts):
            for turn, steps in zip(self.turns(q), self.PUSH):

                @when(both(s == steps[at], turn, real))
                def _():
                    part()

    def before(self, q, s):
        i, b = half(s), odd(s)
        more = q + 1 < self.layers

        @when(both(s == 0, q > 0))
        def _():
            self.stream.pushed(self.layer_at(q - 1), self.keep)

        @when(both(s == 0, more))
        def _():
            for at, device in enumerate(self.place.peers()):
                notify(self.credit.at[at], device)
            for at in range(3):
                await_one(self.credit.at[at])

        self.push_parts(q, s)
        for condition, count, unit in self.sends(q, s):

            @when(condition)
            def _():
                self.stream.forward(self.layer_at(count), self.unit_at(unit))

        @when(b == 0)
        def _():
            self.load(q, i, 1)

        self.fetch_unit(q, s, 0)
        self.stream.loaded(self.w_in_v, self.w_out_v, b, self.load_sem)

    def fetch_unit(self, q, s, late):
        for step, turn, count, unit in self.units(q, late):

            @when(both(s == step + 1, turn))
            def _():
                self.stream.arrive(self.layer_at(count), self.unit_at(unit))
                self.load(count, unit, 0)

    def late(self, q, s):
        self.fetch_unit(q, s, 1)

    def after(self, q, s):
        for condition, count, unit in self.sends(q, s):

            @when(condition)
            def _():
                self.stream.forwarded(self.layer_at(count), self.unit_at(unit))


BACKWARD_UNITS = (3, 2, 1, 0)


class Reduce:
    PARTS = ((0, 1), (0, 0), (1, 1), (1, 0))
    SECOND = (0, 1, 2, 4)
    THIRD = (7, 5)
    OUT = (4, 7)
    SENT = ((5, 5), (0, 1))
    NEXT = (1, 5)
    LAST = (3, 6)

    def __init__(self, place, layers, hbm, vmem, sems, outs):
        self.place, self.layers = place, layers
        self.p_out, self.o_a, self.o_b, self.u_out, self.q_in, self.i_a, self.s_in, self.i_b = hbm
        self.r_v, self.gt_v, self.gm_v, self.o_v, self.it_v, self.out_a, self.out_b, self.in_a, self.in_b = vmem
        (
            self.to_send,
            self.to_recv,
            self.ti_send,
            self.ti_recv,
            self.oa_send,
            self.oa_recv,
            self.ob_send,
            self.ob_recv,
            self.ia_send,
            self.ia_recv,
            self.ib_send,
            self.ib_recv,
            self.p_sem,
            self.q_sem,
            self.out_sem,
            self.in_sem,
            self.out_save,
            self.in_save,
            self.credit_o,
            self.credit_i,
        ) = sems
        self.gw_in, self.gw_out = outs
        self.half_out = self.out_a.shape[1]
        self.side = self.in_a.shape[0] // 2
        self.row = self.side // 2
        self.chunk = self.in_a.shape[1]

    def slot(self, q):
        return q % 2 if isinstance(q, int) else odd(q)

    def twin_out(self):
        return remote(self.r_v, self.o_v, self.to_send, self.to_recv, self.place.twin())

    def twin_in(self, b):
        return remote(self.gt_v, self.it_v.at[b], self.ti_send.at[b], self.ti_recv.at[b], self.place.twin())

    def across_x_out(self, q, i, h):
        s = self.slot(q)
        at = i // TWO
        return remote(
            self.p_out.at[s, i, h], self.o_a.at[s, at, h], self.oa_send.at[at, h], self.oa_recv.at[s, at, h], self.place.across(1)
        )

    def across_y_out(self, q, h):
        s = self.slot(q)
        return remote(self.u_out.at[s, h], self.o_b.at[s, h], self.ob_send.at[h], self.ob_recv.at[s, h], self.place.across(2))

    def across_y_in(self, q, i, b):
        s, far = self.slot(q), pl.ds(pl.multiple_of((1 - self.place.chip_y) * self.side, self.side), self.side)
        there = (i + TWO) % CHIPS
        return remote(
            self.q_in.at[s, i, b, far], self.i_a.at[s, there, b], self.ia_send.at[i, b], self.ia_recv.at[s, there, b], self.place.across(2)
        )

    def across_x_in(self, q, i, b):
        s, far = self.slot(q), pl.ds(pl.multiple_of((1 - self.place.chip_x) * self.row, self.row), self.row)
        there = i ^ 1
        return remote(
            self.s_in.at[s, i, b, far], self.i_b.at[s, there, b], self.ib_send.at[i, b], self.ib_recv.at[s, there, b], self.place.across(1)
        )

    def resend(self, q, copy_of):
        @when(q > 0)
        def _():
            copy_of(q).wait_send()

        copy_of(q).start()

    def save_p(self, q, i):
        s = self.slot(q)
        return [
            pltpu.make_async_copy(self.r_v.at[:, pl.ds(h * self.half_out, self.half_out)], self.p_out.at[s, i, h], self.p_sem.at[h])
            for h in range(TWO)
        ]

    def save_q(self, q, i, b, gm):
        return pltpu.make_async_copy(self.gm_v.at[gm], self.q_in.at[self.slot(q), i, b], self.q_sem.at[b])

    def out_loads(self, a, b):
        return [pltpu.make_async_copy(a, self.out_a, self.out_sem.at[0]), pltpu.make_async_copy(b, self.out_b, self.out_sem.at[1])]

    def out_second(self, q, h):
        s = self.slot(q)
        return self.out_loads(self.p_out.at[s, 1, h], self.o_a.at[s, 0, h])

    def out_third(self, q, h):
        s = self.slot(q)
        return self.out_loads(self.p_out.at[s, 3, h], self.o_a.at[s, 1, h])

    def out_last(self, q, h):
        return [pltpu.make_async_copy(self.o_b.at[self.slot(q), h], self.out_b, self.out_sem.at[1])]

    def out_second_save(self, q, h):
        return pltpu.make_async_copy(self.out_a, self.u_out.at[self.slot(q), h], self.out_save)

    def out_third_save(self, q, h):
        n = self.layers - 1 - q
        return pltpu.make_async_copy(self.out_a, self.gw_out.at[n, :, pl.ds(h * self.half_out, self.half_out)], self.out_save)

    def in_second(self, q, pair, b):
        s, near = self.slot(q), pl.ds(pl.multiple_of(self.place.chip_y * self.side, self.side), self.side)
        copies = []
        for at in range(TWO):
            i, rows = pair + TWO * at, pl.ds(at * self.side, self.side)
            copies.append(pltpu.make_async_copy(self.q_in.at[s, i, b, near], self.in_a.at[rows], self.in_sem.at[0, at]))
            copies.append(pltpu.make_async_copy(self.i_a.at[s, i, b], self.in_b.at[rows], self.in_sem.at[1, at]))
        return copies

    def in_third(self, q, b):
        s, near = self.slot(q), pl.ds(pl.multiple_of(self.place.chip_x * self.row, self.row), self.row)
        copies = []
        for i in range(CHIPS):
            rows = pl.ds(i * self.row, self.row)
            copies.append(pltpu.make_async_copy(self.s_in.at[s, i, b, near], self.in_a.at[rows], self.in_sem.at[0, i]))
            copies.append(pltpu.make_async_copy(self.i_b.at[s, i, b], self.in_b.at[rows], self.in_sem.at[1, i]))
        return copies

    def in_second_save(self, q, pair, b):
        s = self.slot(q)
        return [
            pltpu.make_async_copy(self.in_a.at[pl.ds(at * self.side, self.side)], self.s_in.at[s, pair + TWO * at, b], self.in_save.at[at])
            for at in range(TWO)
        ]

    def in_third_save(self, q, b):
        n = self.layers - 1 - q
        core = self.place.core
        copies = []
        for i in range(CHIPS):
            shard = 2 * self.place.chip_at(BACKWARD_UNITS[i]) + (core if b else 1 - core)
            columns = pl.ds(pl.multiple_of(shard * self.chunk, self.chunk), self.chunk)
            copies.append(pltpu.make_async_copy(self.in_a.at[pl.ds(i * self.row, self.row)], self.gw_in.at[n, :, columns], self.in_save.at[i]))
        return copies

    def add(self, a, b):
        for start in range(0, a.shape[0], ADD_ROWS):
            rows = pl.ds(start, ADD_ROWS)
            a[rows, :] = a[rows, :] + b[rows, :]

    def free(self, semaphore):
        notify(semaphore, self.place.twin())

    def start(self):
        for semaphore in (self.credit_o, self.credit_i.at[0], self.credit_i.at[1]):
            self.free(semaphore)

    def mid(self, q, s):
        here, older, prev = q < self.layers, q > 0, q - 1

        for (pair, b), step in zip(self.PARTS, self.SECOND):

            @when(both(s == step + 1, older))
            def _():
                for copy in self.in_second_save(prev, pair, b):
                    copy.wait()
                for at in range(TWO):
                    self.resend(prev, lambda q, at=at: self.across_x_in(q, pair + TWO * at, b))

        for t in range(STEPS):
            i, b = divmod(t, TWO)
            layer, real = (q, here) if t < 7 else (prev, older)

            @when(both(s == (t + 1) % STEPS, real))
            def _():
                self.twin_in(b).wait_send()
                if b == 0:
                    self.twin_out().wait_send()
                    return
                for copy in self.save_p(layer, i):
                    copy.wait()
                self.save_q(layer, i, 1, 0).wait()
                self.resend(layer, lambda q: self.across_y_in(q, i, 1))

            layer, real = (q, here) if t < 5 else (prev, older)
            if b == 0:

                @when(both(s == (t + 3) % STEPS, real))
                def _():
                    self.save_q(layer, i, 0, 0).wait()
                    self.resend(layer, lambda q: self.across_y_in(q, i, 0))

        for h in range(TWO):

            @when(both(s == TWO + h, here))
            def _():
                self.resend(q, lambda q: self.across_x_out(q, 0, h))

            @when(both(s == 6, here))
            def _():
                self.resend(q, lambda q: self.across_x_out(q, 2, h))

            layer, real = (prev, older) if h else (q, here)
            saved, sent = self.SENT[h]

            @when(both(s == saved, real))
            def _():
                self.out_second_save(layer, h).wait()

            @when(both(s == sent, real))
            def _():
                self.resend(layer, lambda q: self.across_y_out(q, h))

            @when(both(s == self.LAST[h] + 1, older))
            def _():
                self.out_third_save(prev, h).wait()

        @when(both(s == 6, older))
        def _():
            for copy in self.in_third_save(prev, 1):
                copy.wait()

        @when(both(s == 0, q > 1))
        def _():
            for copy in self.in_third_save(q - 2, 0):
                copy.wait()

        for (pair, b), step in zip(self.PARTS, self.SECOND):

            @when(both(s == step, older))
            def _():
                for at in range(TWO):
                    self.across_y_in(prev, (pair + TWO * at + TWO) % CHIPS, b).wait_recv()
                for copy in self.in_second(prev, pair, b):
                    copy.start()

        for b, step in enumerate(self.THIRD):

            @when(both(s == step, older))
            def _():
                for i in range(CHIPS):
                    self.across_x_in(prev, i ^ 1, b).wait_recv()
                for copy in self.in_third(prev, b):
                    copy.start()

        for h in range(TWO):

            @when(both(s == self.OUT[h], here))
            def _():
                self.across_x_out(q, 0, h).wait_recv()
                for copy in self.out_second(q, h):
                    copy.start()

            @when(both(s == self.NEXT[h], older))
            def _():
                self.across_x_out(prev, 2, h).wait_recv()
                for copy in self.out_third(prev, h):
                    copy.start()

            @when(both(s == self.LAST[h], older))
            def _():
                self.across_y_out(prev, h).wait_recv()
                for copy in self.out_last(prev, h):
                    copy.start()

    def end(self, q, s, gm):
        here, older, prev = q < self.layers, q > 0, q - 1
        old = (gm + 1) % 3 if isinstance(gm, int) else lax.rem(gm + 1, 3)

        for t in range(STEPS):
            i, b = divmod(t, TWO)

            @when(both(s == t, here))
            def _():
                more = True if i < 3 else q < self.layers - 1
                await_one(self.credit_i.at[b])
                self.twin_in(b).start()
                if b == 0:
                    await_one(self.credit_o)
                    self.twin_out().start()
                    return
                self.twin_out().wait_recv()
                self.add(self.r_v, self.o_v)

                @when(more)
                def _():
                    self.free(self.credit_o)

                for copy in self.save_p(q, i):
                    copy.start()
                self.twin_in(0).wait_recv()
                self.add(self.gm_v.at[gm], self.it_v.at[0])

                @when(more)
                def _():
                    self.free(self.credit_i.at[0])

                self.save_q(q, i, 1, gm).start()

            if b == 0:
                layer, real = (q, here) if t < 6 else (prev, older)

                @when(both(s == (t + 2) % STEPS, real))
                def _():
                    self.twin_in(1).wait_recv()
                    self.add(self.gm_v.at[old], self.it_v.at[1])

                    @when(True if i < 3 else layer < self.layers - 1)
                    def _():
                        self.free(self.credit_i.at[1])

                    self.save_q(layer, i, 0, old).start()

        def summed(parts, loads, saves):
            for copy in loads:
                copy.wait()
            self.add(*parts)
            for copy in saves:
                copy.start()

        ins, outs = (self.in_a, self.in_b), (self.out_a, self.out_b)
        for (pair, b), step in zip(self.PARTS, self.SECOND):

            @when(both(s == step, older))
            def _():
                summed(ins, self.in_second(prev, pair, b), self.in_second_save(prev, pair, b))

        for b in range(TWO):

            @when(both(s == self.THIRD[b], older))
            def _():
                summed(ins, self.in_third(prev, b), self.in_third_save(prev, b))

            @when(both(s == self.OUT[b], here))
            def _():
                summed(outs, self.out_second(q, b), [self.out_second_save(q, b)])

            @when(both(s == self.NEXT[b], older))
            def _():
                summed(outs, self.out_third(prev, b), [])

            @when(both(s == self.LAST[b], older))
            def _():
                summed(outs, self.out_last(prev, b), [self.out_third_save(prev, b)])

    def finish(self):
        q = self.layers
        last = q - 1
        for s in range(STEPS):
            self.mid(q, s)
            self.end(q, s, (STEPS * q + s) % 3)
        for copy in self.in_third_save(last, 0):
            copy.wait()
        for h in range(TWO):
            for i in (0, 2):
                self.across_x_out(last, i, h).wait_send()
            self.across_y_out(last, h).wait_send()
        for b in range(TWO):
            for i in range(CHIPS):
                self.across_y_in(last, i, b).wait_send()
                self.across_x_in(last, i, b).wait_send()


def forward_stack_kernel(layers, x_ref, w_in_ref, w_out_ref, *refs):
    xs_ref, own_in, own_out, kept_in, kept_out, got_in, got_out, twin_in, twin_out = refs[:9]
    x_v, unit_v, total_v, w_in_v, w_out_v, stage_in, stage_out = refs[9:16]
    x_sem, load_sem, stage_sem, credit = refs[16:20]
    place = Place()
    stream = Stream(place, (0, 1, 2, 3), own_in, own_out, kept_in, kept_out, got_in, got_out, twin_in, twin_out, refs[20:])
    pace = Pace(place, stream, layers, lambda q: q, lambda i: i, True, (w_in_v, w_out_v, load_sem), credit)
    tokens, width = x_v.shape
    tiles = tokens // TOK_TILE

    pairs = ((w_in_ref, stage_in, own_in, 0), (w_out_ref, stage_out, own_out, 1))

    def to_lanes(n, phase):
        for src, stage, own, at in pairs:
            if phase == 0:
                for b in range(stage.shape[0]):
                    pltpu.make_async_copy(src.at[n, :, pl.ds(b * LANES, LANES)], stage.at[b], stage_sem.at[at]).start()
            elif phase == 1:
                pltpu.make_async_copy(own.at[n], stage, stage_sem.at[at]).wait()
                pltpu.make_async_copy(stage, own.at[n], stage_sem.at[at]).start()
            else:
                pltpu.make_async_copy(stage, own.at[n], stage_sem.at[at]).wait()

    fetch = pltpu.make_async_copy(x_ref, x_v, x_sem)
    for phase in range(3):
        to_lanes(0, phase)
    fetch.start()
    meet(place)
    pace.head()
    for phase in range(3):
        to_lanes(1, phase)
    fetch.wait()

    def first_unit(t, carry):
        rows = tile_rows(t)
        x_wide, inv_rms = unit_rows_of(x_v[rows, :])
        put_tile(unit_v, rows, (x_wide * inv_rms).astype(BF16))
        total_v[rows, :] = jnp.zeros((TOK_TILE, width), F32)
        return carry

    lax.fori_loop(0, tiles, first_unit, 0)
    pace.head_end()

    def save(n):
        return pltpu.make_async_copy(x_v, xs_ref.at[n], x_sem)

    def compute(v, last):
        w_in, w_out = lane_join(w_in_v.at[v]), lane_join(w_out_v.at[v])
        pending = []

        def finish():
            t, hidden = pending.pop(0)
            rows = pl.ds(t * TOK_TILE, TOK_TILE)
            total = total_v[rows, :] + jnp.dot(hidden, w_out, preferred_element_type=F32)
            if not last:
                total_v[rows, :] = total
                return
            x_next = (x_v[rows, :].astype(F32) + total).astype(BF16)
            x_v[rows, :] = x_next
            total_v[rows, :] = jnp.zeros((TOK_TILE, width), F32)
            x_wide, inv_rms = unit_rows_of(x_next)
            put_tile(unit_v, rows, (x_wide * inv_rms).astype(BF16))

        for t in range(tiles):
            unit = tile_of(unit_v, pl.ds(t * TOK_TILE, TOK_TILE))
            pre = jnp.dot(unit, w_in, preferred_element_type=F32).astype(BF16).astype(F32)
            tanh = jnp.tanh(pre * (GELU_A + GELU_B * (pre * pre)))
            pending.append((t, (pre * (0.5 * tanh + 0.5)).astype(BF16)))
            if len(pending) > 1:
                finish()
        while pending:
            finish()

    def step(n, s):
        def before(k):
            pace.before(n, k)
            if 0 < k < 4:

                @pl.when(n + 2 < layers)
                def _():
                    to_lanes(n + 2, k - 1)

        def after(k):
            pace.late(n, k)
            pace.after(n, k)

        by_step(s, before)

        @pl.when(s < 7)
        def _():
            compute(odd(s), False)

        @pl.when(s == 7)
        def _():
            @pl.when(n > 0)
            def _():
                save(n - 1).wait()

            compute(1, True)
            save(n).start()

        by_step(s, after)

    def layer_step(n, carry):
        lax.fori_loop(0, STEPS, lambda s, c: (step(n, s), c)[1], 0)
        return carry

    lax.fori_loop(0, layers, layer_step, 0)
    stream.pushed(layers - 1, True)
    save(layers - 1).wait()


def backward_stack_kernel(layers, x_ref, xs_ref, dy_ref, own_in, own_out, kept_in, kept_out, *refs):
    gw_in, gw_out, dx_ref, got_in, got_out, twin_in, twin_out = refs[:7]
    sums_hbm = refs[7:15]
    unit_v, dy_v, du_v, hidden_v, dpre_v, w_in_v, w_out_v, x_v = refs[15:23]
    sums_v = refs[23:32]
    row_sem, x_sem, load_sem, credit = refs[32:36]
    stream_sems, sum_sems = refs[36:44], refs[44:]
    place = Place()
    stream = Stream(place, BACKWARD_UNITS, own_in, own_out, kept_in, kept_out, got_in, got_out, twin_in, twin_out, stream_sems)
    pace = Pace(place, stream, layers, lambda q: layers - 1 - q, lambda i: CHIPS - 1 - i, False, (w_in_v, w_out_v, load_sem), credit)
    sums = Reduce(place, layers, sums_hbm, sums_v, sum_sems, (gw_in, gw_out))
    r_v, gt_v, gm_v = sums_v[:3]
    blocks_d, tokens, _ = unit_v.shape
    width = blocks_d * LANES
    tiles = tokens // TOK_TILE

    meet(place)
    pace.head()
    sums.start()

    def rows_copies(to_vmem, ref):
        copies = []
        for b in range(blocks_d):
            pair = (ref.at[:, pl.ds(b * LANES, LANES)], dy_v.at[b])
            copies.append(pltpu.make_async_copy(*(pair if to_vmem else pair[::-1]), row_sem.at[b]))
        return copies

    dy_copies = rows_copies(True, dy_ref)
    for copy in dy_copies:
        copy.start()

    def fetch(n, which, t):
        dst, sem = x_v.at[which, odd(t)], x_sem.at[which, odd(t)]

        @pl.when(n > 0)
        def _():
            pltpu.make_async_copy(xs_ref.at[n - 1, tile_rows(t)], dst, sem).start()

        @pl.when(n == 0)
        def _():
            pltpu.make_async_copy(x_ref.at[tile_rows(t)], dst, sem).start()

    def fetched(which, t):
        at = odd(t)
        pltpu.make_async_copy(x_ref.at[tile_rows(0)], x_v.at[which, at], x_sem.at[which, at]).wait()
        return x_v[which, at]

    def first_unit(t, carry):
        @pl.when(t + 1 < tiles)
        def _():
            fetch(layers - 1, 1, t + 1)

        rows = tile_rows(t)
        x_wide, inv_rms = unit_rows_of(fetched(1, t))
        put_tile(unit_v, rows, (x_wide * inv_rms).astype(BF16))
        du_v[rows, :] = jnp.zeros((TOK_TILE, width), F32)
        return carry

    fetch(layers - 1, 1, 0)
    lax.fori_loop(0, tiles, first_unit, 0)
    for copy in dy_copies:
        copy.wait()
    pace.head_end()

    def hidden_part(v):
        w_in, w_out = lane_join(w_in_v.at[v]), lane_join(w_out_v.at[v])
        pending = []

        def finish():
            t, dpre = pending.pop(0)
            rows = pl.ds(t * TOK_TILE, TOK_TILE)
            du_v[rows, :] = du_v[rows, :] + lax.dot_general(dpre, w_in, LAST_LAST, preferred_element_type=F32)

        for t in range(tiles):
            rows = pl.ds(t * TOK_TILE, TOK_TILE)
            pre = jnp.dot(tile_of(unit_v, rows), w_in, preferred_element_type=F32).astype(BF16).astype(F32)
            dhidden = lax.dot_general(tile_of(dy_v, rows), w_out, LAST_LAST, preferred_element_type=F32)
            poly = GELU_A + GELU_B * (pre * pre)
            cdf = 0.5 * jnp.tanh(pre * poly) + 0.5
            hidden = pre * cdf
            slope = cdf + (hidden * (6.0 * poly - 4.0 * GELU_A)) * (1.0 - cdf)
            dpre = (slope * dhidden).astype(BF16)
            put_tile(hidden_v, rows, hidden.astype(BF16))
            put_tile(dpre_v, rows, dpre)
            pending.append((t, dpre))
            if len(pending) > 1:
                finish()
        while pending:
            finish()

    def gradient_part(gm):
        r_v[...] = lax.dot_general(lane_join(hidden_v), lane_join(dy_v), FIRST_FIRST, preferred_element_type=F32)
        dpre = lane_join(dpre_v)

        def unit_of(parity):
            per = blocks_d // SHARDS
            parts = [unit_v[(2 * c + parity) * per + b] for c in range(CHIPS) for b in range(per)]
            return jnp.concatenate(parts, axis=1)

        gt_v[...] = lax.dot_general(unit_of(1 - place.core), dpre, FIRST_FIRST, preferred_element_type=F32)
        gm_v[gm] = lax.dot_general(unit_of(place.core), dpre, FIRST_FIRST, preferred_element_type=F32)

    def step(q, s):
        gm = lax.rem(STEPS * q + s, 3)

        def middle(k):
            pace.late(q, k)
            sums.mid(q, k)

        def after(k):
            sums.end(q, k, gm)
            pace.after(q, k)

        by_step(s, lambda k: pace.before(q, k))
        hidden_part(odd(s))
        by_step(s, middle)
        gradient_part(gm)
        by_step(s, after)

    def layer_step(q, carry):
        n = layers - 1 - q
        fetch(n, 0, 0)

        @pl.when(n > 0)
        def _():
            fetch(n - 1, 1, 0)

        lax.fori_loop(0, STEPS, lambda s, c: (step(q, s), c)[1], 0)

        def close(t, carry):
            @pl.when(t + 1 < tiles)
            def _():
                fetch(n, 0, t + 1)

                @pl.when(n > 0)
                def _():
                    fetch(n - 1, 1, t + 1)

            rows = tile_rows(t)
            x_wide, inv_rms = unit_rows_of(fetched(0, t))
            value, du = x_wide * inv_rms, du_v[rows, :]
            row_mean = jnp.mean(du * value, axis=-1, keepdims=True)
            put_tile(dy_v, rows, (tile_of(dy_v, rows).astype(F32) + inv_rms * (du - value * row_mean)).astype(BF16))
            du_v[rows, :] = jnp.zeros((TOK_TILE, width), F32)

            @pl.when(n > 0)
            def _():
                x_wide, inv_rms = unit_rows_of(fetched(1, t))
                put_tile(unit_v, rows, (x_wide * inv_rms).astype(BF16))

            return carry

        lax.fori_loop(0, tiles, close, 0)
        return carry

    lax.fori_loop(0, layers, layer_step, 0)
    dx_copies = rows_copies(False, dx_ref)
    for copy in dx_copies:
        copy.start()
    sums.finish()
    stream.pushed(0, False)
    for copy in dx_copies:
        copy.wait()


def stream_semaphores():
    dma = pltpu.SemaphoreType.DMA
    return [dma((TWO, 3, CHIPS))] * TWO + [dma((TWO, 3))] * TWO + [dma((CHIPS, CHIPS)), dma((TWO, CHIPS, CHIPS)), dma((CHIPS,)), dma((TWO, CHIPS))]


def sum_semaphores():
    dma, regular = pltpu.SemaphoreType.DMA, pltpu.SemaphoreType.REGULAR
    return [
        dma,
        dma,
        dma((TWO,)),
        dma((TWO,)),
        dma((TWO, TWO)),
        dma((TWO, TWO, TWO)),
        dma((TWO,)),
        dma((TWO, TWO)),
        dma((CHIPS, TWO)),
        dma((TWO, CHIPS, TWO)),
        dma((CHIPS, TWO)),
        dma((TWO, CHIPS, TWO)),
        dma((TWO,)),
        dma((TWO,)),
        dma((TWO,)),
        dma((TWO, CHIPS)),
        dma,
        dma((CHIPS,)),
        regular,
        regular((TWO,)),
    ]


def stream_buffers(piece_in, piece_out):
    return [
        jax.ShapeDtypeStruct((TWO, TWO) + piece_in, BF16),
        jax.ShapeDtypeStruct((TWO, TWO) + piece_out, BF16),
        jax.ShapeDtypeStruct((TWO, CHIPS) + piece_in, BF16),
        jax.ShapeDtypeStruct((TWO, CHIPS) + piece_out, BF16),
    ]


ANYWHERE = pl.BlockSpec(memory_space=pl.ANY)


def forward_stack(x_rows, w_in, w_out):
    layers, depth, hidden_size = w_in.shape
    tokens, width = x_rows.shape
    chunk = w_out.shape[1]
    piece_in, piece_out = (hidden_size // LANES, depth, LANES), (width // LANES, chunk, LANES)
    pieces = [jax.ShapeDtypeStruct((layers,) + piece, BF16) for piece in (piece_in, piece_out)]
    shapes = [jax.ShapeDtypeStruct((layers, tokens, width), BF16)] + pieces * 2 + stream_buffers(piece_in, piece_out)
    outs = pl.pallas_call(
        functools.partial(forward_stack_kernel, layers),
        in_specs=[ANYWHERE] * 3,
        out_specs=[ANYWHERE] * len(shapes),
        out_shape=shapes,
        scratch_shapes=[
            pltpu.VMEM((tokens, width), BF16),
            pltpu.VMEM((width // LANES, tokens, LANES), BF16),
            pltpu.VMEM((tokens, width), F32),
            pltpu.VMEM((TWO, chunk // LANES, width, LANES), BF16),
            pltpu.VMEM((TWO, width // LANES, chunk, LANES), BF16),
            pltpu.VMEM(piece_in, BF16),
            pltpu.VMEM(piece_out, BF16),
            pltpu.SemaphoreType.DMA,
            pltpu.SemaphoreType.DMA((TWO, SHARDS + 1)),
            pltpu.SemaphoreType.DMA((TWO,)),
            pltpu.SemaphoreType.REGULAR((3,)),
        ]
        + stream_semaphores(),
        compiler_params=pltpu.CompilerParams(vmem_limit_bytes=VMEM_LIMIT, collective_id=0, has_side_effects=True),
        cost_estimate=pl.CostEstimate(flops=4 * layers * tokens * width * hidden_size, bytes_accessed=100_000_000, transcendentals=0),
        name="forward_stack",
    )(x_rows, w_in, w_out)
    return outs[:5]


def backward_stack(x_rows, xs, grad_rows, own_in, own_out, kept_in, kept_out):
    layers, blocks_f, depth, _ = own_in.shape
    blocks_d, chunk = own_out.shape[1], own_out.shape[2]
    tokens, width = x_rows.shape
    half, quarter = width // 2, width // 4
    hidden_size = blocks_f * LANES

    def sums(*shape):
        return jax.ShapeDtypeStruct(shape, F32)

    shapes = (
        [sums(layers, depth, hidden_size), sums(layers, chunk, width), jax.ShapeDtypeStruct((tokens, width), BF16)]
        + stream_buffers(own_in.shape[1:], own_out.shape[1:])
        + [
            sums(TWO, CHIPS, TWO, chunk, half),
            sums(TWO, TWO, TWO, chunk, half),
            sums(TWO, TWO, chunk, half),
            sums(TWO, TWO, chunk, half),
            sums(TWO, CHIPS, TWO, half, chunk),
            sums(TWO, CHIPS, TWO, quarter, chunk),
            sums(TWO, CHIPS, TWO, quarter, chunk),
            sums(TWO, CHIPS, TWO, depth, chunk),
        ]
    )
    outs = pl.pallas_call(
        functools.partial(backward_stack_kernel, layers),
        in_specs=[ANYWHERE] * 7,
        out_specs=[ANYWHERE] * len(shapes),
        out_shape=shapes,
        scratch_shapes=[
            pltpu.VMEM((blocks_d, tokens, LANES), BF16),
            pltpu.VMEM((blocks_d, tokens, LANES), BF16),
            pltpu.VMEM((tokens, width), F32),
            pltpu.VMEM((chunk // LANES, tokens, LANES), BF16),
            pltpu.VMEM((chunk // LANES, tokens, LANES), BF16),
            pltpu.VMEM((TWO, chunk // LANES, width, LANES), BF16),
            pltpu.VMEM((TWO, blocks_d, chunk, LANES), BF16),
            pltpu.VMEM((TWO, TWO, TOK_TILE, width), BF16),
            pltpu.VMEM((chunk, width), F32),
            pltpu.VMEM((half, chunk), F32),
            pltpu.VMEM((3, half, chunk), F32),
            pltpu.VMEM((chunk, width), F32),
            pltpu.VMEM((TWO, half, chunk), F32),
            pltpu.VMEM((chunk, half), F32),
            pltpu.VMEM((chunk, half), F32),
            pltpu.VMEM((half, chunk), F32),
            pltpu.VMEM((half, chunk), F32),
            pltpu.SemaphoreType.DMA((blocks_d,)),
            pltpu.SemaphoreType.DMA((TWO, TWO)),
            pltpu.SemaphoreType.DMA((TWO, SHARDS + 1)),
            pltpu.SemaphoreType.REGULAR((3,)),
        ]
        + stream_semaphores()
        + sum_semaphores(),
        compiler_params=pltpu.CompilerParams(vmem_limit_bytes=VMEM_LIMIT, collective_id=1, has_side_effects=True),
        cost_estimate=pl.CostEstimate(flops=10 * layers * tokens * width * hidden_size, bytes_accessed=300_000_000, transcendentals=0),
        name="backward_stack",
    )(x_rows, xs, grad_rows, own_in, own_out, kept_in, kept_out)
    return outs[:3]


def solution(mesh):
    row_spec = P(("local", "data"), None)
    weight_spec = P(None, ("local", "data"), None)

    def device_step(x_rows, grad_rows, w_in, w_out):
        xs, own_in, own_out, kept_in, kept_out = forward_stack(x_rows, w_in, w_out)
        gw_in, gw_out, dx = backward_stack(x_rows, xs, grad_rows, own_in, own_out, kept_in, kept_out)
        return xs[w_in.shape[0] - 1], gw_in, gw_out, dx

    return jax.shard_map(
        device_step,
        mesh=mesh,
        in_specs=(row_spec, row_spec, weight_spec, weight_spec),
        out_specs=(row_spec, weight_spec, weight_spec, row_spec),
        check_vma=False,
    )
```
